32 devices in a mesh: dp: 2 (over x), ws: 16 (over z, y, core).
Axes of the slice: x: 2, y: 2, z: 4, core: 2. Of those that a mesh axis runs over, the one named last changes fastest.
Arguments:
- hidden: bfloat16 [256, 768], P(('dp', 'ws')), parts along dimension 0
- self_k: bfloat16 [256, 12, 192, 64], P(('dp', 'ws')), parts along dimension 0
- self_v: bfloat16 [256, 12, 192, 64], P(('dp', 'ws')), parts along dimension 0
- cross_k: bfloat16 [256, 12, 384, 64], P(('dp', 'ws')), parts along dimension 0
- cross_v: bfloat16 [256, 12, 384, 64], P(('dp', 'ws')), parts along dimension 0
- positions: int32 [256], P(('dp', 'ws')), parts along dimension 0
- enc_mask: int32 [256, 384], P(('dp', 'ws')), parts along dimension 0
- rel_bias: float32 [12, 192], replicated
- expert_idx: int32 [256], P(('dp', 'ws')), parts along dimension 0
- ln_self: float32 [768], replicated
- ln_cross: float32 [768], replicated
- ln_ffn: float32 [768], replicated
- wq_self: bfloat16 [768, 768], P(None, 'ws')
- wk_self: bfloat16 [768, 768], P(None, 'ws')
- wv_self: bfloat16 [768, 768], P(None, 'ws')
- wo_self: bfloat16 [768, 768], P(None, 'ws')
- wq_cross: bfloat16 [768, 768], P(None, 'ws')
- wo_cross: bfloat16 [768, 768], P(None, 'ws')
- w_router: float32 [768, 16], P(None, 'ws')
- w_in: bfloat16 [16, 768, 3072], P(None, None, 'ws')
- w_out: bfloat16 [16, 3072, 768], P(None, 'ws')
Outputs:
- output 1: bfloat16 [256, 768], P(('dp', 'ws')), parts along dimension 0
- output 2: bfloat16 [256, 12, 192, 64], P(('dp', 'ws')), parts along dimension 0
- output 3: bfloat16 [256, 12, 192, 64], P(('dp', 'ws')), parts along dimension 0
There are 2 independent parts. The reference program is written for one: setup_inputs(seed, part) draws one part's arguments, and reference() takes and returns one part's arrays. A program takes and returns all parts, laid end to end along the dimension named above; an argument that names none is the same for every part.
All inputs are finite; a program needn't handle non-finite values.
Results may differ from the reference program's by a relative error of at most 0.0111322.
Values are sent between devices in bfloat16 or wider.
A program may use at most 1 GiB of HBM per device.

```python
import jax
import jax.numpy as jnp
from jax import lax

D_MODEL = 768
NUM_HEADS = 12
HEAD_DIM = 64
D_FF = 3072
EXPERTS = 16
CACHE_LEN = 192
SRC_LEN = 384
GROUP_ROWS = 128

ATTN_WIDTH = NUM_HEADS * HEAD_DIM
CAPACITY = (2 * GROUP_ROWS + EXPERTS - 1) // EXPERTS
EPSILON = 1e-6
NEG_BIG = -1e30


def scaled_normal(key, shape, scale):
    return (jax.random.normal(key, shape, jnp.float32) * scale).astype(jnp.bfloat16)


def setup_inputs(seed: int = 0, part: int = 0) -> dict:
    base_key = jax.random.key(seed)
    shared = jax.random.split(base_key, 13)
    part_keys = jax.random.split(jax.random.fold_in(base_key, part), 12)
    row_ids = jnp.arange(GROUP_ROWS)
    cache_shape = (GROUP_ROWS, NUM_HEADS, CACHE_LEN, HEAD_DIM)
    src_shape = (GROUP_ROWS, NUM_HEADS, SRC_LEN, HEAD_DIM)
    hidden = scaled_normal(part_keys[0], (GROUP_ROWS, D_MODEL), 1.0)
    self_k = scaled_normal(part_keys[1], cache_shape, 1.0)
    self_v = scaled_normal(part_keys[2], cache_shape, 1.0)
    cross_k = scaled_normal(part_keys[3], src_shape, 1.0)
    cross_v = scaled_normal(part_keys[4], src_shape, 1.0)
    positions = jax.random.randint(part_keys[5], (GROUP_ROWS,), 0, CACHE_LEN)
    last_row = jax.random.randint(part_keys[6], (), 0, GROUP_ROWS)
    positions = jnp.where(row_ids == last_row, CACHE_LEN - 1, positions).astype(jnp.int32)
    src_lens = jax.random.randint(part_keys[7], (GROUP_ROWS,), 1, SRC_LEN + 1)
    full_row = jax.random.randint(part_keys[8], (), 0, GROUP_ROWS)
    src_lens = jnp.where(row_ids == full_row, SRC_LEN, src_lens)
    enc_mask = (jnp.arange(SRC_LEN)[None, :] < src_lens[:, None]).astype(jnp.int32)
    hot_expert = jax.random.randint(part_keys[9], (), 0, EXPERTS)
    free_pick = jax.random.randint(part_keys[10], (GROUP_ROWS,), 0, EXPERTS)
    row_order = jax.random.permutation(part_keys[11], GROUP_ROWS)
    hot_rows = jnp.zeros((GROUP_ROWS,), jnp.int32).at[row_order[:CAPACITY + 1]].set(1)
    expert_idx = jnp.where(hot_rows == 1, hot_expert, free_pick).astype(jnp.int32)
    return {
        'hidden': hidden,
        'self_k': self_k,
        'self_v': self_v,
        'cross_k': cross_k,
        'cross_v': cross_v,
        'positions': positions,
        'enc_mask': enc_mask,
        'rel_bias': jax.random.normal(shared[0], (NUM_HEADS, CACHE_LEN), jnp.float32),
        'expert_idx': expert_idx,
        'ln_self': jax.random.uniform(shared[1], (D_MODEL,), jnp.float32, 0.5, 1.5),
        'ln_cross': jax.random.uniform(shared[2], (D_MODEL,), jnp.float32, 0.5, 1.5),
        'ln_ffn': jax.random.uniform(shared[3], (D_MODEL,), jnp.float32, 0.5, 1.5),
        'wq_self': scaled_normal(shared[4], (D_MODEL, ATTN_WIDTH), 1.5 * (D_MODEL * HEAD_DIM) ** -0.5),
        'wk_self': scaled_normal(shared[5], (D_MODEL, ATTN_WIDTH), D_MODEL ** -0.5),
        'wv_self': scaled_normal(shared[6], (D_MODEL, ATTN_WIDTH), D_MODEL ** -0.5),
        'wo_self': scaled_normal(shared[7], (ATTN_WIDTH, D_MODEL), ATTN_WIDTH ** -0.5),
        'wq_cross': scaled_normal(shared[8], (D_MODEL, ATTN_WIDTH), 1.5 * (D_MODEL * HEAD_DIM) ** -0.5),
        'wo_cross': scaled_normal(shared[9], (ATTN_WIDTH, D_MODEL), ATTN_WIDTH ** -0.5),
        'w_router': jax.random.normal(shared[10], (D_MODEL, EXPERTS), jnp.float32) * D_MODEL ** -0.5,
        'w_in': scaled_normal(shared[11], (EXPERTS, D_MODEL, D_FF), D_MODEL ** -0.5),
        'w_out': scaled_normal(shared[12], (EXPERTS, D_FF, D_MODEL), (EXPERTS / D_FF) ** 0.5),
    }


def rms_norm(hidden, scale):
    hid_f32 = hidden.astype(jnp.float32)
    inv_rms = lax.rsqrt(jnp.mean(hid_f32 * hid_f32, axis=-1, keepdims=True) + EPSILON)
    return (hid_f32 * inv_rms * scale).astype(jnp.bfloat16)


def attend_row(row_args):
    queries, cache_keys, cache_vals, score_bias = row_args
    scores = jnp.einsum('hd,hld->hl', queries.astype(jnp.float32), cache_keys.astype(jnp.float32)) + score_bias
    attn_probs = jax.nn.softmax(scores, axis=-1).astype(jnp.bfloat16)
    context = jnp.einsum('hl,hld->hd', attn_probs.astype(jnp.float32), cache_vals.astype(jnp.float32))
    return context.astype(jnp.bfloat16)


def project(x_norm, weight):
    return jnp.dot(x_norm, weight, preferred_element_type=jnp.float32).astype(jnp.bfloat16)


def reference(hidden, self_k, self_v, cross_k, cross_v, positions, enc_mask, rel_bias, expert_idx,
              ln_self, ln_cross, ln_ffn, wq_self, wk_self, wv_self, wo_self, wq_cross, wo_cross,
              w_router, w_in, w_out):
    head_shape = (GROUP_ROWS, NUM_HEADS, HEAD_DIM)
    x_norm = rms_norm(hidden, ln_self)
    queries = project(x_norm, wq_self).reshape(head_shape)
    k_new = project(x_norm, wk_self).reshape(head_shape)
    v_new = project(x_norm, wv_self).reshape(head_shape)
    distance = positions[:, None] - jnp.arange(CACHE_LEN)[None, :]
    write_mask = (distance == 0)[:, None, :, None]
    new_self_k = jnp.where(write_mask, k_new[:, :, None, :], self_k)
    new_self_v = jnp.where(write_mask, v_new[:, :, None, :], self_v)
    pos_bias = jnp.take(rel_bias, jnp.clip(distance, 0, CACHE_LEN - 1), axis=1)
    pos_bias = jnp.where(distance[None] >= 0, pos_bias, NEG_BIG).transpose(1, 0, 2)
    context = lax.map(attend_row, (queries, new_self_k, new_self_v, pos_bias))
    attn_out = jnp.dot(context.reshape(GROUP_ROWS, ATTN_WIDTH), wo_self, preferred_element_type=jnp.float32)
    after_self = (hidden.astype(jnp.float32) + attn_out).astype(jnp.bfloat16)

    x_norm = rms_norm(after_self, ln_cross)
    queries = project(x_norm, wq_cross).reshape(head_shape)
    mask_bias = jnp.where(enc_mask == 1, 0.0, NEG_BIG)[:, None, :]
    context = lax.map(attend_row, (queries, cross_k, cross_v, mask_bias))
    attn_out = jnp.dot(context.reshape(GROUP_ROWS, ATTN_WIDTH), wo_cross, preferred_element_type=jnp.float32)
    after_cross = (after_self.astype(jnp.float32) + attn_out).astype(jnp.bfloat16)

    x_norm = rms_norm(after_cross, ln_ffn)
    logits = jnp.dot(x_norm.astype(jnp.float32), w_router, precision=lax.Precision.HIGHEST,
                     preferred_element_type=jnp.float32)
    router_probs = jax.nn.softmax(logits, axis=-1)
    chosen = jnp.arange(EXPERTS)[None, :] == expert_idx[:, None]
    gate_val = jnp.sum(jnp.where(chosen, router_probs, 0.0), axis=-1)
    row_ids = jnp.arange(GROUP_ROWS)
    earlier = (expert_idx[None, :] == expert_idx[:, None]) & (row_ids[None, :] < row_ids[:, None])
    slot_idx = jnp.sum(earlier.astype(jnp.int32), axis=1)
    keep_gate = jnp.where(slot_idx < CAPACITY, gate_val, 0.0)

    def expert_row(row_args):
        x_row, expert = row_args
        ffn_hidden = jnp.dot(x_row[None, :], w_in[expert], preferred_element_type=jnp.float32)
        ffn_hidden = jax.nn.relu(ffn_hidden).astype(jnp.bfloat16)
        ffn_out = jnp.dot(ffn_hidden, w_out[expert], preferred_element_type=jnp.float32)
        return ffn_out.astype(jnp.bfloat16)[0]

    expert_out = lax.map(expert_row, (x_norm, expert_idx))
    hidden_out = (after_cross.astype(jnp.float32) + expert_out.astype(jnp.float32) * keep_gate[:, None]).astype(jnp.bfloat16)
    return (hidden_out, new_self_k, new_self_v)
```

```python
import jax
import jax.numpy as jnp
from jax import lax
from jax.experimental import pallas as pl
from jax.experimental.pallas import tpu as pltpu
from jax.sharding import PartitionSpec as P

EPS = 1e-6
NEG = -1e30
F32 = jnp.float32
BF16 = jnp.bfloat16
MESH = pl.DeviceIdType.MESH

ROWS = 8
D = 768
HEADS = 12
HPAD = 16
LS = 192
LC = 384
NDEV = 16
CB = 48
NT = (((1,), (1,)), ((), ()))

ALL_OFFS = [(kz, ky, kc) for kz in (2, 3, 1, 0) for ky in (1, 0) for kc in (1, 0) if (kz, ky, kc) != (0, 0, 0)]
SUB_OFFS = [(0, 1, 1), (0, 1, 0), (0, 0, 1)]
Z_OFFS = [(2, 0, 0), (3, 0, 0), (1, 0, 0)]


def dot_nt(a, b, **kw):
    return lax.dot_general(a, b, NT, preferred_element_type=F32, **kw)


def iota(shape, axis):
    return lax.broadcasted_iota(jnp.int32, shape, axis)


def rms(x, g):
    inv = lax.rsqrt(jnp.mean(x * x, axis=-1, keepdims=True) + EPS)
    return (x * inv * g).astype(BF16)


def head_mask():
    row = iota((HPAD, D), 0) * 64
    col = iota((HPAD, D), 1)
    return (col >= row) & (col < row + 64)


def attention(q8, k_ref, v_ref, bias_of, s_ref, ctx_ref):
    hm = head_mask()
    for b in range(ROWS):
        qb = jnp.where(hm, jnp.broadcast_to(q8[b:b + 1, :], (HPAD, D)), 0.0).astype(BF16)
        s_ref[b] = jnp.dot(qb, k_ref[b], preferred_element_type=F32) + bias_of(b)
    s = s_ref[...]
    p = jnp.exp(s - jnp.max(s, axis=-1, keepdims=True))
    s_ref[...] = p / jnp.sum(p, axis=-1, keepdims=True)
    for b in range(ROWS):
        cb = dot_nt(s_ref[b].astype(BF16), v_ref[b])
        ctx_ref[b:b + 1, :] = jnp.sum(jnp.where(hm, cb, 0.0), axis=0, keepdims=True)


def kernel(hid, kT, vT, ckT, cvT, pos_s, mask, rel, idx_s, ln1, ln2, ln3, wq, wk, wv, wo, wqc, woc, wr, win, wout,
           out_h, out_k, out_v,
           ck_v, cv_v, win_v, wout_v, mask_v, rel_v, ln_v, wqkv, m1, st2, r2, wgo, wgq, wgc, rw,
           c3, r4, st5, r5, c6, r7, st8, r8, bias_s, s_self, s_cross, ctx_v, h2_v, x3_v, u_v, k_v, v_v,
           ld, snd, rcv):
    me = lax.axis_index('ws')
    z = me // 4
    s = me % 4
    y = s // 2
    c = s % 2

    def peer_of(off):
        kz, ky, kc = off
        return ((z + kz) % 4) * 4 + ((y + ky) % 2) * 2 + (c + kc) % 2

    def send(src, dst, ph, off):
        pltpu.make_async_remote_copy(src_ref=src, dst_ref=dst, send_sem=snd.at[ph], recv_sem=rcv.at[ph],
                                     device_id={'ws': peer_of(off)}, device_id_type=MESH).start()

    def desc(buf, ph):
        return pltpu.make_async_remote_copy(src_ref=buf, dst_ref=buf, send_sem=snd.at[ph], recv_sem=rcv.at[ph],
                                            device_id={'ws': me}, device_id_type=MESH)

    bar = pltpu.get_barrier_semaphore()
    for off in ALL_OFFS:
        pl.semaphore_signal(bar, inc=1, device_id={'ws': peer_of(off)}, device_id_type=MESH)

    loads = {}

    def load(name, src, dst):
        cp = pltpu.make_async_copy(src, dst, ld.at[len(loads)])
        cp.start()
        loads[name] = cp

    load('hid', hid, m1.at[me, :, pl.ds(0, D)])
    load('wq', wq, wqkv.at[pl.ds(0, CB)])
    load('wk', wk, wqkv.at[pl.ds(CB, CB)])
    load('wv', wv, wqkv.at[pl.ds(2 * CB, CB)])
    load('ln1', ln1, ln_v.at[0])
    load('ln2', ln2, ln_v.at[1])
    load('ln3', ln3, ln_v.at[2])
    load('rel', rel, rel_v)
    load('mask', mask, mask_v)
    load('wr', wr, rw.at[me])
    load('wo', wo, wgo.at[z])
    load('wqc', wqc, wgq.at[z])
    load('woc', woc, wgc.at[z])
    load('k', kT, k_v)
    load('v', vT, v_v)
    load('ck', ckT, ck_v)
    load('cv', cvT, cv_v)
    load('win', win, win_v)
    load('wout', wout, wout_v)

    row8 = iota((ROWS, 128), 0)
    idx_own = jnp.zeros((ROWS, 128), jnp.int32)
    for i in range(ROWS):
        idx_own = jnp.where(row8 == i, idx_s[i], idx_own)
    idx_own = idx_own.astype(F32)
    m1[me, :, D:D + 128] = idx_own.astype(BF16)
    wqkv[3 * CB:256, :] = jnp.zeros((256 - 3 * CB, D), BF16)
    loads['hid'].wait()
    pl.semaphore_wait(bar, NDEV - 1)

    for off in ALL_OFFS:
        send(m1.at[me], m1.at[me], 0, off)

    loads['rel'].wait()
    loads['mask'].wait()
    rel_f = rel_v[...]
    rel_hi = rel_f.astype(BF16)
    rem = rel_f - rel_hi.astype(F32)
    rel_mid = rem.astype(BF16)
    rel_lo = (rem - rel_mid.astype(F32)).astype(BF16)
    src_i = iota((LS, LS), 0)
    dst_i = iota((LS, LS), 1)
    lane12 = iota((HEADS, LS), 1)
    bias_s[...] = jnp.zeros((ROWS, HPAD, LS), F32)
    for b in range(ROWS):
        pick = jnp.where(src_i + dst_i == pos_s[b], 1.0, 0.0).astype(BF16)
        bb = jnp.dot(rel_hi, pick, preferred_element_type=F32)
        bb = bb + jnp.dot(rel_mid, pick, preferred_element_type=F32)
        bb = bb + jnp.dot(rel_lo, pick, preferred_element_type=F32)
        bias_s[b, 0:HEADS, :] = jnp.where(lane12 <= pos_s[b], bb, NEG)
    for name in ('wq', 'wk', 'wv', 'ln1', 'ln2', 'ln3', 'wr', 'wo', 'wqc', 'woc'):
        loads[name].wait()

    desc(m1.at[pl.ds(0, NDEV - 1)], 0).wait_recv()
    hall = m1[:, :, 0:D].astype(F32).reshape(NDEV * ROWS, D)
    xn = rms(hall, ln_v[0])
    st2[...] = dot_nt(xn, wqkv[...]).reshape(NDEV, ROWS, 256).astype(BF16)
    r2[me] = st2[me]
    for off in ALL_OFFS:
        send(st2.at[peer_of(off)], r2.at[me], 1, off)
    for i, w in enumerate((wgo, wgq, wgc)):
        for off in Z_OFFS:
            send(w.at[z], w.at[z], 8 + i, off)
    for off in ALL_OFFS:
        send(rw.at[me], rw.at[me], 11, off)

    sel_r = iota((4 * CB, D), 0)
    sel_q = ((sel_r >= CB).astype(jnp.int32) + (sel_r >= 2 * CB).astype(jnp.int32)
             + (sel_r >= 3 * CB).astype(jnp.int32))
    sel = (iota((4 * CB, D), 1) == sel_r + sel_q * (4 * CB - CB) + s * CB)
    sel = jnp.where(sel, 1.0, 0.0).astype(BF16)
    h_sub = m1[pl.ds(4 * z, 4), :, 0:D].astype(F32).reshape(4 * ROWS, D).astype(BF16)
    h_blk = dot_nt(h_sub, sel)

    idx_all = m1[:, :, D:D + 128].astype(F32).reshape(NDEV * ROWS, 128)
    idx_t = idx_all.T
    earlier = (idx_t[0:ROWS, :] == idx_own) & (iota((ROWS, 128), 1) < me * ROWS + row8)
    slot = jnp.sum(jnp.where(earlier, 1.0, 0.0), axis=-1, keepdims=True)

    loads['k'].wait()
    loads['v'].wait()
    desc(r2.at[pl.ds(0, NDEV - 1)], 1).wait_recv()
    rv = r2[...].astype(F32)

    def columns(lo):
        return jnp.concatenate([rv[d, :, lo:lo + CB] for d in range(NDEV)], axis=-1)

    q8 = columns(0)
    k_cols = columns(CB).T
    v_cols = columns(2 * CB).T
    lane_s = iota((D, LS), 1)
    for b in range(ROWS):
        hit = lane_s == pos_s[b]
        k_v[b] = jnp.where(hit, jnp.broadcast_to(k_cols[:, b:b + 1], (D, LS)), k_v[b].astype(F32)).astype(BF16)
        v_v[b] = jnp.where(hit, jnp.broadcast_to(v_cols[:, b:b + 1], (D, LS)), v_v[b].astype(F32)).astype(BF16)
    st_k = pltpu.make_async_copy(k_v, out_k, ld.at[0])
    st_v = pltpu.make_async_copy(v_v, out_v, ld.at[1])
    st_k.start()
    st_v.start()
    attention(q8, k_v, v_v, lambda b: bias_s[b], s_self, ctx_v)

    def subgroup(buf, ph):
        for off in SUB_OFFS:
            send(buf.at[s], buf.at[s], ph, off)

    def natural(pieces):
        return jnp.concatenate([pieces[t][:, q * CB:(q + 1) * CB] for q in range(4) for t in range(4)], axis=-1)

    c3[s] = ctx_v[...].astype(BF16)
    subgroup(c3, 2)
    desc(wgo.at[pl.ds(0, 3)], 8).wait_recv()
    desc(c3.at[pl.ds(0, 3)], 2).wait_recv()
    ctx = c3[...].astype(F32).reshape(4 * ROWS, D).astype(BF16)
    h1_blk = (h_blk + dot_nt(ctx, wgo[...].reshape(4 * CB, D))).astype(BF16)
    r4[s, :, 0:4 * CB] = h1_blk
    subgroup(r4, 3)
    desc(wgq.at[pl.ds(0, 3)], 9).wait_recv()
    desc(r4.at[pl.ds(0, 3)], 3).wait_recv()
    r4f = r4[...].astype(F32)
    h1 = natural([r4f[t] for t in range(4)])
    x2 = rms(h1, ln_v[1])
    st5[:, :, 0:4 * CB] = dot_nt(x2, wgq[...].reshape(4 * CB, D)).reshape(4, ROWS, 4 * CB).astype(BF16)
    r5[s] = st5[s]
    for off in SUB_OFFS:
        kz, ky, kc = off
        send(st5.at[((y + ky) % 2) * 2 + (c + kc) % 2], r5.at[s], 4, off)
    loads['ck'].wait()
    loads['cv'].wait()
    desc(r5.at[pl.ds(0, 3)], 4).wait_recv()
    r5f = r5[...].astype(F32)
    q2 = natural([r5f[t] for t in range(4)])
    attention(q2, ck_v, cv_v, lambda b: jnp.where(mask_v[b:b + 1, :] == 1, 0.0, NEG), s_cross, ctx_v)

    c6[s] = ctx_v[...].astype(BF16)
    subgroup(c6, 5)
    desc(wgc.at[pl.ds(0, 3)], 10).wait_recv()
    desc(c6.at[pl.ds(0, 3)], 5).wait_recv()
    ctx2 = c6[...].astype(F32).reshape(4 * ROWS, D).astype(BF16)
    h2_blk = (h1_blk.astype(F32) + dot_nt(ctx2, wgc[...].reshape(4 * CB, D))).astype(BF16)
    r7[me, :, 0:4 * CB] = h2_blk
    for off in ALL_OFFS:
        send(r7.at[me], r7.at[me], 6, off)
    loads['win'].wait()
    loads['wout'].wait()
    desc(r7.at[pl.ds(0, NDEV - 1)], 6).wait_recv()
    for t in range(4):
        h2g = natural([r7[4 * t + u].astype(F32) for u in range(4)])
        h2_v[32 * t:32 * t + 32, :] = h2g
        x3_v[32 * t:32 * t + 32, :] = rms(h2g, ln_v[2]).astype(F32)
    x3 = x3_v[...].astype(BF16)
    idx3 = jnp.concatenate([idx_all, idx_all, idx_all], axis=-1)
    half = (iota((NDEV * ROWS, 384), 1) >= 192).astype(F32)
    for p in range(8):
        hh = dot_nt(x3, win_v[2 * p:2 * p + 2].reshape(384, D))
        u_v[:, 384 * p:384 * p + 384] = jnp.where(idx3 == half + float(2 * p), jnp.maximum(hh, 0.0), 0.0).astype(BF16)
    for n in range(3):
        yn = jnp.dot(u_v[...], wout_v[:, :, 256 * n:256 * n + 256].reshape(NDEV * 192, 256),
                     preferred_element_type=F32)
        st8[:, :, 256 * n:256 * n + 256] = yn.reshape(NDEV, ROWS, 256)
    for off in ALL_OFFS:
        send(st8.at[peer_of(off)], r8.at[me], 7, off)
    r8[me] = st8[me]

    desc(rw.at[pl.ds(0, NDEV - 1)], 11).wait_recv()
    x3_own = x3_v[pl.ds(pl.multiple_of(me * ROWS, ROWS), ROWS), :]
    h2_own = h2_v[pl.ds(pl.multiple_of(me * ROWS, ROWS), ROWS), :]
    logits = dot_nt(x3_own, rw[...].reshape(NDEV, D), precision=lax.Precision.HIGHEST)
    ex = jnp.exp(logits - jnp.max(logits, axis=-1, keepdims=True))
    probs = ex / jnp.sum(ex, axis=-1, keepdims=True)
    mine = iota((ROWS, NDEV), 1).astype(F32) == idx_own[:, 0:NDEV]
    gate = jnp.sum(jnp.where(mine, probs, 0.0), axis=-1, keepdims=True)
    gate = jnp.where(slot < float(NDEV), gate, 0.0)

    desc(r8.at[pl.ds(0, NDEV - 1)], 7).wait_recv()
    yv = jnp.sum(r8[...], axis=0).astype(BF16).astype(F32)
    out_h[...] = (h2_own + yv * gate).astype(BF16)

    st_k.wait()
    st_v.wait()
    for buf, ph in ((m1, 0), (st2, 1), (r7, 6), (st8, 7), (rw, 11)):
        desc(buf.at[pl.ds(0, NDEV - 1)], ph).wait_send()
    for buf, ph in ((c3, 2), (r4, 3), (st5, 4), (c6, 5), (wgo, 8), (wgq, 9), (wgc, 10)):
        desc(buf.at[pl.ds(0, 3)], ph).wait_send()


def solution(mesh):
    rows = ('dp', 'ws')
    row_vec = P(rows)
    row_mat = P(rows, None)
    cache = P(rows, None, None, None)
    col = P(None, 'ws')
    in_specs = (row_mat, cache, cache, cache, cache, row_vec, row_mat, P(None, None), row_vec,
                P(None), P(None), P(None), col, col, col, col, col, col,
                col, P(None, None, 'ws'), P(None, 'ws', None))
    out_specs = (row_mat, cache, cache)

    any_spec = pl.BlockSpec(memory_space=pl.ANY)
    smem = pl.BlockSpec(memory_space=pltpu.SMEM)
    vmem = pl.BlockSpec(memory_space=pltpu.VMEM)

    def block(hidden, self_k, self_v, cross_k, cross_v, positions, enc_mask, rel_bias, expert_idx,
              ln_self, ln_cross, ln_ffn, wq_self, wk_self, wv_self, wo_self, wq_cross, wo_cross,
              w_router, w_in, w_out):
        def flat(cache_arr):
            return jnp.swapaxes(cache_arr, 2, 3).reshape(ROWS, D, cache_arr.shape[2])

        def unflat(arr):
            return jnp.swapaxes(arr.reshape(ROWS, HEADS, 64, LS), 2, 3)

        args = (hidden, flat(self_k), flat(self_v), flat(cross_k), flat(cross_v), positions, enc_mask, rel_bias,
                expert_idx, ln_self.reshape(1, D), ln_cross.reshape(1, D), ln_ffn.reshape(1, D),
                wq_self.T, wk_self.T, wv_self.T, wo_self.T, wq_cross.T, wo_cross.T, w_router.T,
                jnp.swapaxes(w_in, 1, 2), w_out)
        specs = [any_spec] * len(args)
        specs[5] = smem
        specs[8] = smem
        V = pltpu.VMEM
        scratch = [
            V((ROWS, D, LC), BF16), V((ROWS, D, LC), BF16), V((NDEV, 192, D), BF16), V((NDEV, 192, D), BF16),
            V((ROWS, LC), jnp.int32), V((HEADS, LS), F32), V((3, 1, D), F32), V((256, D), BF16),
            V((NDEV, ROWS, D + 128), BF16), V((NDEV, ROWS, 256), BF16), V((NDEV, ROWS, 256), BF16),
            V((4, CB, D), BF16), V((4, CB, D), BF16), V((4, CB, D), BF16), V((NDEV, 1, D), F32),
            V((4, ROWS, D), BF16), V((4, 4 * ROWS, 256), BF16), V((4, ROWS, 256), BF16), V((4, ROWS, 256), BF16),
            V((4, ROWS, D), BF16), V((NDEV, 4 * ROWS, 256), BF16), V((NDEV, ROWS, D), F32), V((NDEV, ROWS, D), F32),
            V((ROWS, HPAD, LS), F32), V((ROWS, HPAD, LS), F32), V((ROWS, HPAD, LC), F32), V((ROWS, D), F32),
            V((NDEV * ROWS, D), F32), V((NDEV * ROWS, D), F32), V((NDEV * ROWS, NDEV * 192), BF16),
            V((ROWS, D, LS), BF16), V((ROWS, D, LS), BF16),
            pltpu.SemaphoreType.DMA((19,)), pltpu.SemaphoreType.DMA((12,)), pltpu.SemaphoreType.DMA((12,)),
        ]
        h_out, k_out, v_out = pl.pallas_call(
            kernel,
            out_shape=(jax.ShapeDtypeStruct((ROWS, D), BF16), jax.ShapeDtypeStruct((ROWS, D, LS), BF16),
                       jax.ShapeDtypeStruct((ROWS, D, LS), BF16)),
            in_specs=specs,
            out_specs=(vmem, any_spec, any_spec),
            scratch_shapes=scratch,
            compiler_params=pltpu.CompilerParams(collective_id=0, has_side_effects=True,
                                                 vmem_limit_bytes=60 * 1024 * 1024),
        )(*args)
        return h_out, unflat(k_out), unflat(v_out)

    return jax.shard_map(block, mesh=mesh, in_specs=in_specs, out_specs=out_specs, check_vma=False)
```

```python
import jax
import jax.numpy as jnp
from jax import lax
from jax.experimental import pallas as pl
from jax.experimental.pallas import tpu as pltpu
from jax.sharding import PartitionSpec as P

EPS = 1e-6
NEG = -1e30
F32 = jnp.float32
BF16 = jnp.bfloat16
MESH = pl.DeviceIdType.MESH

ROWS = 8
D = 768
HEADS = 12
HPAD = 16
LS = 192
LC = 384
NDEV = 16
CB = 48
NT = (((1,), (1,)), ((), ()))

ALL_OFFS = [(kz, ky, kc) for kz in (2, 3, 1, 0) for ky in (1, 0) for kc in (1, 0) if (kz, ky, kc) != (0, 0, 0)]
CHIP_OFFS = [off for off in ALL_OFFS if off[2] == 0]
SUB_OFFS = [(0, 1, 1), (0, 1, 0), (0, 0, 1)]
Z_OFFS = [(2, 0, 0), (3, 0, 0), (1, 0, 0)]


def dot_nt(a, b, **kw):
    return lax.dot_general(a, b, NT, preferred_element_type=F32, **kw)


def iota(shape, axis):
    return lax.broadcasted_iota(jnp.int32, shape, axis)


def rms(x, g):
    inv = lax.rsqrt(jnp.mean(x * x, axis=-1, keepdims=True) + EPS)
    return (x * inv * g).astype(BF16)


def head_mask():
    row = iota((HPAD, D), 0) * 64
    col = iota((HPAD, D), 1)
    return (col >= row) & (col < row + 64)


def attention(q8, k_ref, v_ref, bias_of, s_ref, ctx_ref):
    hm = head_mask()
    for b in range(ROWS):
        qb = jnp.where(hm, jnp.broadcast_to(q8[b:b + 1, :], (HPAD, D)), 0.0).astype(BF16)
        s_ref[b] = jnp.dot(qb, k_ref[b], preferred_element_type=F32) + bias_of(b)
    s = s_ref[...]
    p = jnp.exp(s - jnp.max(s, axis=-1, keepdims=True))
    s_ref[...] = p / jnp.sum(p, axis=-1, keepdims=True)
    for b in range(ROWS):
        cb = dot_nt(s_ref[b].astype(BF16), v_ref[b])
        ctx_ref[b:b + 1, :] = jnp.sum(jnp.where(hm, cb, 0.0), axis=0, keepdims=True)


def kernel(hid, kT, vT, ckT, cvT, pos_s, mask, rel, idx_s, ln1, ln2, ln3, wq, wk, wv, wo, wqc, woc, wr, win, wout,
           out_h, k_v, v_v,
           ck_v, cv_v, win_v, wout_v, mask_v, rel_v, ln1_v, ln2_v, ln3_v, wqkv, m1, ix, st2, r2, wgo, wgq, wgc, rw,
           c3, r4, st5, r5, c6, r7, st8, r8, st9, r9, bias_s, s_self, s_cross, ctx_v, h2_v, x3_v, u_v,
           ld, snd, rcv):
    me = lax.axis_index('ws')
    z = me // 4
    s = me % 4
    y = s // 2
    c = s % 2

    def peer_of(off):
        kz, ky, kc = off
        return ((z + kz) % 4) * 4 + ((y + ky) % 2) * 2 + (c + kc) % 2

    def send(src, dst, ph, off):
        pltpu.make_async_remote_copy(src_ref=src, dst_ref=dst, send_sem=snd.at[ph], recv_sem=rcv.at[ph],
                                     device_id={'ws': peer_of(off)}, device_id_type=MESH).start()

    def desc(buf, ph):
        return pltpu.make_async_remote_copy(src_ref=buf, dst_ref=buf, send_sem=snd.at[ph], recv_sem=rcv.at[ph],
                                            device_id={'ws': me}, device_id_type=MESH)

    bar = pltpu.get_barrier_semaphore()
    for off in ALL_OFFS:
        pl.semaphore_signal(bar, inc=1, device_id={'ws': peer_of(off)}, device_id_type=MESH)

    loads = {}

    def load(name, src, dst):
        cp = pltpu.make_async_copy(src, dst, ld.at[len(loads)])
        cp.start()
        loads[name] = cp

    load('hid', hid, m1.at[me])
    load('wq', wq, wqkv.at[pl.ds(0, CB)])
    load('wk', wk, wqkv.at[pl.ds(CB, CB)])
    load('wv', wv, wqkv.at[pl.ds(2 * CB, CB)])
    load('ln1', ln1, ln1_v)
    load('ln2', ln2, ln2_v)
    load('ln3', ln3, ln3_v)
    load('rel', rel, rel_v)
    load('mask', mask, mask_v)
    load('wr', wr, rw.at[me])
    load('wo', wo, wgo.at[z])
    load('wqc', wqc, wgq.at[z])
    load('woc', woc, wgc.at[z])
    load('k', kT, k_v)
    load('v', vT, v_v)
    load('ck', ckT, ck_v)
    load('cv', cvT, cv_v)
    load('win', win, win_v)
    load('wout', wout, wout_v)

    row8 = iota((ROWS, 128), 0)
    idx_own = jnp.zeros((ROWS, 128), jnp.int32)
    for i in range(ROWS):
        idx_own = jnp.where(row8 == i, idx_s[i], idx_own)
    idx_own = idx_own.astype(F32)
    ix[me] = idx_own.astype(BF16)
    wqkv[3 * CB:256, :] = jnp.zeros((256 - 3 * CB, D), BF16)
    loads['hid'].wait()
    pl.semaphore_wait(bar, NDEV - 1)

    for off in ALL_OFFS:
        send(m1.at[me], m1.at[me], 0, off)
    loads['wo'].wait()
    for off in Z_OFFS:
        send(wgo.at[z], wgo.at[z], 8, off)

    loads['rel'].wait()
    loads['mask'].wait()
    rel_f = rel_v[...]
    rel_hi = rel_f.astype(BF16)
    rem = rel_f - rel_hi.astype(F32)
    rel_mid = rem.astype(BF16)
    rel_lo = (rem - rel_mid.astype(F32)).astype(BF16)
    src_i = iota((LS, LS), 0)
    dst_i = iota((LS, LS), 1)
    lane12 = iota((HEADS, LS), 1)
    bias_s[...] = jnp.zeros((ROWS, HPAD, LS), F32)
    for b in range(ROWS):
        pick = jnp.where(src_i + dst_i == pos_s[b], 1.0, 0.0).astype(BF16)
        bb = jnp.dot(rel_hi, pick, preferred_element_type=F32)
        bb = bb + jnp.dot(rel_mid, pick, preferred_element_type=F32)
        bb = bb + jnp.dot(rel_lo, pick, preferred_element_type=F32)
        bias_s[b, 0:HEADS, :] = jnp.where(lane12 <= pos_s[b], bb, NEG)
    for name in ('wq', 'wk', 'wv', 'ln1', 'ln2', 'ln3', 'wr', 'wqc', 'woc'):
        loads[name].wait()

    desc(m1.at[pl.ds(0, NDEV - 1)], 0).wait_recv()
    hall = m1[...].astype(F32).reshape(NDEV * ROWS, D)
    xn = rms(hall, ln1_v[...].reshape(1, D))
    st2[...] = dot_nt(xn, wqkv[...]).reshape(NDEV, ROWS, 256).astype(BF16)
    r2[me] = st2[me]
    for off in ALL_OFFS:
        send(st2.at[peer_of(off)], r2.at[me], 1, off)
    for i, w in enumerate((wgq, wgc)):
        for off in Z_OFFS:
            send(w.at[z], w.at[z], 9 + i, off)
    for off in ALL_OFFS:
        send(ix.at[me], ix.at[me], 12, off)
        send(rw.at[me], rw.at[me], 11, off)

    sel_r = iota((4 * CB, D), 0)
    sel_q = ((sel_r >= CB).astype(jnp.int32) + (sel_r >= 2 * CB).astype(jnp.int32)
             + (sel_r >= 3 * CB).astype(jnp.int32))
    sel = (iota((4 * CB, D), 1) == sel_r + sel_q * (4 * CB - CB) + s * CB)
    sel = jnp.where(sel, 1.0, 0.0).astype(BF16)
    h_sub = m1[pl.ds(4 * z, 4)].astype(F32).reshape(4 * ROWS, D).astype(BF16)
    h_blk = dot_nt(h_sub, sel)

    loads['k'].wait()
    loads['v'].wait()
    desc(r2.at[pl.ds(0, NDEV - 1)], 1).wait_recv()
    rv = r2[...].astype(F32)

    def columns(lo):
        return jnp.concatenate([rv[d, :, lo:lo + CB] for d in range(NDEV)], axis=-1)

    q8 = columns(0)
    k_cols = columns(CB).T
    v_cols = columns(2 * CB).T
    lane_s = iota((D, LS), 1)
    for b in range(ROWS):
        hit = lane_s == pos_s[b]
        k_v[b] = jnp.where(hit, jnp.broadcast_to(k_cols[:, b:b + 1], (D, LS)), k_v[b].astype(F32)).astype(BF16)
        v_v[b] = jnp.where(hit, jnp.broadcast_to(v_cols[:, b:b + 1], (D, LS)), v_v[b].astype(F32)).astype(BF16)
    attention(q8, k_v, v_v, lambda b: bias_s[b], s_self, ctx_v)

    def subgroup(buf, ph):
        for off in SUB_OFFS:
            send(buf.at[s], buf.at[s], ph, off)

    def natural(pieces):
        return jnp.concatenate([pieces[t][:, q * CB:(q + 1) * CB] for q in range(4) for t in range(4)], axis=-1)

    def unpack(blk):
        tail = jnp.concatenate([blk[32:48, 0:64], blk[32:48, 64:128]], axis=0)
        return jnp.concatenate([blk[0:32, :], tail], axis=-1)

    c3[s] = ctx_v[...].astype(BF16)
    subgroup(c3, 2)
    desc(wgo.at[pl.ds(0, 3)], 8).wait_recv()
    desc(c3.at[pl.ds(0, 3)], 2).wait_recv()
    ctx = c3[...].astype(F32).reshape(4 * ROWS, D).astype(BF16)
    h1_blk = (h_blk + dot_nt(ctx, wgo[...].reshape(4 * CB, D))).astype(BF16)
    r4[s, :, 0:4 * CB] = h1_blk
    subgroup(r4, 3)
    desc(wgq.at[pl.ds(0, 3)], 9).wait_recv()
    desc(r4.at[pl.ds(0, 3)], 3).wait_recv()
    r4f = r4[...].astype(F32)
    h1 = natural([r4f[t] for t in range(4)])
    x2 = rms(h1, ln2_v[...].reshape(1, D))
    st5[:, :, 0:4 * CB] = dot_nt(x2, wgq[...].reshape(4 * CB, D)).reshape(4, ROWS, 4 * CB).astype(BF16)
    r5[s] = st5[s]
    for off in SUB_OFFS:
        kz, ky, kc = off
        send(st5.at[((y + ky) % 2) * 2 + (c + kc) % 2], r5.at[s], 4, off)
    loads['ck'].wait()
    loads['cv'].wait()
    desc(r5.at[pl.ds(0, 3)], 4).wait_recv()
    r5f = r5[...].astype(F32)
    q2 = natural([r5f[t] for t in range(4)])
    attention(q2, ck_v, cv_v, lambda b: jnp.where(mask_v[b:b + 1, :] == 1, 0.0, NEG), s_cross, ctx_v)

    c6[s] = ctx_v[...].astype(BF16)
    subgroup(c6, 5)
    desc(wgc.at[pl.ds(0, 3)], 10).wait_recv()
    desc(c6.at[pl.ds(0, 3)], 5).wait_recv()
    ctx2 = c6[...].astype(F32).reshape(4 * ROWS, D).astype(BF16)
    h2_blk = (h1_blk.astype(F32) + dot_nt(ctx2, wgc[...].reshape(4 * CB, D))).astype(BF16)
    h2_f = h2_blk.astype(F32)
    r7[me, 0:32, :] = h2_f[:, 0:128].astype(BF16)
    r7[me, 32:48, :] = jnp.concatenate([h2_f[0:16, 128:192], h2_f[16:32, 128:192]], axis=-1).astype(BF16)
    for off in ALL_OFFS:
        send(r7.at[me], r7.at[me], 6, off)
    desc(ix.at[pl.ds(0, NDEV - 1)], 12).wait_recv()
    idx_all = ix[...].astype(F32).reshape(NDEV * ROWS, 128)
    idx_t = idx_all.T
    earlier = (idx_t[0:ROWS, :] == idx_own) & (iota((ROWS, 128), 1) < me * ROWS + row8)
    slot = jnp.sum(jnp.where(earlier, 1.0, 0.0), axis=-1, keepdims=True)
    loads['win'].wait()
    loads['wout'].wait()
    desc(r7.at[pl.ds(0, NDEV - 1)], 6).wait_recv()
    for t in range(4):
        h2g = natural([unpack(r7[4 * t + u].astype(F32)) for u in range(4)])
        h2_v[32 * t:32 * t + 32, :] = h2g
        x3_v[32 * t:32 * t + 32, :] = rms(h2g, ln3_v[...].reshape(1, D)).astype(F32)
    x3 = x3_v[...].astype(BF16)
    idx3 = jnp.concatenate([idx_all, idx_all, idx_all], axis=-1)
    half = (iota((NDEV * ROWS, 384), 1) >= 192).astype(F32)
    for p in range(8):
        hh = dot_nt(x3, win_v[2 * p:2 * p + 2].reshape(384, D))
        u_v[:, 384 * p:384 * p + 384] = jnp.where(idx3 == half + float(2 * p), jnp.maximum(hh, 0.0), 0.0).astype(BF16)
    chip = me // 2
    sibling = (0, 0, 1)

    def partial(n):
        yn = jnp.dot(u_v[...], wout_v[:, :, 256 * n:256 * n + 256].reshape(NDEV * 192, 256),
                     preferred_element_type=F32).reshape(8, 2, ROWS, 256)
        st8[n, 0] = yn[:, 0]
        st8[n, 1] = yn[:, 1]
        send(st8.at[n, 1 - c], r8.at[n], 13 + n, sibling)

    def reduce_send(n):
        desc(r8.at[n], 13 + n).wait_recv()
        st9[n] = st8[n, c] + r8[n]
        for off in CHIP_OFFS:
            send(st9.at[n, peer_of(off) // 2], r9.at[n, chip], 16 + n, off)
        r9[n, chip] = st9[n, chip]

    partial(0)
    partial(1)
    reduce_send(0)
    partial(2)
    reduce_send(1)
    reduce_send(2)

    desc(rw.at[pl.ds(0, NDEV - 1)], 11).wait_recv()
    x3_own = x3_v[pl.ds(pl.multiple_of(me * ROWS, ROWS), ROWS), :]
    h2_own = h2_v[pl.ds(pl.multiple_of(me * ROWS, ROWS), ROWS), :]
    logits = dot_nt(x3_own, rw[...].reshape(NDEV, D), precision=lax.Precision.HIGHEST)
    ex = jnp.exp(logits - jnp.max(logits, axis=-1, keepdims=True))
    probs = ex / jnp.sum(ex, axis=-1, keepdims=True)
    mine = iota((ROWS, NDEV), 1).astype(F32) == idx_own[:, 0:NDEV]
    gate = jnp.sum(jnp.where(mine, probs, 0.0), axis=-1, keepdims=True)
    gate = jnp.where(slot < float(NDEV), gate, 0.0)

    for n in range(3):
        desc(r9.at[n, pl.ds(0, 7)], 16 + n).wait_recv()
    yv = jnp.concatenate([jnp.sum(r9[n], axis=0) for n in range(3)], axis=-1).astype(BF16).astype(F32)
    out_h[...] = (h2_own + yv * gate).astype(BF16)

    for buf, ph in ((m1, 0), (st2, 1), (r7, 6), (rw, 11), (ix, 12)):
        desc(buf.at[pl.ds(0, NDEV - 1)], ph).wait_send()
    for n in range(3):
        desc(st9.at[n, pl.ds(0, 7)], 16 + n).wait_send()
        desc(r8.at[n], 13 + n).wait_send()
    for buf, ph in ((c3, 2), (r4, 3), (st5, 4), (c6, 5), (wgo, 8), (wgq, 9), (wgc, 10)):
        desc(buf.at[pl.ds(0, 3)], ph).wait_send()


def store(h_in, k_in, v_in, h_out, k_out, v_out, sem):
    copies = [pltpu.make_async_copy(src, dst, sem.at[i])
              for i, (src, dst) in enumerate(((k_in, k_out), (v_in, v_out), (h_in, h_out)))]
    for cp in copies:
        cp.start()
    for cp in copies:
        cp.wait()


def solution(mesh):
    rows = ('dp', 'ws')
    row_vec = P(rows)
    row_mat = P(rows, None)
    cache = P(rows, None, None, None)
    col = P(None, 'ws')
    in_specs = (row_mat, cache, cache, cache, cache, row_vec, row_mat, P(None, None), row_vec,
                P(None), P(None), P(None), col, col, col, col, col, col,
                col, P(None, None, 'ws'), P(None, 'ws', None))
    out_specs = (row_mat, cache, cache)

    any_spec = pl.BlockSpec(memory_space=pltpu.HBM)
    smem = pl.BlockSpec(memory_space=pltpu.SMEM)
    vmem = pl.BlockSpec(memory_space=pltpu.VMEM)

    def block(hidden, self_k, self_v, cross_k, cross_v, positions, enc_mask, rel_bias, expert_idx,
              ln_self, ln_cross, ln_ffn, wq_self, wk_self, wv_self, wo_self, wq_cross, wo_cross,
              w_router, w_in, w_out):
        def flat(cache_arr):
            return jnp.swapaxes(cache_arr, 2, 3).reshape(ROWS, D, cache_arr.shape[2])

        def unflat(arr):
            return jnp.swapaxes(arr.reshape(ROWS, HEADS, 64, LS), 2, 3)

        args = (hidden, flat(self_k), flat(self_v), flat(cross_k), flat(cross_v), positions, enc_mask, rel_bias,
                expert_idx, ln_self, ln_cross, ln_ffn,
                wq_self.T, wk_self.T, wv_self.T, wo_self.T, wq_cross.T, wo_cross.T, w_router.T,
                jnp.swapaxes(w_in, 1, 2), w_out)
        specs = [any_spec] * len(args)
        specs[5] = smem
        specs[8] = smem
        V = pltpu.VMEM
        scratch = [
            V((ROWS, D, LC), BF16), V((ROWS, D, LC), BF16), V((NDEV, 192, D), BF16), V((NDEV, 192, D), BF16),
            V((ROWS, LC), jnp.int32), V((HEADS, LS), F32), V((D,), F32), V((D,), F32), V((D,), F32), V((256, D), BF16),
            V((NDEV, ROWS, D), BF16), V((NDEV, ROWS, 128), BF16), V((NDEV, ROWS, 256), BF16), V((NDEV, ROWS, 256), BF16),
            V((4, CB, D), BF16), V((4, CB, D), BF16), V((4, CB, D), BF16), V((NDEV, 1, D), F32),
            V((4, ROWS, D), BF16), V((4, 4 * ROWS, 256), BF16), V((4, ROWS, 256), BF16), V((4, ROWS, 256), BF16),
            V((4, ROWS, D), BF16), V((NDEV, CB, 128), BF16), V((3, 2, 8, ROWS, 256), F32), V((3, 8, ROWS, 256), F32),
            V((3, 8, ROWS, 256), F32), V((3, 8, ROWS, 256), F32),
            V((ROWS, HPAD, LS), F32), V((ROWS, HPAD, LS), F32), V((ROWS, HPAD, LC), F32), V((ROWS, D), F32),
            V((NDEV * ROWS, D), F32), V((NDEV * ROWS, D), F32), V((NDEV * ROWS, NDEV * 192), BF16),
            pltpu.SemaphoreType.DMA((19,)), pltpu.SemaphoreType.DMA((19,)), pltpu.SemaphoreType.DMA((19,)),
        ]
        h_out, k_out, v_out = pl.pallas_call(
            kernel,
            out_shape=(V((ROWS, D), BF16), V((ROWS, D, LS), BF16), V((ROWS, D, LS), BF16)),
            in_specs=specs,
            out_specs=(vmem, vmem, vmem),
            scratch_shapes=scratch,
            compiler_params=pltpu.CompilerParams(collective_id=0, has_side_effects=True,
                                                 vmem_limit_bytes=67043328 - 2 * 3145728 - 16384),
        )(*args)
        outs = (jax.ShapeDtypeStruct((ROWS, D), BF16), jax.ShapeDtypeStruct((ROWS, D, LS), BF16),
                jax.ShapeDtypeStruct((ROWS, D, LS), BF16))
        h_out, k_out, v_out = pl.pallas_call(
            store, out_shape=outs, in_specs=[vmem] * 3, out_specs=(any_spec,) * 3,
            scratch_shapes=[pltpu.SemaphoreType.DMA((3,))],
            compiler_params=pltpu.CompilerParams(vmem_limit_bytes=4 * 1024 * 1024),
        )(h_out, k_out, v_out)
        return h_out, unflat(k_out), unflat(v_out)

    return jax.shard_map(block, mesh=mesh, in_specs=in_specs, out_specs=out_specs, check_vma=False)
```

```python
import jax
import jax.numpy as jnp
from jax import lax
from jax.experimental import pallas as pl
from jax.experimental.pallas import tpu as pltpu
from jax.sharding import PartitionSpec as P

EPS = 1e-6
NEG = -1e30
F32 = jnp.float32
BF16 = jnp.bfloat16
MESH = pl.DeviceIdType.MESH

ROWS = 8
D = 768
HEADS = 12
HPAD = 16
LS = 192
LC = 384
NDEV = 16
CB = 48
NT = (((1,), (1,)), ((), ()))

ALL_OFFS = [(kz, ky, kc) for kz in (2, 3, 1, 0) for ky in (1, 0) for kc in (1, 0) if (kz, ky, kc) != (0, 0, 0)]
CHIP_OFFS = [off for off in ALL_OFFS if off[2] == 0]
SUB_OFFS = [(0, 1, 1), (0, 1, 0), (0, 0, 1)]
Z_OFFS = [(2, 0, 0), (3, 0, 0), (1, 0, 0)]


def dot_nt(a, b, **kw):
    return lax.dot_general(a, b, NT, preferred_element_type=F32, **kw)


def iota(shape, axis):
    return lax.broadcasted_iota(jnp.int32, shape, axis)


def rms(x, g):
    inv = lax.rsqrt(jnp.mean(x * x, axis=-1, keepdims=True) + EPS)
    return (x * inv * g).astype(BF16)


def head_mask():
    row = iota((HPAD, D), 0) * 64
    col = iota((HPAD, D), 1)
    return (col >= row) & (col < row + 64)


def attention(q8, k_ref, v_ref, bias_of, s_ref, ctx_ref):
    hm = head_mask()
    for b in range(ROWS):
        qb = jnp.where(hm, jnp.broadcast_to(q8[b:b + 1, :], (HPAD, D)), 0.0).astype(BF16)
        s_ref[b] = jnp.dot(qb, k_ref[b], preferred_element_type=F32) + bias_of(b)
    s = s_ref[...]
    p = jnp.exp(s - jnp.max(s, axis=-1, keepdims=True))
    s_ref[...] = p / jnp.sum(p, axis=-1, keepdims=True)
    for b in range(ROWS):
        cb = dot_nt(s_ref[b].astype(BF16), v_ref[b])
        ctx_ref[b:b + 1, :] = jnp.sum(jnp.where(hm, cb, 0.0), axis=0, keepdims=True)


def kernel(hid, kT, vT, ckT, cvT, pos_s, mask, rel, idx_s, ln1, ln2, ln3, wq, wk, wv, wo, wqc, woc, wr, win, wout,
           out_h, k_v, v_v,
           ck_v, cv_v, win_v, wout_v, mask_v, rel_v, ln1_v, ln2_v, ln3_v, wqkv, m1, ix, st2, r2, wgo, wgq, wgc, rw,
           c3, r4, st5, r5, c6, r7, st8, r8, st9, r9, bias_s, s_self, s_cross, ctx_v, h2_v, x3_v, u_v,
           ld, snd, rcv):
    me = lax.axis_index('ws')
    z = me // 4
    s = me % 4
    y = s // 2
    c = s % 2

    def peer_of(off):
        kz, ky, kc = off
        return ((z + kz) % 4) * 4 + ((y + ky) % 2) * 2 + (c + kc) % 2

    def send(src, dst, ph, off):
        pltpu.make_async_remote_copy(src_ref=src, dst_ref=dst, send_sem=snd.at[ph], recv_sem=rcv.at[ph],
                                     device_id={'ws': peer_of(off)}, device_id_type=MESH).start()

    def desc(buf, ph):
        return pltpu.make_async_remote_copy(src_ref=buf, dst_ref=buf, send_sem=snd.at[ph], recv_sem=rcv.at[ph],
                                            device_id={'ws': me}, device_id_type=MESH)

    bar = pltpu.get_barrier_semaphore()
    for off in ALL_OFFS:
        pl.semaphore_signal(bar, inc=1, device_id={'ws': peer_of(off)}, device_id_type=MESH)

    loads = {}

    def load(name, src, dst):
        cp = pltpu.make_async_copy(src, dst, ld.at[len(loads)])
        cp.start()
        loads[name] = cp

    load('hid', hid, m1.at[me])
    load('wq', wq, wqkv.at[pl.ds(0, CB)])
    load('wk', wk, wqkv.at[pl.ds(CB, CB)])
    load('wv', wv, wqkv.at[pl.ds(2 * CB, CB)])
    load('ln1', ln1, ln1_v)
    load('ln2', ln2, ln2_v)
    load('ln3', ln3, ln3_v)
    load('rel', rel, rel_v)
    load('mask', mask, mask_v)
    load('wr', wr, rw.at[me])
    load('wo', wo, wgo.at[z])
    load('wqc', wqc, wgq.at[z])
    load('woc', woc, wgc.at[z])

    row8 = iota((ROWS, 128), 0)
    idx_own = jnp.zeros((ROWS, 128), jnp.int32)
    for i in range(ROWS):
        idx_own = jnp.where(row8 == i, idx_s[i], idx_own)
    idx_own = idx_own.astype(F32)
    ix[me] = idx_own.astype(BF16)
    wqkv[3 * CB:256, :] = jnp.zeros((256 - 3 * CB, D), BF16)
    loads['hid'].wait()
    pl.semaphore_wait(bar, NDEV - 1)

    for off in ALL_OFFS:
        send(m1.at[me], m1.at[me], 0, off)
    loads['wo'].wait()
    for off in Z_OFFS:
        send(wgo.at[z], wgo.at[z], 8, off)
    load('k', kT, k_v)
    load('v', vT, v_v)

    loads['rel'].wait()
    loads['mask'].wait()
    rel_f = rel_v[...]
    rel_hi = rel_f.astype(BF16)
    rem = rel_f - rel_hi.astype(F32)
    rel_mid = rem.astype(BF16)
    rel_lo = (rem - rel_mid.astype(F32)).astype(BF16)
    src_i = iota((LS, LS), 0)
    dst_i = iota((LS, LS), 1)
    lane12 = iota((HEADS, LS), 1)
    bias_s[...] = jnp.zeros((ROWS, HPAD, LS), F32)
    for b in range(ROWS):
        pick = jnp.where(src_i + dst_i == pos_s[b], 1.0, 0.0).astype(BF16)
        bb = jnp.dot(rel_hi, pick, preferred_element_type=F32)
        bb = bb + jnp.dot(rel_mid, pick, preferred_element_type=F32)
        bb = bb + jnp.dot(rel_lo, pick, preferred_element_type=F32)
        bias_s[b, 0:HEADS, :] = jnp.where(lane12 <= pos_s[b], bb, NEG)
    for name in ('wq', 'wk', 'wv', 'ln1', 'ln2', 'ln3', 'wr', 'wqc', 'woc'):
        loads[name].wait()

    desc(m1.at[pl.ds(0, NDEV - 1)], 0).wait_recv()
    hall = m1[...].astype(F32).reshape(NDEV * ROWS, D)
    xn = rms(hall, ln1_v[...].reshape(1, D))
    st2[...] = dot_nt(xn, wqkv[...]).reshape(NDEV, ROWS, 256).astype(BF16)
    r2[me] = st2[me]
    for off in ALL_OFFS:
        send(st2.at[peer_of(off)], r2.at[me], 1, off)
    for i, w in enumerate((wgq, wgc)):
        for off in Z_OFFS:
            send(w.at[z], w.at[z], 9 + i, off)
    for off in ALL_OFFS:
        send(ix.at[me], ix.at[me], 12, off)
        send(rw.at[me], rw.at[me], 11, off)
    load('ck', ckT, ck_v)
    load('cv', cvT, cv_v)

    sel_r = iota((4 * CB, D), 0)
    sel_q = ((sel_r >= CB).astype(jnp.int32) + (sel_r >= 2 * CB).astype(jnp.int32)
             + (sel_r >= 3 * CB).astype(jnp.int32))
    sel = (iota((4 * CB, D), 1) == sel_r + sel_q * (4 * CB - CB) + s * CB)
    sel = jnp.where(sel, 1.0, 0.0).astype(BF16)
    h_sub = m1[pl.ds(4 * z, 4)].astype(F32).reshape(4 * ROWS, D).astype(BF16)
    h_blk = dot_nt(h_sub, sel)

    loads['k'].wait()
    loads['v'].wait()
    desc(r2.at[pl.ds(0, NDEV - 1)], 1).wait_recv()
    rv = r2[...].astype(F32)

    def columns(lo):
        return jnp.concatenate([rv[d, :, lo:lo + CB] for d in range(NDEV)], axis=-1)

    q8 = columns(0)
    k_cols = columns(CB).T
    v_cols = columns(2 * CB).T
    lane_s = iota((D, LS), 1)
    for b in range(ROWS):
        hit = lane_s == pos_s[b]
        k_v[b] = jnp.where(hit, jnp.broadcast_to(k_cols[:, b:b + 1], (D, LS)), k_v[b].astype(F32)).astype(BF16)
        v_v[b] = jnp.where(hit, jnp.broadcast_to(v_cols[:, b:b + 1], (D, LS)), v_v[b].astype(F32)).astype(BF16)
    attention(q8, k_v, v_v, lambda b: bias_s[b], s_self, ctx_v)

    def subgroup(buf, ph):
        for off in SUB_OFFS:
            send(buf.at[s], buf.at[s], ph, off)

    def natural(pieces):
        return jnp.concatenate([pieces[t][:, q * CB:(q + 1) * CB] for q in range(4) for t in range(4)], axis=-1)

    def unpack(blk):
        tail = jnp.concatenate([blk[32:48, 0:64], blk[32:48, 64:128]], axis=0)
        return jnp.concatenate([blk[0:32, :], tail], axis=-1)

    c3[s] = ctx_v[...].astype(BF16)
    subgroup(c3, 2)
    load('win', win, win_v)
    load('wout', wout, wout_v)
    desc(wgo.at[pl.ds(0, 3)], 8).wait_recv()
    desc(c3.at[pl.ds(0, 3)], 2).wait_recv()
    ctx = c3[...].astype(F32).reshape(4 * ROWS, D).astype(BF16)
    h1_blk = (h_blk + dot_nt(ctx, wgo[...].reshape(4 * CB, D))).astype(BF16)
    r4[s, :, 0:4 * CB] = h1_blk
    subgroup(r4, 3)
    desc(wgq.at[pl.ds(0, 3)], 9).wait_recv()
    desc(r4.at[pl.ds(0, 3)], 3).wait_recv()
    r4f = r4[...].astype(F32)
    h1 = natural([r4f[t] for t in range(4)])
    x2 = rms(h1, ln2_v[...].reshape(1, D))
    st5[:, :, 0:4 * CB] = dot_nt(x2, wgq[...].reshape(4 * CB, D)).reshape(4, ROWS, 4 * CB).astype(BF16)
    r5[s] = st5[s]
    for off in SUB_OFFS:
        kz, ky, kc = off
        send(st5.at[((y + ky) % 2) * 2 + (c + kc) % 2], r5.at[s], 4, off)
    loads['ck'].wait()
    loads['cv'].wait()
    desc(r5.at[pl.ds(0, 3)], 4).wait_recv()
    r5f = r5[...].astype(F32)
    q2 = natural([r5f[t] for t in range(4)])
    attention(q2, ck_v, cv_v, lambda b: jnp.where(mask_v[b:b + 1, :] == 1, 0.0, NEG), s_cross, ctx_v)

    c6[s] = ctx_v[...].astype(BF16)
    subgroup(c6, 5)
    desc(wgc.at[pl.ds(0, 3)], 10).wait_recv()
    desc(c6.at[pl.ds(0, 3)], 5).wait_recv()
    ctx2 = c6[...].astype(F32).reshape(4 * ROWS, D).astype(BF16)
    h2_blk = (h1_blk.astype(F32) + dot_nt(ctx2, wgc[...].reshape(4 * CB, D))).astype(BF16)
    h2_f = h2_blk.astype(F32)
    r7[me, 0:32, :] = h2_f[:, 0:128].astype(BF16)
    r7[me, 32:48, :] = jnp.concatenate([h2_f[0:16, 128:192], h2_f[16:32, 128:192]], axis=-1).astype(BF16)
    for off in ALL_OFFS:
        send(r7.at[me], r7.at[me], 6, off)
    desc(ix.at[pl.ds(0, NDEV - 1)], 12).wait_recv()
    idx_all = ix[...].astype(F32).reshape(NDEV * ROWS, 128)
    idx_t = idx_all.T
    earlier = (idx_t[0:ROWS, :] == idx_own) & (iota((ROWS, 128), 1) < me * ROWS + row8)
    slot = jnp.sum(jnp.where(earlier, 1.0, 0.0), axis=-1, keepdims=True)
    loads['win'].wait()
    loads['wout'].wait()
    desc(r7.at[pl.ds(0, NDEV - 1)], 6).wait_recv()
    for t in range(4):
        h2g = natural([unpack(r7[4 * t + u].astype(F32)) for u in range(4)])
        h2_v[32 * t:32 * t + 32, :] = h2g
        x3_v[32 * t:32 * t + 32, :] = rms(h2g, ln3_v[...].reshape(1, D)).astype(F32)
    x3 = x3_v[...].astype(BF16)
    idx3 = jnp.concatenate([idx_all, idx_all, idx_all], axis=-1)
    half = (iota((NDEV * ROWS, 384), 1) >= 192).astype(F32)
    for p in range(8):
        hh = dot_nt(x3, win_v[2 * p:2 * p + 2].reshape(384, D))
        u_v[:, 384 * p:384 * p + 384] = jnp.where(idx3 == half + float(2 * p), jnp.maximum(hh, 0.0), 0.0).astype(BF16)
    chip = me // 2
    sibling = (0, 0, 1)

    def partial(n):
        yn = jnp.dot(u_v[...], wout_v[:, :, 256 * n:256 * n + 256].reshape(NDEV * 192, 256),
                     preferred_element_type=F32).reshape(8, 2, ROWS, 256)
        st8[n, 0] = yn[:, 0]
        st8[n, 1] = yn[:, 1]
        send(st8.at[n, 1 - c], r8.at[n], 13 + n, sibling)

    def reduce_send(n):
        desc(r8.at[n], 13 + n).wait_recv()
        st9[n] = st8[n, c] + r8[n]
        for off in CHIP_OFFS:
            send(st9.at[n, peer_of(off) // 2], r9.at[n, chip], 16 + n, off)
        r9[n, chip] = st9[n, chip]

    partial(0)
    partial(1)
    reduce_send(0)
    partial(2)
    reduce_send(1)
    reduce_send(2)

    desc(rw.at[pl.ds(0, NDEV - 1)], 11).wait_recv()
    x3_own = x3_v[pl.ds(pl.multiple_of(me * ROWS, ROWS), ROWS), :]
    h2_own = h2_v[pl.ds(pl.multiple_of(me * ROWS, ROWS), ROWS), :]
    logits = dot_nt(x3_own, rw[...].reshape(NDEV, D), precision=lax.Precision.HIGHEST)
    ex = jnp.exp(logits - jnp.max(logits, axis=-1, keepdims=True))
    probs = ex / jnp.sum(ex, axis=-1, keepdims=True)
    mine = iota((ROWS, NDEV), 1).astype(F32) == idx_own[:, 0:NDEV]
    gate = jnp.sum(jnp.where(mine, probs, 0.0), axis=-1, keepdims=True)
    gate = jnp.where(slot < float(NDEV), gate, 0.0)

    for n in range(3):
        desc(r9.at[n, pl.ds(0, 7)], 16 + n).wait_recv()
    yv = jnp.concatenate([jnp.sum(r9[n], axis=0) for n in range(3)], axis=-1).astype(BF16).astype(F32)
    out_h[...] = (h2_own + yv * gate).astype(BF16)

    for buf, ph in ((m1, 0), (st2, 1), (r7, 6), (rw, 11), (ix, 12)):
        desc(buf.at[pl.ds(0, NDEV - 1)], ph).wait_send()
    for n in range(3):
        desc(st9.at[n, pl.ds(0, 7)], 16 + n).wait_send()
        desc(r8.at[n], 13 + n).wait_send()
    for buf, ph in ((c3, 2), (r4, 3), (st5, 4), (c6, 5), (wgo, 8), (wgq, 9), (wgc, 10)):
        desc(buf.at[pl.ds(0, 3)], ph).wait_send()


def store(h_in, k_in, v_in, h_out, k_out, v_out, sem):
    copies = [pltpu.make_async_copy(src, dst, sem.at[i])
              for i, (src, dst) in enumerate(((k_in, k_out), (v_in, v_out), (h_in, h_out)))]
    for cp in copies:
        cp.start()
    for cp in copies:
        cp.wait()


def solution(mesh):
    rows = ('dp', 'ws')
    row_vec = P(rows)
    row_mat = P(rows, None)
    cache = P(rows, None, None, None)
    col = P(None, 'ws')
    in_specs = (row_mat, cache, cache, cache, cache, row_vec, row_mat, P(None, None), row_vec,
                P(None), P(None), P(None), col, col, col, col, col, col,
                col, P(None, None, 'ws'), P(None, 'ws', None))
    out_specs = (row_mat, cache, cache)

    any_spec = pl.BlockSpec(memory_space=pltpu.HBM)
    smem = pl.BlockSpec(memory_space=pltpu.SMEM)
    vmem = pl.BlockSpec(memory_space=pltpu.VMEM)

    def block(hidden, self_k, self_v, cross_k, cross_v, positions, enc_mask, rel_bias, expert_idx,
              ln_self, ln_cross, ln_ffn, wq_self, wk_self, wv_self, wo_self, wq_cross, wo_cross,
              w_router, w_in, w_out):
        def flat(cache_arr):
            return jnp.swapaxes(cache_arr, 2, 3).reshape(ROWS, D, cache_arr.shape[2])

        def unflat(arr):
            return jnp.swapaxes(arr.reshape(ROWS, HEADS, 64, LS), 2, 3)

        args = (hidden, flat(self_k), flat(self_v), flat(cross_k), flat(cross_v), positions, enc_mask, rel_bias,
                expert_idx, ln_self, ln_cross, ln_ffn,
                wq_self.T, wk_self.T, wv_self.T, wo_self.T, wq_cross.T, wo_cross.T, w_router.T,
                jnp.swapaxes(w_in, 1, 2), w_out)
        specs = [any_spec] * len(args)
        specs[5] = smem
        specs[8] = smem
        V = pltpu.VMEM
        scratch = [
            V((ROWS, D, LC), BF16), V((ROWS, D, LC), BF16), V((NDEV, 192, D), BF16), V((NDEV, 192, D), BF16),
            V((ROWS, LC), jnp.int32), V((HEADS, LS), F32), V((D,), F32), V((D,), F32), V((D,), F32), V((256, D), BF16),
            V((NDEV, ROWS, D), BF16), V((NDEV, ROWS, 128), BF16), V((NDEV, ROWS, 256), BF16), V((NDEV, ROWS, 256), BF16),
            V((4, CB, D), BF16), V((4, CB, D), BF16), V((4, CB, D), BF16), V((NDEV, 1, D), F32),
            V((4, ROWS, D), BF16), V((4, 4 * ROWS, 256), BF16), V((4, ROWS, 256), BF16), V((4, ROWS, 256), BF16),
            V((4, ROWS, D), BF16), V((NDEV, CB, 128), BF16), V((3, 2, 8, ROWS, 256), F32), V((3, 8, ROWS, 256), F32),
            V((3, 8, ROWS, 256), F32), V((3, 8, ROWS, 256), F32),
            V((ROWS, HPAD, LS), F32), V((ROWS, HPAD, LS), F32), V((ROWS, HPAD, LC), F32), V((ROWS, D), F32),
            V((NDEV * ROWS, D), F32), V((NDEV * ROWS, D), F32), V((NDEV * ROWS, NDEV * 192), BF16),
            pltpu.SemaphoreType.DMA((19,)), pltpu.SemaphoreType.DMA((19,)), pltpu.SemaphoreType.DMA((19,)),
        ]
        h_out, k_out, v_out = pl.pallas_call(
            kernel,
            out_shape=(V((ROWS, D), BF16), V((ROWS, D, LS), BF16), V((ROWS, D, LS), BF16)),
            in_specs=specs,
            out_specs=(vmem, vmem, vmem),
            scratch_shapes=scratch,
            compiler_params=pltpu.CompilerParams(collective_id=0, has_side_effects=True,
                                                 vmem_limit_bytes=67043328 - 2 * 3145728 - 16384),
        )(*args)
        outs = (jax.ShapeDtypeStruct((ROWS, D), BF16), jax.ShapeDtypeStruct((ROWS, D, LS), BF16),
                jax.ShapeDtypeStruct((ROWS, D, LS), BF16))
        h_out, k_out, v_out = pl.pallas_call(
            store, out_shape=outs, in_specs=[vmem] * 3, out_specs=(any_spec,) * 3,
            scratch_shapes=[pltpu.SemaphoreType.DMA((3,))],
            compiler_params=pltpu.CompilerParams(vmem_limit_bytes=4 * 1024 * 1024),
        )(h_out, k_out, v_out)
        return h_out, unflat(k_out), unflat(v_out)

    return jax.shard_map(block, mesh=mesh, in_specs=in_specs, out_specs=out_specs, check_vma=False)
```

```python
import jax
import jax.numpy as jnp
from jax import lax
from jax.experimental import pallas as pl
from jax.experimental.pallas import tpu as pltpu
from jax.sharding import PartitionSpec as P

EPS = 1e-6
NEG = -1e30
F32 = jnp.float32
BF16 = jnp.bfloat16
MESH = pl.DeviceIdType.MESH

ROWS = 8
D = 768
HEADS = 12
HPAD = 16
LS = 192
LC = 384
NDEV = 16
CB = 48
NT = (((1,), (1,)), ((), ()))

ALL_OFFS = [(kz, ky, kc) for kz in (2, 3, 1, 0) for ky in (1, 0) for kc in (1, 0) if (kz, ky, kc) != (0, 0, 0)]
CHIP_OFFS = [off for off in ALL_OFFS if off[2] == 0]
NEAR_FIRST = [(0, 1, 0), (1, 0, 0), (3, 0, 0), (1, 1, 0), (3, 1, 0), (2, 0, 0), (2, 1, 0)]
SIBLING = (0, 0, 1)
SUB_OFFS = [(0, 1, 1), (0, 1, 0), (0, 0, 1)]
Z_OFFS = [(2, 0, 0), (3, 0, 0), (1, 0, 0)]


def dot_nt(a, b, **kw):
    return lax.dot_general(a, b, NT, preferred_element_type=F32, **kw)


def iota(shape, axis):
    return lax.broadcasted_iota(jnp.int32, shape, axis)


def rms(x, g):
    inv = lax.rsqrt(jnp.mean(x * x, axis=-1, keepdims=True) + EPS)
    return (x * inv * g).astype(BF16)


def head_mask():
    row = iota((HPAD, D), 0) * 64
    col = iota((HPAD, D), 1)
    return (col >= row) & (col < row + 64)


def attention(q8, k_ref, v_ref, bias_of, s_ref, ctx_ref):
    hm = head_mask()
    for b in range(ROWS):
        qb = jnp.where(hm, jnp.broadcast_to(q8[b:b + 1, :], (HPAD, D)), 0.0).astype(BF16)
        s_ref[b] = jnp.dot(qb, k_ref[b], preferred_element_type=F32) + bias_of(b)
    s = s_ref[...]
    p = jnp.exp(s - jnp.max(s, axis=-1, keepdims=True))
    s_ref[...] = p / jnp.sum(p, axis=-1, keepdims=True)
    for b in range(ROWS):
        cb = dot_nt(s_ref[b].astype(BF16), v_ref[b])
        ctx_ref[b:b + 1, :] = jnp.sum(jnp.where(hm, cb, 0.0), axis=0, keepdims=True)


def kernel(hid, kT, vT, ckT, cvT, pos_s, mask, rel, idx_s, ln1, ln2, ln3, wq, wk, wv, wo, wqc, woc, wr, win, wout,
           out_h, k_v, v_v,
           ck_v, cv_v, win_v, wout_v, mask_v, rel_v, ln1_v, ln2_v, ln3_v, wqkv, m1, ix, st2, r2, wgo, wgq, wgc, rw,
           c3, r4, st5, r5, c6, r7, st8, r8, st9, r9, bias_s, s_self, s_cross, ctx_v, h2_v, x3_v, u_v,
           ld, snd, rcv, direct):
    me = lax.axis_index('ws')
    dpi = lax.axis_index('dp')
    z = me // 4
    s = me % 4
    y = s // 2
    c = s % 2

    def peer_of(off):
        kz, ky, kc = off
        return ((z + kz) % 4) * 4 + ((y + ky) % 2) * 2 + (c + kc) % 2

    def send(src, dst, ph, off):
        pltpu.make_async_remote_copy(src_ref=src, dst_ref=dst, send_sem=snd.at[ph], recv_sem=rcv.at[ph],
                                     device_id={'ws': peer_of(off)}, device_id_type=MESH).start()

    def desc(buf, ph):
        return pltpu.make_async_remote_copy(src_ref=buf, dst_ref=buf, send_sem=snd.at[ph], recv_sem=rcv.at[ph],
                                            device_id={'ws': me}, device_id_type=MESH)

    def gather_start(buf, ph, row):
        for off in CHIP_OFFS:
            k = NEAR_FIRST.index(off)
            pltpu.make_async_remote_copy(src_ref=buf.at[me], dst_ref=buf.at[me], send_sem=snd.at[ph],
                                         recv_sem=direct.at[row, k], device_id={'ws': peer_of(off)},
                                         device_id_type=MESH).start()
        send(buf.at[me], buf.at[me], ph, SIBLING)

    def gather_finish(buf, ph, row):
        for k, (kz, ky, kc) in enumerate(NEAR_FIRST):
            src = peer_of((4 - kz, ky, 0))
            pltpu.make_async_remote_copy(src_ref=buf.at[src], dst_ref=buf.at[src], send_sem=snd.at[ph],
                                         recv_sem=direct.at[row, k], device_id={'ws': me},
                                         device_id_type=MESH).wait_recv()
            send(buf.at[src], buf.at[src], ph, SIBLING)
        desc(buf.at[pl.ds(0, 8)], ph).wait_recv()

    def weight_start(w, ph):
        for off in Z_OFFS:
            send(w.at[z, dpi], w.at[z, dpi], ph, off)

    def weight_pass(w, ph):
        desc(w.at[pl.ds(0, 3), 0], ph).wait_recv()
        for kz in (1, 2, 3):
            src = (z + kz) % 4
            pltpu.make_async_remote_copy(src_ref=w.at[src, dpi], dst_ref=w.at[src, dpi], send_sem=snd.at[ph + 11],
                                         recv_sem=rcv.at[ph + 11], device_id={'dp': 1 - dpi, 'ws': me},
                                         device_id_type=MESH).start()

    def weight_finish(w, ph):
        desc(w.at[pl.ds(0, 3), 0], ph + 11).wait_recv()

    bar = pltpu.get_barrier_semaphore()
    pl.semaphore_signal(bar, inc=1, device_id={'dp': 1 - dpi, 'ws': me}, device_id_type=MESH)
    for off in ALL_OFFS:
        pl.semaphore_signal(bar, inc=1, device_id={'ws': peer_of(off)}, device_id_type=MESH)

    loads = {}

    def load(name, src, dst):
        cp = pltpu.make_async_copy(src, dst, ld.at[len(loads)])
        cp.start()
        loads[name] = cp

    load('hid', hid, m1.at[me])
    load('wq', wq, wqkv.at[pl.ds(0, CB)])
    load('wk', wk, wqkv.at[pl.ds(CB, CB)])
    load('wv', wv, wqkv.at[pl.ds(2 * CB, CB)])
    load('ln1', ln1, ln1_v)
    load('ln2', ln2, ln2_v)
    load('ln3', ln3, ln3_v)
    load('rel', rel, rel_v)
    load('mask', mask, mask_v)
    load('wr', wr, rw.at[me])
    load('wo0', wo.at[pl.ds(0, CB // 2)], wgo.at[z, 0])
    load('wo1', wo.at[pl.ds(CB // 2, CB // 2)], wgo.at[z, 1])
    load('wqc0', wqc.at[pl.ds(0, CB // 2)], wgq.at[z, 0])
    load('wqc1', wqc.at[pl.ds(CB // 2, CB // 2)], wgq.at[z, 1])
    load('woc0', woc.at[pl.ds(0, CB // 2)], wgc.at[z, 0])
    load('woc1', woc.at[pl.ds(CB // 2, CB // 2)], wgc.at[z, 1])

    row8 = iota((ROWS, 128), 0)
    idx_own = jnp.zeros((ROWS, 128), jnp.int32)
    for i in range(ROWS):
        idx_own = jnp.where(row8 == i, idx_s[i], idx_own)
    idx_own = idx_own.astype(F32)
    ix[me] = idx_own.astype(BF16)
    wqkv[3 * CB:256, :] = jnp.zeros((256 - 3 * CB, D), BF16)
    loads['hid'].wait()
    pl.semaphore_wait(bar, NDEV)

    gather_start(m1, 0, 0)
    loads['wo0'].wait()
    loads['wo1'].wait()
    weight_start(wgo, 8)
    load('k', kT, k_v)
    load('v', vT, v_v)

    loads['rel'].wait()
    loads['mask'].wait()
    rel_f = rel_v[...]
    rel_hi = rel_f.astype(BF16)
    rem = rel_f - rel_hi.astype(F32)
    rel_mid = rem.astype(BF16)
    rel_lo = (rem - rel_mid.astype(F32)).astype(BF16)
    src_i = iota((LS, LS), 0)
    dst_i = iota((LS, LS), 1)
    lane12 = iota((HEADS, LS), 1)
    bias_s[...] = jnp.zeros((ROWS, HPAD, LS), F32)
    for b in range(ROWS):
        pick = jnp.where(src_i + dst_i == pos_s[b], 1.0, 0.0).astype(BF16)
        bb = jnp.dot(rel_hi, pick, preferred_element_type=F32)
        bb = bb + jnp.dot(rel_mid, pick, preferred_element_type=F32)
        bb = bb + jnp.dot(rel_lo, pick, preferred_element_type=F32)
        bias_s[b, 0:HEADS, :] = jnp.where(lane12 <= pos_s[b], bb, NEG)
    for name in ('wq', 'wk', 'wv', 'ln1', 'ln2', 'ln3', 'wr', 'wqc0', 'wqc1', 'woc0', 'woc1'):
        loads[name].wait()

    gather_finish(m1, 0, 0)
    hall = m1[...].astype(F32).reshape(NDEV * ROWS, D)
    xn = rms(hall, ln1_v[...].reshape(1, D))
    st2[...] = dot_nt(xn, wqkv[...]).reshape(NDEV, ROWS, 256).astype(BF16)
    r2[me] = st2[me]
    for off in ALL_OFFS:
        send(st2.at[peer_of(off)], r2.at[me], 1, off)
    weight_start(wgq, 9)
    weight_start(wgc, 10)
    for off in ALL_OFFS:
        send(ix.at[me], ix.at[me], 12, off)
        send(rw.at[me], rw.at[me], 11, off)
    load('ck', ckT, ck_v)
    load('cv', cvT, cv_v)

    sel_r = iota((4 * CB, D), 0)
    sel_q = ((sel_r >= CB).astype(jnp.int32) + (sel_r >= 2 * CB).astype(jnp.int32)
             + (sel_r >= 3 * CB).astype(jnp.int32))
    sel = (iota((4 * CB, D), 1) == sel_r + sel_q * (4 * CB - CB) + s * CB)
    sel = jnp.where(sel, 1.0, 0.0).astype(BF16)
    h_sub = m1[pl.ds(4 * z, 4)].astype(F32).reshape(4 * ROWS, D).astype(BF16)
    h_blk = dot_nt(h_sub, sel)

    loads['k'].wait()
    loads['v'].wait()
    desc(r2.at[pl.ds(0, NDEV - 1)], 1).wait_recv()
    weight_pass(wgo, 8)
    rv = r2[...].astype(F32)

    def columns(lo):
        return jnp.concatenate([rv[d, :, lo:lo + CB] for d in range(NDEV)], axis=-1)

    q8 = columns(0)
    k_cols = columns(CB).T
    v_cols = columns(2 * CB).T
    lane_s = iota((D, LS), 1)
    for b in range(ROWS):
        hit = lane_s == pos_s[b]
        k_v[b] = jnp.where(hit, jnp.broadcast_to(k_cols[:, b:b + 1], (D, LS)), k_v[b].astype(F32)).astype(BF16)
        v_v[b] = jnp.where(hit, jnp.broadcast_to(v_cols[:, b:b + 1], (D, LS)), v_v[b].astype(F32)).astype(BF16)
    attention(q8, k_v, v_v, lambda b: bias_s[b], s_self, ctx_v)

    def subgroup(buf, ph):
        for off in SUB_OFFS:
            send(buf.at[s], buf.at[s], ph, off)

    def natural(pieces):
        return jnp.concatenate([pieces[t][:, q * CB:(q + 1) * CB] for q in range(4) for t in range(4)], axis=-1)

    def unpack(blk):
        tail = jnp.concatenate([blk[32:48, 0:64], blk[32:48, 64:128]], axis=0)
        return jnp.concatenate([blk[0:32, :], tail], axis=-1)

    c3[s] = ctx_v[...].astype(BF16)
    subgroup(c3, 2)
    weight_pass(wgq, 9)
    load('win', win, win_v)
    load('wout', wout, wout_v)
    desc(c3.at[pl.ds(0, 3)], 2).wait_recv()
    weight_finish(wgo, 8)
    ctx = c3[...].astype(F32).reshape(4 * ROWS, D).astype(BF16)
    h1_blk = (h_blk + dot_nt(ctx, wgo[...].reshape(4 * CB, D))).astype(BF16)
    r4[s, :, 0:4 * CB] = h1_blk
    subgroup(r4, 3)
    desc(r4.at[pl.ds(0, 3)], 3).wait_recv()
    weight_finish(wgq, 9)
    r4f = r4[...].astype(F32)
    h1 = natural([r4f[t] for t in range(4)])
    x2 = rms(h1, ln2_v[...].reshape(1, D))
    st5[:, :, 0:4 * CB] = dot_nt(x2, wgq[...].reshape(4 * CB, D)).reshape(4, ROWS, 4 * CB).astype(BF16)
    r5[s] = st5[s]
    for off in SUB_OFFS:
        kz, ky, kc = off
        send(st5.at[((y + ky) % 2) * 2 + (c + kc) % 2], r5.at[s], 4, off)
    weight_pass(wgc, 10)
    loads['ck'].wait()
    loads['cv'].wait()
    desc(r5.at[pl.ds(0, 3)], 4).wait_recv()
    r5f = r5[...].astype(F32)
    q2 = natural([r5f[t] for t in range(4)])
    attention(q2, ck_v, cv_v, lambda b: jnp.where(mask_v[b:b + 1, :] == 1, 0.0, NEG), s_cross, ctx_v)

    c6[s] = ctx_v[...].astype(BF16)
    subgroup(c6, 5)
    desc(c6.at[pl.ds(0, 3)], 5).wait_recv()
    weight_finish(wgc, 10)
    ctx2 = c6[...].astype(F32).reshape(4 * ROWS, D).astype(BF16)
    h2_blk = (h1_blk.astype(F32) + dot_nt(ctx2, wgc[...].reshape(4 * CB, D))).astype(BF16)
    h2_f = h2_blk.astype(F32)
    r7[me, 0:32, :] = h2_f[:, 0:128].astype(BF16)
    r7[me, 32:48, :] = jnp.concatenate([h2_f[0:16, 128:192], h2_f[16:32, 128:192]], axis=-1).astype(BF16)
    gather_start(r7, 6, 1)
    desc(ix.at[pl.ds(0, NDEV - 1)], 12).wait_recv()
    idx_all = ix[...].astype(F32).reshape(NDEV * ROWS, 128)
    idx_t = idx_all.T
    earlier = (idx_t[0:ROWS, :] == idx_own) & (iota((ROWS, 128), 1) < me * ROWS + row8)
    slot = jnp.sum(jnp.where(earlier, 1.0, 0.0), axis=-1, keepdims=True)
    loads['win'].wait()
    loads['wout'].wait()
    gather_finish(r7, 6, 1)
    for t in range(4):
        h2g = natural([unpack(r7[4 * t + u].astype(F32)) for u in range(4)])
        h2_v[32 * t:32 * t + 32, :] = h2g
        x3_v[32 * t:32 * t + 32, :] = rms(h2g, ln3_v[...].reshape(1, D)).astype(F32)
    x3 = x3_v[...].astype(BF16)
    idx3 = jnp.concatenate([idx_all, idx_all, idx_all], axis=-1)
    half = (iota((NDEV * ROWS, 384), 1) >= 192).astype(F32)
    for p in range(8):
        hh = dot_nt(x3, win_v[2 * p:2 * p + 2].reshape(384, D))
        u_v[:, 384 * p:384 * p + 384] = jnp.where(idx3 == half + float(2 * p), jnp.maximum(hh, 0.0), 0.0).astype(BF16)
    chip = me // 2

    def partial(n):
        yn = jnp.dot(u_v[...], wout_v[:, :, 256 * n:256 * n + 256].reshape(NDEV * 192, 256),
                     preferred_element_type=F32).reshape(8, 2, ROWS, 256)
        st8[n, 0] = yn[:, 0]
        st8[n, 1] = yn[:, 1]
        send(st8.at[n, 1 - c], r8.at[n], 13 + n, SIBLING)

    def reduce_send(n):
        desc(r8.at[n], 13 + n).wait_recv()
        st9[n] = st8[n, c] + r8[n]
        for off in CHIP_OFFS:
            send(st9.at[n, peer_of(off) // 2], r9.at[n, chip], 16 + n, off)
        r9[n, chip] = st9[n, chip]

    partial(0)
    partial(1)
    reduce_send(0)
    partial(2)
    reduce_send(1)
    reduce_send(2)

    desc(rw.at[pl.ds(0, NDEV - 1)], 11).wait_recv()
    x3_own = x3_v[pl.ds(pl.multiple_of(me * ROWS, ROWS), ROWS), :]
    h2_own = h2_v[pl.ds(pl.multiple_of(me * ROWS, ROWS), ROWS), :]
    logits = dot_nt(x3_own, rw[...].reshape(NDEV, D), precision=lax.Precision.HIGHEST)
    ex = jnp.exp(logits - jnp.max(logits, axis=-1, keepdims=True))
    probs = ex / jnp.sum(ex, axis=-1, keepdims=True)
    mine = iota((ROWS, NDEV), 1).astype(F32) == idx_own[:, 0:NDEV]
    gate = jnp.sum(jnp.where(mine, probs, 0.0), axis=-1, keepdims=True)
    gate = jnp.where(slot < float(NDEV), gate, 0.0)

    for n in range(3):
        desc(r9.at[n, pl.ds(0, 7)], 16 + n).wait_recv()
    yv = jnp.concatenate([jnp.sum(r9[n], axis=0) for n in range(3)], axis=-1).astype(BF16).astype(F32)
    out_h[...] = (h2_own + yv * gate).astype(BF16)

    for buf, ph in ((m1, 0), (st2, 1), (r7, 6), (rw, 11), (ix, 12)):
        desc(buf.at[pl.ds(0, NDEV - 1)], ph).wait_send()
    for n in range(3):
        desc(st9.at[n, pl.ds(0, 7)], 16 + n).wait_send()
        desc(r8.at[n], 13 + n).wait_send()
    for buf, ph in ((c3, 2), (r4, 3), (st5, 4), (c6, 5)):
        desc(buf.at[pl.ds(0, 3)], ph).wait_send()
    for w, ph in ((wgo, 8), (wgq, 9), (wgc, 10)):
        desc(w.at[pl.ds(0, 3), 0], ph).wait_send()
        desc(w.at[pl.ds(0, 3), 0], ph + 11).wait_send()


def store(h_in, k_in, v_in, h_out, k_out, v_out, sem):
    copies = [pltpu.make_async_copy(src, dst, sem.at[i])
              for i, (src, dst) in enumerate(((k_in, k_out), (v_in, v_out), (h_in, h_out)))]
    for cp in copies:
        cp.start()
    for cp in copies:
        cp.wait()


def solution(mesh):
    rows = ('dp', 'ws')
    row_vec = P(rows)
    row_mat = P(rows, None)
    cache = P(rows, None, None, None)
    col = P(None, 'ws')
    in_specs = (row_mat, cache, cache, cache, cache, row_vec, row_mat, P(None, None), row_vec,
                P(None), P(None), P(None), col, col, col, col, col, col,
                col, P(None, None, 'ws'), P(None, 'ws', None))
    out_specs = (row_mat, cache, cache)

    any_spec = pl.BlockSpec(memory_space=pltpu.HBM)
    smem = pl.BlockSpec(memory_space=pltpu.SMEM)
    vmem = pl.BlockSpec(memory_space=pltpu.VMEM)

    def block(hidden, self_k, self_v, cross_k, cross_v, positions, enc_mask, rel_bias, expert_idx,
              ln_self, ln_cross, ln_ffn, wq_self, wk_self, wv_self, wo_self, wq_cross, wo_cross,
              w_router, w_in, w_out):
        def flat(cache_arr):
            return jnp.swapaxes(cache_arr, 2, 3).reshape(ROWS, D, cache_arr.shape[2])

        def unflat(arr):
            return jnp.swapaxes(arr.reshape(ROWS, HEADS, 64, LS), 2, 3)

        args = (hidden, flat(self_k), flat(self_v), flat(cross_k), flat(cross_v), positions, enc_mask, rel_bias,
                expert_idx, ln_self, ln_cross, ln_ffn,
                wq_self.T, wk_self.T, wv_self.T, wo_self.T, wq_cross.T, wo_cross.T, w_router.T,
                jnp.swapaxes(w_in, 1, 2), w_out)
        specs = [any_spec] * len(args)
        specs[5] = smem
        specs[8] = smem
        V = pltpu.VMEM
        scratch = [
            V((ROWS, D, LC), BF16), V((ROWS, D, LC), BF16), V((NDEV, 192, D), BF16), V((NDEV, 192, D), BF16),
            V((ROWS, LC), jnp.int32), V((HEADS, LS), F32), V((D,), F32), V((D,), F32), V((D,), F32), V((256, D), BF16),
            V((NDEV, ROWS, D), BF16), V((NDEV, ROWS, 128), BF16), V((NDEV, ROWS, 256), BF16), V((NDEV, ROWS, 256), BF16),
            V((4, 2, CB // 2, D), BF16), V((4, 2, CB // 2, D), BF16), V((4, 2, CB // 2, D), BF16), V((NDEV, 1, D), F32),
            V((4, ROWS, D), BF16), V((4, 4 * ROWS, 256), BF16), V((4, ROWS, 256), BF16), V((4, ROWS, 256), BF16),
            V((4, ROWS, D), BF16), V((NDEV, CB, 128), BF16), V((3, 2, 8, ROWS, 256), F32), V((3, 8, ROWS, 256), F32),
            V((3, 8, ROWS, 256), F32), V((3, 8, ROWS, 256), F32),
            V((ROWS, HPAD, LS), F32), V((ROWS, HPAD, LS), F32), V((ROWS, HPAD, LC), F32), V((ROWS, D), F32),
            V((NDEV * ROWS, D), F32), V((NDEV * ROWS, D), F32), V((NDEV * ROWS, NDEV * 192), BF16),
            pltpu.SemaphoreType.DMA((22,)), pltpu.SemaphoreType.DMA((22,)), pltpu.SemaphoreType.DMA((22,)),
            pltpu.SemaphoreType.DMA((2, 7)),
        ]
        h_out, k_out, v_out = pl.pallas_call(
            kernel,
            out_shape=(V((ROWS, D), BF16), V((ROWS, D, LS), BF16), V((ROWS, D, LS), BF16)),
            in_specs=specs,
            out_specs=(vmem, vmem, vmem),
            scratch_shapes=scratch,
            compiler_params=pltpu.CompilerParams(collective_id=0, has_side_effects=True,
                                                 vmem_limit_bytes=67043328 - 2 * 3145728 - 16384),
        )(*args)
        outs = (jax.ShapeDtypeStruct((ROWS, D), BF16), jax.ShapeDtypeStruct((ROWS, D, LS), BF16),
                jax.ShapeDtypeStruct((ROWS, D, LS), BF16))
        h_out, k_out, v_out = pl.pallas_call(
            store, out_shape=outs, in_specs=[vmem] * 3, out_specs=(any_spec,) * 3,
            scratch_shapes=[pltpu.SemaphoreType.DMA((3,))],
            compiler_params=pltpu.CompilerParams(vmem_limit_bytes=4 * 1024 * 1024),
        )(h_out, k_out, v_out)
        return h_out, unflat(k_out), unflat(v_out)

    return jax.shard_map(block, mesh=mesh, in_specs=in_specs, out_specs=out_specs, check_vma=False)
```

```python
import jax
import jax.numpy as jnp
from jax import lax
from jax.experimental import pallas as pl
from jax.experimental.pallas import tpu as pltpu
from jax.sharding import PartitionSpec as P

EPS = 1e-6
NEG = -1e30
F32 = jnp.float32
BF16 = jnp.bfloat16
MESH = pl.DeviceIdType.MESH

ROWS = 8
D = 768
HEADS = 12
HPAD = 16
LS = 192
LC = 384
NDEV = 16
CB = 48
NT = (((1,), (1,)), ((), ()))

ALL_OFFS = [(kz, ky, kc) for kz in (2, 3, 1, 0) for ky in (1, 0) for kc in (1, 0) if (kz, ky, kc) != (0, 0, 0)]
CHIP_OFFS = [off for off in ALL_OFFS if off[2] == 0]
NEAR_FIRST = [(0, 1, 0), (1, 0, 0), (3, 0, 0), (1, 1, 0), (3, 1, 0), (2, 0, 0), (2, 1, 0)]
SIBLING = (0, 0, 1)
SUB_OFFS = [(0, 1, 1), (0, 1, 0), (0, 0, 1)]
Z_OFFS = [(2, 0, 0), (3, 0, 0), (1, 0, 0)]


def dot_nt(a, b, **kw):
    return lax.dot_general(a, b, NT, preferred_element_type=F32, **kw)


def iota(shape, axis):
    return lax.broadcasted_iota(jnp.int32, shape, axis)


def rms(x, g):
    inv = lax.rsqrt(jnp.mean(x * x, axis=-1, keepdims=True) + EPS)
    return (x * inv * g).astype(BF16)


def head_mask():
    row = iota((HPAD, D), 0) * 64
    col = iota((HPAD, D), 1)
    return (col >= row) & (col < row + 64)


def attention(q8, k_ref, v_ref, bias_of, s_ref, ctx_ref, q_ref, patch=None):
    hm = head_mask()
    for b in range(ROWS):
        qb = jnp.where(hm, jnp.broadcast_to(q8[b:b + 1, :], (HPAD, D)), 0.0).astype(BF16)
        q_ref[b] = qb
    if patch is not None:
        k8, v8, hit_of = patch
        new = dot_nt(q_ref[...].reshape(ROWS * HPAD, D), k8.astype(BF16))
        row = iota((ROWS * HPAD, ROWS), 0)
        col = iota((ROWS * HPAD, ROWS), 1) * HPAD
        new = jnp.sum(jnp.where((row >= col) & (row < col + HPAD), new, 0.0), axis=-1, keepdims=True)
    for b in range(ROWS):
        sb = jnp.dot(q_ref[b], k_ref[b], preferred_element_type=F32)
        if patch is not None:
            sb = jnp.where(hit_of(b), new[b * HPAD:(b + 1) * HPAD], sb)
        s_ref[b] = sb + bias_of(b)
    s = s_ref[...]
    p = jnp.exp(s - jnp.max(s, axis=-1, keepdims=True))
    s_ref[...] = p / jnp.sum(p, axis=-1, keepdims=True)
    for b in range(ROWS):
        pb = s_ref[b].astype(BF16)
        if patch is None:
            cb = dot_nt(pb, v_ref[b])
        else:
            pf = pb.astype(F32)
            hit = hit_of(b)
            at_pos = jnp.sum(jnp.where(hit, pf, 0.0), axis=-1, keepdims=True)
            cb = dot_nt(jnp.where(hit, 0.0, pf).astype(BF16), v_ref[b]) + at_pos * v8[b:b + 1, :]
        ctx_ref[b:b + 1, :] = jnp.sum(jnp.where(hm, cb, 0.0), axis=0, keepdims=True)


def kernel(hid, kT, vT, ckT, cvT, pos, mask, rel, idx, ln1, ln2, ln3, wq, wk, wv, wo, wqc, woc, wr, win, wout,
           out_h, k_v, v_v,
           ck_v, cv_v, win_v, wout_v, mask_v, rel_v, ln1_v, ln2_v, ln3_v, wqkv, m1, ix, st2, r2, wgo, wgq, wgc, rw,
           c3, r4, st5, r5, c6, r7, st8, r8, st9, r9, bias_s, s_self, s_cross, ctx_v, h2_v, x3_v, u_v,
           k_old, v_old, hs, q_v, pos_s, idx_s, ld, snd, rcv, direct, fwd):
    me = lax.axis_index('ws')
    dpi = lax.axis_index('dp')
    z = me // 4
    s = me % 4
    y = s // 2
    c = s % 2

    def peer_of(off):
        kz, ky, kc = off
        return ((z + kz) % 4) * 4 + ((y + ky) % 2) * 2 + (c + kc) % 2

    def send(src, dst, ph, off):
        pltpu.make_async_remote_copy(src_ref=src, dst_ref=dst, send_sem=snd.at[ph], recv_sem=rcv.at[ph],
                                     device_id={'ws': peer_of(off)}, device_id_type=MESH).start()

    def desc(buf, ph):
        return pltpu.make_async_remote_copy(src_ref=buf, dst_ref=buf, send_sem=snd.at[ph], recv_sem=rcv.at[ph],
                                            device_id={'ws': me}, device_id_type=MESH)

    def gather_start(buf, ph, row):
        for off in CHIP_OFFS:
            k = NEAR_FIRST.index(off)
            pltpu.make_async_remote_copy(src_ref=buf.at[me], dst_ref=buf.at[me], send_sem=snd.at[ph],
                                         recv_sem=direct.at[row, k], device_id={'ws': peer_of(off)},
                                         device_id_type=MESH).start()

    def gather_finish(buf, ph, row):
        for k, (kz, ky, kc) in enumerate(NEAR_FIRST):
            src = peer_of((4 - kz, ky, 0))
            pltpu.make_async_remote_copy(src_ref=buf.at[src], dst_ref=buf.at[src], send_sem=snd.at[ph],
                                         recv_sem=direct.at[row, k], device_id={'ws': me},
                                         device_id_type=MESH).wait_recv()
            send(buf.at[src], buf.at[src], ph, SIBLING)
        desc(buf.at[pl.ds(0, 8)], ph).wait_recv()

    def subgroup(buf, ph):
        for off in SUB_OFFS:
            send(buf.at[s], buf.at[s], ph, off)

    def weight_start(w, ph):
        for off in Z_OFFS:
            send(w.at[z, dpi], w.at[z, dpi], ph, off)

    def weight_pass(w, ph):
        desc(w.at[pl.ds(0, 3), 0], ph).wait_recv()
        for kz in (1, 2, 3):
            src = (z + kz) % 4
            pltpu.make_async_remote_copy(src_ref=w.at[src, dpi], dst_ref=w.at[src, dpi], send_sem=snd.at[ph + 11],
                                         recv_sem=rcv.at[ph + 11], device_id={'dp': 1 - dpi, 'ws': me},
                                         device_id_type=MESH).start()

    def weight_finish(w, ph):
        desc(w.at[pl.ds(0, 3), 0], ph + 11).wait_recv()

    bar = pltpu.get_barrier_semaphore()
    pl.semaphore_signal(bar, inc=1, device_id={'dp': 1 - dpi, 'ws': me}, device_id_type=MESH)
    for off in ALL_OFFS:
        pl.semaphore_signal(bar, inc=1, device_id={'ws': peer_of(off)}, device_id_type=MESH)

    loads = {}

    def load(name, src, dst):
        cp = pltpu.make_async_copy(src, dst, ld.at[len(loads)])
        cp.start()
        loads[name] = cp

    load('hid', hid, hs.at[s])
    load('ln1', ln1, ln1_v)
    load('pos', pos, pos_s)
    load('idx', idx, idx_s)
    load('wq', wq, wqkv.at[pl.ds(0, CB)])
    load('wk', wk, wqkv.at[pl.ds(CB, CB)])
    load('wv', wv, wqkv.at[pl.ds(2 * CB, CB)])
    load('ln2', ln2, ln2_v)
    load('ln3', ln3, ln3_v)
    load('rel', rel, rel_v)
    load('mask', mask, mask_v)
    load('wr', wr, rw.at[me])
    load('wo0', wo.at[pl.ds(0, CB // 2)], wgo.at[z, 0])
    load('wo1', wo.at[pl.ds(CB // 2, CB // 2)], wgo.at[z, 1])
    load('wqc0', wqc.at[pl.ds(0, CB // 2)], wgq.at[z, 0])
    load('wqc1', wqc.at[pl.ds(CB // 2, CB // 2)], wgq.at[z, 1])
    load('woc0', woc.at[pl.ds(0, CB // 2)], wgc.at[z, 0])
    load('woc1', woc.at[pl.ds(CB // 2, CB // 2)], wgc.at[z, 1])

    wqkv[3 * CB:256, :] = jnp.zeros((256 - 3 * CB, D), BF16)
    loads['hid'].wait()
    loads['ln1'].wait()
    m1[me] = rms(hs[s].astype(F32), ln1_v[...].reshape(1, D))
    pl.semaphore_wait(bar, NDEV)

    gather_start(m1, 0, 0)
    send(m1.at[me], m1.at[me], 0, SIBLING)
    loads['wo0'].wait()
    loads['wo1'].wait()
    weight_start(wgo, 8)
    subgroup(hs, 7)
    load('k', kT, k_old)
    load('v', vT, v_old)
    loads['pos'].wait()
    loads['idx'].wait()
    row8 = iota((ROWS, 128), 0)
    idx_own = jnp.zeros((ROWS, 128), jnp.int32)
    for i in range(ROWS):
        idx_own = jnp.where(row8 == i, idx_s[i], idx_own)
    idx_own = idx_own.astype(F32)
    ix[me] = idx_own.astype(BF16)

    loads['rel'].wait()
    loads['mask'].wait()
    rel_f = rel_v[...]
    rel_hi = rel_f.astype(BF16)
    rem = rel_f - rel_hi.astype(F32)
    rel_mid = rem.astype(BF16)
    rel_lo = (rem - rel_mid.astype(F32)).astype(BF16)
    src_i = iota((LS, LS), 0)
    dst_i = iota((LS, LS), 1)
    lane12 = iota((HEADS, LS), 1)
    bias_s[...] = jnp.zeros((ROWS, HPAD, LS), F32)
    for b in range(ROWS):
        pick = jnp.where(src_i + dst_i == pos_s[b], 1.0, 0.0).astype(BF16)
        bb = jnp.dot(rel_hi, pick, preferred_element_type=F32)
        bb = bb + jnp.dot(rel_mid, pick, preferred_element_type=F32)
        bb = bb + jnp.dot(rel_lo, pick, preferred_element_type=F32)
        bias_s[b, 0:HEADS, :] = jnp.where(lane12 <= pos_s[b], bb, NEG)
    for name in ('wq', 'wk', 'wv', 'ln2', 'ln3', 'wr', 'wqc0', 'wqc1', 'woc0', 'woc1'):
        loads[name].wait()

    gather_finish(m1, 0, 0)
    xn = m1[...].astype(F32).reshape(NDEV * ROWS, D).astype(BF16)
    st2[...] = dot_nt(xn, wqkv[...]).reshape(NDEV, ROWS, 256).astype(BF16)
    r2[me] = st2[me]
    for off in ALL_OFFS:
        send(st2.at[peer_of(off)], r2.at[me], 1, off)
    weight_start(wgq, 9)
    weight_start(wgc, 10)
    for off in ALL_OFFS:
        send(ix.at[me], ix.at[me], 12, off)
        send(rw.at[me], rw.at[me], 11, off)
    load('ck', ckT, ck_v)
    load('cv', cvT, cv_v)

    sel_r = iota((4 * CB, D), 0)
    sel_q = ((sel_r >= CB).astype(jnp.int32) + (sel_r >= 2 * CB).astype(jnp.int32)
             + (sel_r >= 3 * CB).astype(jnp.int32))
    sel = (iota((4 * CB, D), 1) == sel_r + sel_q * (4 * CB - CB) + s * CB)
    sel = jnp.where(sel, 1.0, 0.0).astype(BF16)
    desc(hs.at[pl.ds(0, 3)], 7).wait_recv()
    h_sub = hs[...].astype(F32).reshape(4 * ROWS, D).astype(BF16)
    h_blk = dot_nt(h_sub, sel)

    loads['k'].wait()
    loads['v'].wait()
    desc(r2.at[pl.ds(0, NDEV - 1)], 1).wait_recv()
    weight_pass(wgo, 8)
    rv = r2[...].astype(F32)

    def columns(lo):
        return jnp.concatenate([rv[d, :, lo:lo + CB] for d in range(NDEV)], axis=-1)

    q8 = columns(0)
    k8 = columns(CB)
    v8 = columns(2 * CB)
    lane_h = iota((HPAD, LS), 1)
    attention(q8, k_old, v_old, lambda b: bias_s[b], s_self, ctx_v, q_v,
              (k8, v8, lambda b: lane_h == pos_s[b]))

    def update(new, old, out):
        cols = new.T
        lane_s = iota((D, LS), 1)
        for b in range(ROWS):
            out[b] = jnp.where(lane_s == pos_s[b], jnp.broadcast_to(cols[:, b:b + 1], (D, LS)),
                               old[b].astype(F32)).astype(BF16)

    def natural(pieces):
        return jnp.concatenate([pieces[t][:, q * CB:(q + 1) * CB] for q in range(4) for t in range(4)], axis=-1)

    def unpack(blk):
        tail = jnp.concatenate([blk[32:48, 0:64], blk[32:48, 64:128]], axis=0)
        return jnp.concatenate([blk[0:32, :], tail], axis=-1)

    c3[s] = ctx_v[...].astype(BF16)
    subgroup(c3, 2)
    update(k8, k_old, k_v)
    weight_pass(wgq, 9)
    update(v8, v_old, v_v)
    load('win', win, win_v)
    load('wout', wout, wout_v)
    desc(c3.at[pl.ds(0, 3)], 2).wait_recv()
    weight_finish(wgo, 8)
    ctx = c3[...].astype(F32).reshape(4 * ROWS, D).astype(BF16)
    h1_blk = (h_blk + dot_nt(ctx, wgo[...].reshape(4 * CB, D))).astype(BF16)
    r4[s, :, 0:4 * CB] = h1_blk
    subgroup(r4, 3)
    desc(r4.at[pl.ds(0, 3)], 3).wait_recv()
    weight_finish(wgq, 9)
    r4f = r4[...].astype(F32)
    h1 = natural([r4f[t] for t in range(4)])
    x2 = rms(h1, ln2_v[...].reshape(1, D))
    st5[:, :, 0:4 * CB] = dot_nt(x2, wgq[...].reshape(4 * CB, D)).reshape(4, ROWS, 4 * CB).astype(BF16)
    r5[s] = st5[s]
    for off in SUB_OFFS:
        kz, ky, kc = off
        send(st5.at[((y + ky) % 2) * 2 + (c + kc) % 2], r5.at[s], 4, off)
    weight_pass(wgc, 10)
    loads['ck'].wait()
    loads['cv'].wait()
    desc(r5.at[pl.ds(0, 3)], 4).wait_recv()
    r5f = r5[...].astype(F32)
    q2 = natural([r5f[t] for t in range(4)])
    attention(q2, ck_v, cv_v, lambda b: jnp.where(mask_v[b:b + 1, :] == 1, 0.0, NEG), s_cross, ctx_v, q_v)

    c6[s] = ctx_v[...].astype(BF16)
    subgroup(c6, 5)
    desc(c6.at[pl.ds(0, 3)], 5).wait_recv()
    weight_finish(wgc, 10)
    ctx2 = c6[...].astype(F32).reshape(4 * ROWS, D).astype(BF16)
    h2_blk = (h1_blk.astype(F32) + dot_nt(ctx2, wgc[...].reshape(4 * CB, D))).astype(BF16)
    h2_f = h2_blk.astype(F32)
    r7[me, 0:32, :] = h2_f[:, 0:128].astype(BF16)
    r7[me, 32:48, :] = jnp.concatenate([h2_f[0:16, 128:192], h2_f[16:32, 128:192]], axis=-1).astype(BF16)

    def one(buf, sem):
        return pltpu.make_async_remote_copy(src_ref=buf, dst_ref=buf, send_sem=snd.at[6], recv_sem=sem,
                                            device_id={'ws': me}, device_id_type=MESH)

    def pass_on(src, k):
        pltpu.make_async_remote_copy(src_ref=r7.at[src], dst_ref=r7.at[src], send_sem=snd.at[6], recv_sem=fwd.at[k],
                                     device_id={'ws': peer_of(SIBLING)}, device_id_type=MESH).start()

    gather_start(r7, 6, 1)
    pass_on(me, 7)
    desc(ix.at[pl.ds(0, NDEV - 1)], 12).wait_recv()
    idx_all = ix[...].astype(F32).reshape(NDEV * ROWS, 128)
    idx_t = idx_all.T
    earlier = (idx_t[0:ROWS, :] == idx_own) & (iota((ROWS, 128), 1) < me * ROWS + row8)
    slot = jnp.sum(jnp.where(earlier, 1.0, 0.0), axis=-1, keepdims=True)
    loads['win'].wait()
    loads['wout'].wait()

    def arrive(k):
        kz, ky, kc = NEAR_FIRST[k]
        src = peer_of((4 - kz, ky, 0))
        one(r7.at[src], direct.at[1, k]).wait_recv()
        pass_on(src, k)

    def group(kz, parts):
        for k in parts:
            one(r7.at[0], fwd.at[k]).wait_recv()
        t = (z + 4 - kz) % 4
        h2g = natural([unpack(r7[4 * t + u].astype(F32)) for u in range(4)])
        at = pl.ds(pl.multiple_of(32 * t, 32), 32)
        h2_v[at, :] = h2g
        x3_v[at, :] = rms(h2g, ln3_v[...].reshape(1, D))

    for k in range(5):
        arrive(k)
    group(0, (7, 0))
    arrive(5)
    arrive(6)
    group(1, (1, 3))
    group(3, (2, 4))
    group(2, (5, 6))
    x3 = x3_v[...]
    idx3 = jnp.concatenate([idx_all, idx_all, idx_all], axis=-1)
    half = (iota((NDEV * ROWS, 384), 1) >= 192).astype(F32)
    for p in range(8):
        hh = dot_nt(x3, win_v[2 * p:2 * p + 2].reshape(384, D))
        u_v[:, 384 * p:384 * p + 384] = jnp.where(idx3 == half + float(2 * p), jnp.maximum(hh, 0.0), 0.0).astype(BF16)
    chip = me // 2

    def partial(n):
        yn = jnp.dot(u_v[...], wout_v[:, :, 256 * n:256 * n + 256].reshape(NDEV * 192, 256),
                     preferred_element_type=F32).reshape(8, 2, ROWS, 256)
        st8[n, 0] = yn[:, 0]
        st8[n, 1] = yn[:, 1]
        send(st8.at[n, 1 - c], r8.at[n], 13 + n, SIBLING)

    def reduce_send(n):
        desc(r8.at[n], 13 + n).wait_recv()
        st9[n] = st8[n, c] + r8[n]
        for off in CHIP_OFFS:
            send(st9.at[n, peer_of(off) // 2], r9.at[n, chip], 16 + n, off)
        r9[n, chip] = st9[n, chip]

    partial(0)
    partial(1)
    partial(2)
    reduce_send(0)
    reduce_send(1)
    reduce_send(2)

    desc(rw.at[pl.ds(0, NDEV - 1)], 11).wait_recv()
    h2_own = h2_v[pl.ds(pl.multiple_of(me * ROWS, ROWS), ROWS), :]
    x3_own = rms(h2_own, ln3_v[...].reshape(1, D)).astype(F32)
    logits = dot_nt(x3_own, rw[...].reshape(NDEV, D), precision=lax.Precision.HIGHEST)
    ex = jnp.exp(logits - jnp.max(logits, axis=-1, keepdims=True))
    probs = ex / jnp.sum(ex, axis=-1, keepdims=True)
    mine = iota((ROWS, NDEV), 1).astype(F32) == idx_own[:, 0:NDEV]
    gate = jnp.sum(jnp.where(mine, probs, 0.0), axis=-1, keepdims=True)
    gate = jnp.where(slot < float(NDEV), gate, 0.0)

    for n in range(3):
        desc(r9.at[n, pl.ds(0, 7)], 16 + n).wait_recv()
    yv = jnp.concatenate([jnp.sum(r9[n], axis=0) for n in range(3)], axis=-1).astype(BF16).astype(F32)
    out_h[...] = (h2_own + yv * gate).astype(BF16)

    for buf, ph in ((m1, 0), (st2, 1), (r7, 6), (rw, 11), (ix, 12)):
        desc(buf.at[pl.ds(0, NDEV - 1)], ph).wait_send()
    for n in range(3):
        desc(st9.at[n, pl.ds(0, 7)], 16 + n).wait_send()
        desc(r8.at[n], 13 + n).wait_send()
    for buf, ph in ((c3, 2), (r4, 3), (st5, 4), (c6, 5), (hs, 7)):
        desc(buf.at[pl.ds(0, 3)], ph).wait_send()
    for w, ph in ((wgo, 8), (wgq, 9), (wgc, 10)):
        desc(w.at[pl.ds(0, 3), 0], ph).wait_send()
        desc(w.at[pl.ds(0, 3), 0], ph + 11).wait_send()


def store(h_in, k_in, v_in, h_out, k_out, v_out, sem):
    copies = [pltpu.make_async_copy(src, dst, sem.at[i])
              for i, (src, dst) in enumerate(((k_in, k_out), (v_in, v_out), (h_in, h_out)))]
    for cp in copies:
        cp.start()
    for cp in copies:
        cp.wait()


def solution(mesh):
    rows = ('dp', 'ws')
    row_vec = P(rows)
    row_mat = P(rows, None)
    cache = P(rows, None, None, None)
    col = P(None, 'ws')
    in_specs = (row_mat, cache, cache, cache, cache, row_vec, row_mat, P(None, None), row_vec,
                P(None), P(None), P(None), col, col, col, col, col, col,
                col, P(None, None, 'ws'), P(None, 'ws', None))
    out_specs = (row_mat, cache, cache)

    any_spec = pl.BlockSpec(memory_space=pltpu.HBM)
    vmem = pl.BlockSpec(memory_space=pltpu.VMEM)

    def block(hidden, self_k, self_v, cross_k, cross_v, positions, enc_mask, rel_bias, expert_idx,
              ln_self, ln_cross, ln_ffn, wq_self, wk_self, wv_self, wo_self, wq_cross, wo_cross,
              w_router, w_in, w_out):
        def flat(cache_arr):
            return jnp.swapaxes(cache_arr, 2, 3).reshape(ROWS, D, cache_arr.shape[2])

        def unflat(arr):
            return jnp.swapaxes(arr.reshape(ROWS, HEADS, 64, LS), 2, 3)

        args = (hidden, flat(self_k), flat(self_v), flat(cross_k), flat(cross_v), positions, enc_mask, rel_bias,
                expert_idx, ln_self, ln_cross, ln_ffn,
                wq_self.T, wk_self.T, wv_self.T, wo_self.T, wq_cross.T, wo_cross.T, w_router.T,
                jnp.swapaxes(w_in, 1, 2), w_out)
        specs = [any_spec] * len(args)
        V = pltpu.VMEM
        scratch = [
            V((ROWS, D, LC), BF16), V((ROWS, D, LC), BF16), V((NDEV, 192, D), BF16), V((NDEV, 192, D), BF16),
            V((ROWS, LC), jnp.int32), V((HEADS, LS), F32), V((D,), F32), V((D,), F32), V((D,), F32), V((256, D), BF16),
            V((NDEV, ROWS, D), BF16), V((NDEV, ROWS, 128), BF16), V((NDEV, ROWS, 256), BF16), V((NDEV, ROWS, 256), BF16),
            V((4, 2, CB // 2, D), BF16), V((4, 2, CB // 2, D), BF16), V((4, 2, CB // 2, D), BF16), V((NDEV, 1, D), F32),
            V((4, ROWS, D), BF16), V((4, 4 * ROWS, 256), BF16), V((4, ROWS, 256), BF16), V((4, ROWS, 256), BF16),
            V((4, ROWS, D), BF16), V((NDEV, CB, 128), BF16), V((3, 2, 8, ROWS, 256), F32), V((3, 8, ROWS, 256), F32),
            V((3, 8, ROWS, 256), F32), V((3, 8, ROWS, 256), F32),
            V((ROWS, HPAD, LS), F32), V((ROWS, HPAD, LS), F32), V((ROWS, HPAD, LC), F32), V((ROWS, D), F32),
            V((NDEV * ROWS, D), F32), V((NDEV * ROWS, D), BF16), V((NDEV * ROWS, NDEV * 192), BF16),
            V((ROWS, D, LS), BF16), V((ROWS, D, LS), BF16), V((4, ROWS, D), BF16), V((ROWS, HPAD, D), BF16),
            pltpu.SMEM((ROWS,), jnp.int32), pltpu.SMEM((ROWS,), jnp.int32),
            pltpu.SemaphoreType.DMA((24,)), pltpu.SemaphoreType.DMA((22,)), pltpu.SemaphoreType.DMA((22,)),
            pltpu.SemaphoreType.DMA((2, 7)), pltpu.SemaphoreType.DMA((8,)),
        ]
        h_out, k_out, v_out = pl.pallas_call(
            kernel,
            out_shape=(V((ROWS, D), BF16), V((ROWS, D, LS), BF16), V((ROWS, D, LS), BF16)),
            in_specs=specs,
            out_specs=(vmem, vmem, vmem),
            scratch_shapes=scratch,
            compiler_params=pltpu.CompilerParams(collective_id=0, has_side_effects=True,
                                                 vmem_limit_bytes=67043328 - 2 * 3145728 - 16384),
        )(*args)
        outs = (jax.ShapeDtypeStruct((ROWS, D), BF16), jax.ShapeDtypeStruct((ROWS, D, LS), BF16),
                jax.ShapeDtypeStruct((ROWS, D, LS), BF16))
        h_out, k_out, v_out = pl.pallas_call(
            store, out_shape=outs, in_specs=[vmem] * 3, out_specs=(any_spec,) * 3,
            scratch_shapes=[pltpu.SemaphoreType.DMA((3,))],
            compiler_params=pltpu.CompilerParams(vmem_limit_bytes=4 * 1024 * 1024),
        )(h_out, k_out, v_out)
        return h_out, unflat(k_out), unflat(v_out)

    return jax.shard_map(block, mesh=mesh, in_specs=in_specs, out_specs=out_specs, check_vma=False)
```

```python
import jax
import jax.numpy as jnp
from jax import lax
from jax.experimental import pallas as pl
from jax.experimental.pallas import tpu as pltpu
from jax.sharding import PartitionSpec as P

EPS = 1e-6
NEG = -1e30
F32 = jnp.float32
BF16 = jnp.bfloat16
MESH = pl.DeviceIdType.MESH

ROWS = 8
D = 768
HEADS = 12
HPAD = 16
LS = 192
LC = 384
NDEV = 16
CB = 48
NT = (((1,), (1,)), ((), ()))

ALL_OFFS = [(kz, ky, kc) for kz in (2, 3, 1, 0) for ky in (1, 0) for kc in (1, 0) if (kz, ky, kc) != (0, 0, 0)]
CHIP_OFFS = [off for off in ALL_OFFS if off[2] == 0]
SIBLING = (0, 0, 1)
SUB_OFFS = [(0, 1, 1), (0, 1, 0), (0, 0, 1)]
Z_OFFS = [(2, 0, 0), (3, 0, 0), (1, 0, 0)]


def dot_nt(a, b, **kw):
    return lax.dot_general(a, b, NT, preferred_element_type=F32, **kw)


def iota(shape, axis):
    return lax.broadcasted_iota(jnp.int32, shape, axis)


def rms(x, g):
    inv = lax.rsqrt(jnp.mean(x * x, axis=-1, keepdims=True) + EPS)
    return (x * inv * g).astype(BF16)


def head_mask():
    row = iota((HPAD, D), 0) * 64
    col = iota((HPAD, D), 1)
    return (col >= row) & (col < row + 64)


def attention(q8, k_ref, v_ref, bias_of, s_ref, ctx_ref, q_ref, patch=None):
    hm = head_mask()
    for b in range(ROWS):
        qb = jnp.where(hm, jnp.broadcast_to(q8[b:b + 1, :], (HPAD, D)), 0.0).astype(BF16)
        q_ref[b] = qb
    if patch is not None:
        k8, v8, hit_of = patch
        new = dot_nt(q_ref[...].reshape(ROWS * HPAD, D), k8.astype(BF16))
        row = iota((ROWS * HPAD, ROWS), 0)
        col = iota((ROWS * HPAD, ROWS), 1) * HPAD
        new = jnp.sum(jnp.where((row >= col) & (row < col + HPAD), new, 0.0), axis=-1, keepdims=True)
    for b in range(ROWS):
        sb = jnp.dot(q_ref[b], k_ref[b], preferred_element_type=F32)
        if patch is not None:
            sb = jnp.where(hit_of(b), new[b * HPAD:(b + 1) * HPAD], sb)
        s_ref[b] = sb + bias_of(b)
    s = s_ref[...]
    p = jnp.exp(s - jnp.max(s, axis=-1, keepdims=True))
    s_ref[...] = p / jnp.sum(p, axis=-1, keepdims=True)
    for b in range(ROWS):
        pb = s_ref[b].astype(BF16)
        if patch is None:
            cb = dot_nt(pb, v_ref[b])
        else:
            pf = pb.astype(F32)
            hit = hit_of(b)
            at_pos = jnp.sum(jnp.where(hit, pf, 0.0), axis=-1, keepdims=True)
            cb = dot_nt(jnp.where(hit, 0.0, pf).astype(BF16), v_ref[b]) + at_pos * v8[b:b + 1, :]
        ctx_ref[b:b + 1, :] = jnp.sum(jnp.where(hm, cb, 0.0), axis=0, keepdims=True)


def kernel(hid, kT, vT, ckT, cvT, pos, mask, rel, idx, ln1, ln2, ln3, wq, wk, wv, wo, wqc, woc, wr, win, wout,
           out_h, k_v, v_v,
           ck_v, cv_v, win_v, wout_v, mask_v, rel_v, ln1_v, ln2_v, ln3_v, wqkv, m1, ix, st2, r2, wgo, wgq, wgc, rw,
           c3, r4, st5, r5, c6, r7, st8, r8, st9, r9, bias_s, s_self, s_cross, ctx_v, h2_v, x3_v, u_v,
           k_old, v_old, hs, q_v, pos_s, idx_s, ld, snd, rcv, direct, fwd):
    me = lax.axis_index('ws')
    dpi = lax.axis_index('dp')
    z = me // 4
    s = me % 4
    y = s // 2
    c = s % 2

    z_near = (z, z + 1 - 2 * (z % 2), 2 - z // 2, 3 * (1 - z // 2))
    chip = me // 2

    def chip_of(dist, ky):
        return z_near[dist] * 2 + (y + ky) % 2

    near_first = [(dist, ky) for dist in range(4) for ky in (0, 1)][1:]

    def peer_of(off):
        kz, ky, kc = off
        return ((z + kz) % 4) * 4 + ((y + ky) % 2) * 2 + (c + kc) % 2

    def send(src, dst, ph, off):
        pltpu.make_async_remote_copy(src_ref=src, dst_ref=dst, send_sem=snd.at[ph], recv_sem=rcv.at[ph],
                                     device_id={'ws': peer_of(off)}, device_id_type=MESH).start()

    def desc(buf, ph):
        return pltpu.make_async_remote_copy(src_ref=buf, dst_ref=buf, send_sem=snd.at[ph], recv_sem=rcv.at[ph],
                                            device_id={'ws': me}, device_id_type=MESH)

    def gather_start(buf, ph, row):
        for dist, ky in near_first[::-1]:
            pltpu.make_async_remote_copy(src_ref=buf.at[me], dst_ref=buf.at[me], send_sem=snd.at[ph],
                                         recv_sem=direct.at[row, chip],
                                         device_id={'ws': chip_of(dist, ky) * 2 + c}, device_id_type=MESH).start()
        gather_pass(buf, ph, row, me, chip)

    def gather_pass(buf, ph, row, src, src_chip):
        pltpu.make_async_remote_copy(src_ref=buf.at[src], dst_ref=buf.at[src], send_sem=snd.at[ph],
                                     recv_sem=fwd.at[row, src_chip],
                                     device_id={'ws': peer_of(SIBLING)}, device_id_type=MESH).start()

    def arrived(buf, ph, sem):
        pltpu.make_async_remote_copy(src_ref=buf.at[0], dst_ref=buf.at[0], send_sem=snd.at[ph], recv_sem=sem,
                                     device_id={'ws': me}, device_id_type=MESH).wait_recv()

    def gather_step(buf, ph, row, dist, ky):
        src_chip = chip_of(dist, ky)
        arrived(buf, ph, direct.at[row, src_chip])
        gather_pass(buf, ph, row, src_chip * 2 + c, src_chip)

    def subgroup(buf, ph):
        for off in SUB_OFFS:
            send(buf.at[s], buf.at[s], ph, off)

    def weight_start(w, ph):
        for off in Z_OFFS:
            send(w.at[z, dpi], w.at[z, dpi], ph, off)

    def weight_pass(w, ph):
        desc(w.at[pl.ds(0, 3), 0], ph).wait_recv()
        for kz in (1, 2, 3):
            src = (z + kz) % 4
            pltpu.make_async_remote_copy(src_ref=w.at[src, dpi], dst_ref=w.at[src, dpi], send_sem=snd.at[ph + 11],
                                         recv_sem=rcv.at[ph + 11], device_id={'dp': 1 - dpi, 'ws': me},
                                         device_id_type=MESH).start()

    def weight_finish(w, ph):
        desc(w.at[pl.ds(0, 3), 0], ph + 11).wait_recv()

    bar = pltpu.get_barrier_semaphore()
    pl.semaphore_signal(bar, inc=1, device_id={'dp': 1 - dpi, 'ws': me}, device_id_type=MESH)
    for off in ALL_OFFS:
        pl.semaphore_signal(bar, inc=1, device_id={'ws': peer_of(off)}, device_id_type=MESH)

    loads = {}

    def load(name, src, dst):
        cp = pltpu.make_async_copy(src, dst, ld.at[len(loads)])
        cp.start()
        loads[name] = cp

    load('hid', hid, hs.at[s])
    load('ln1', ln1, ln1_v)
    load('pos', pos, pos_s)
    load('idx', idx, idx_s)
    load('wq', wq, wqkv.at[pl.ds(0, CB)])
    load('wk', wk, wqkv.at[pl.ds(CB, CB)])
    load('wv', wv, wqkv.at[pl.ds(2 * CB, CB)])
    load('ln2', ln2, ln2_v)
    load('ln3', ln3, ln3_v)
    load('rel', rel, rel_v)
    load('mask', mask, mask_v)
    load('wr', wr, rw.at[me])
    load('wo0', wo.at[pl.ds(0, CB // 2)], wgo.at[z, 0])
    load('wo1', wo.at[pl.ds(CB // 2, CB // 2)], wgo.at[z, 1])
    load('wqc0', wqc.at[pl.ds(0, CB // 2)], wgq.at[z, 0])
    load('wqc1', wqc.at[pl.ds(CB // 2, CB // 2)], wgq.at[z, 1])
    load('woc0', woc.at[pl.ds(0, CB // 2)], wgc.at[z, 0])
    load('woc1', woc.at[pl.ds(CB // 2, CB // 2)], wgc.at[z, 1])

    wqkv[3 * CB:256, :] = jnp.zeros((256 - 3 * CB, D), BF16)
    loads['hid'].wait()
    loads['ln1'].wait()
    m1[me] = rms(hs[s].astype(F32), ln1_v[...].reshape(1, D))
    pl.semaphore_wait(bar, NDEV)

    gather_start(m1, 0, 0)
    subgroup(hs, 7)
    load('k', kT, k_old)
    load('v', vT, v_old)
    loads['pos'].wait()
    loads['idx'].wait()
    row8 = iota((ROWS, 128), 0)
    idx_own = jnp.zeros((ROWS, 128), jnp.int32)
    for i in range(ROWS):
        idx_own = jnp.where(row8 == i, idx_s[i], idx_own)
    idx_own = idx_own.astype(F32)
    ix[me] = idx_own.astype(BF16)

    loads['rel'].wait()
    loads['mask'].wait()
    rel_f = rel_v[...]
    rel_hi = rel_f.astype(BF16)
    rem = rel_f - rel_hi.astype(F32)
    rel_mid = rem.astype(BF16)
    rel_lo = (rem - rel_mid.astype(F32)).astype(BF16)
    src_i = iota((LS, LS), 0)
    dst_i = iota((LS, LS), 1)
    lane12 = iota((HEADS, LS), 1)
    bias_s[...] = jnp.zeros((ROWS, HPAD, LS), F32)
    for b in range(ROWS):
        pick = jnp.where(src_i + dst_i == pos_s[b], 1.0, 0.0).astype(BF16)
        bb = jnp.dot(rel_hi, pick, preferred_element_type=F32)
        bb = bb + jnp.dot(rel_mid, pick, preferred_element_type=F32)
        bb = bb + jnp.dot(rel_lo, pick, preferred_element_type=F32)
        bias_s[b, 0:HEADS, :] = jnp.where(lane12 <= pos_s[b], bb, NEG)
    for name in ('wq', 'wk', 'wv', 'ln2', 'ln3', 'wr', 'wqc0', 'wqc1', 'woc0', 'woc1'):
        loads[name].wait()

    for dist, ky in near_first:
        gather_step(m1, 0, 0, dist, ky)
        if (dist, ky) == (1, 1):
            loads['wo0'].wait()
            loads['wo1'].wait()
            weight_start(wgo, 8)
    for dist in range(4):
        for ky in (0, 1):
            arrived(m1, 0, fwd.at[0, chip_of(dist, ky)])
    xn = m1[...].astype(F32).reshape(NDEV * ROWS, D).astype(BF16)
    st2[...] = dot_nt(xn, wqkv[...]).reshape(NDEV, ROWS, 256).astype(BF16)
    r2[me] = st2[me]
    for off in ALL_OFFS:
        send(st2.at[peer_of(off)], r2.at[me], 1, off)
    weight_start(wgq, 9)
    weight_start(wgc, 10)
    load('ck', ckT, ck_v)
    load('cv', cvT, cv_v)

    sel_r = iota((4 * CB, D), 0)
    sel_q = ((sel_r >= CB).astype(jnp.int32) + (sel_r >= 2 * CB).astype(jnp.int32)
             + (sel_r >= 3 * CB).astype(jnp.int32))
    sel = (iota((4 * CB, D), 1) == sel_r + sel_q * (4 * CB - CB) + s * CB)
    sel = jnp.where(sel, 1.0, 0.0).astype(BF16)
    desc(hs.at[pl.ds(0, 3)], 7).wait_recv()
    h_sub = hs[...].astype(F32).reshape(4 * ROWS, D).astype(BF16)
    h_blk = dot_nt(h_sub, sel)

    loads['k'].wait()
    loads['v'].wait()
    desc(r2.at[pl.ds(0, NDEV - 1)], 1).wait_recv()
    weight_pass(wgo, 8)
    rv = r2[...].astype(F32)

    def columns(lo):
        return jnp.concatenate([rv[d, :, lo:lo + CB] for d in range(NDEV)], axis=-1)

    q8 = columns(0)
    k8 = columns(CB)
    v8 = columns(2 * CB)
    lane_h = iota((HPAD, LS), 1)
    attention(q8, k_old, v_old, lambda b: bias_s[b], s_self, ctx_v, q_v,
              (k8, v8, lambda b: lane_h == pos_s[b]))

    def update(new, old, out):
        cols = new.T
        lane_s = iota((D, LS), 1)
        for b in range(ROWS):
            out[b] = jnp.where(lane_s == pos_s[b], jnp.broadcast_to(cols[:, b:b + 1], (D, LS)),
                               old[b].astype(F32)).astype(BF16)

    def natural(pieces):
        return jnp.concatenate([pieces[t][:, q * CB:(q + 1) * CB] for q in range(4) for t in range(4)], axis=-1)

    def unpack(blk):
        tail = jnp.concatenate([blk[32:48, 0:64], blk[32:48, 64:128]], axis=0)
        return jnp.concatenate([blk[0:32, :], tail], axis=-1)

    c3[s] = ctx_v[...].astype(BF16)
    subgroup(c3, 2)
    update(k8, k_old, k_v)
    weight_pass(wgq, 9)
    update(v8, v_old, v_v)
    load('win', win, win_v)
    load('wout', wout, wout_v)
    desc(c3.at[pl.ds(0, 3)], 2).wait_recv()
    weight_finish(wgo, 8)
    ctx = c3[...].astype(F32).reshape(4 * ROWS, D).astype(BF16)
    h1_blk = (h_blk + dot_nt(ctx, wgo[...].reshape(4 * CB, D))).astype(BF16)
    r4[s, :, 0:4 * CB] = h1_blk
    subgroup(r4, 3)
    desc(r4.at[pl.ds(0, 3)], 3).wait_recv()
    weight_finish(wgq, 9)
    r4f = r4[...].astype(F32)
    h1 = natural([r4f[t] for t in range(4)])
    x2 = rms(h1, ln2_v[...].reshape(1, D))
    st5[:, :, 0:4 * CB] = dot_nt(x2, wgq[...].reshape(4 * CB, D)).reshape(4, ROWS, 4 * CB).astype(BF16)
    r5[s] = st5[s]
    for off in SUB_OFFS:
        kz, ky, kc = off
        send(st5.at[((y + ky) % 2) * 2 + (c + kc) % 2], r5.at[s], 4, off)
    weight_pass(wgc, 10)
    for off in ALL_OFFS:
        send(ix.at[me], ix.at[me], 12, off)
        send(rw.at[me], rw.at[me], 11, off)
    loads['ck'].wait()
    loads['cv'].wait()
    desc(r5.at[pl.ds(0, 3)], 4).wait_recv()
    r5f = r5[...].astype(F32)
    q2 = natural([r5f[t] for t in range(4)])
    attention(q2, ck_v, cv_v, lambda b: jnp.where(mask_v[b:b + 1, :] == 1, 0.0, NEG), s_cross, ctx_v, q_v)

    c6[s] = ctx_v[...].astype(BF16)
    subgroup(c6, 5)
    desc(c6.at[pl.ds(0, 3)], 5).wait_recv()
    weight_finish(wgc, 10)
    ctx2 = c6[...].astype(F32).reshape(4 * ROWS, D).astype(BF16)
    h2_blk = (h1_blk.astype(F32) + dot_nt(ctx2, wgc[...].reshape(4 * CB, D))).astype(BF16)
    h2_f = h2_blk.astype(F32)
    r7[me, 0:32, :] = h2_f[:, 0:128].astype(BF16)
    r7[me, 32:48, :] = jnp.concatenate([h2_f[0:16, 128:192], h2_f[16:32, 128:192]], axis=-1).astype(BF16)

    gather_start(r7, 6, 1)
    desc(ix.at[pl.ds(0, NDEV - 1)], 12).wait_recv()
    idx_all = ix[...].astype(F32).reshape(NDEV * ROWS, 128)
    idx_t = idx_all.T
    earlier = (idx_t[0:ROWS, :] == idx_own) & (iota((ROWS, 128), 1) < me * ROWS + row8)
    slot = jnp.sum(jnp.where(earlier, 1.0, 0.0), axis=-1, keepdims=True)
    loads['win'].wait()
    loads['wout'].wait()

    def group(dist):
        for ky in (0, 1):
            arrived(r7, 6, fwd.at[1, chip_of(dist, ky)])
        t = z_near[dist]
        h2g = natural([unpack(r7[4 * t + u].astype(F32)) for u in range(4)])
        at = pl.ds(pl.multiple_of(32 * t, 32), 32)
        h2_v[at, :] = h2g
        x3_v[at, :] = rms(h2g, ln3_v[...].reshape(1, D))

    for dist, ky in near_first[:5]:
        gather_step(r7, 6, 1, dist, ky)
    group(0)
    gather_step(r7, 6, 1, *near_first[5])
    gather_step(r7, 6, 1, *near_first[6])
    group(1)
    group(2)
    group(3)
    x3 = x3_v[...]
    idx3 = jnp.concatenate([idx_all, idx_all, idx_all], axis=-1)
    half = (iota((NDEV * ROWS, 384), 1) >= 192).astype(F32)
    for p in range(8):
        hh = dot_nt(x3, win_v[2 * p:2 * p + 2].reshape(384, D))
        u_v[:, 384 * p:384 * p + 384] = jnp.where(idx3 == half + float(2 * p), jnp.maximum(hh, 0.0), 0.0).astype(BF16)
    def partial(n):
        yn = jnp.dot(u_v[...], wout_v[:, :, 256 * n:256 * n + 256].reshape(NDEV * 192, 256),
                     preferred_element_type=F32).reshape(8, 2, ROWS, 256)
        st8[n, 0] = yn[:, 0]
        st8[n, 1] = yn[:, 1]
        send(st8.at[n, 1 - c], r8.at[n], 13 + n, SIBLING)

    def reduce_send(n):
        desc(r8.at[n], 13 + n).wait_recv()
        st9[n] = st8[n, c] + r8[n]
        for off in CHIP_OFFS:
            send(st9.at[n, peer_of(off) // 2], r9.at[n, chip], 16 + n, off)
        r9[n, chip] = st9[n, chip]

    partial(0)
    partial(1)
    partial(2)
    reduce_send(0)
    reduce_send(1)
    reduce_send(2)

    desc(rw.at[pl.ds(0, NDEV - 1)], 11).wait_recv()
    h2_own = h2_v[pl.ds(pl.multiple_of(me * ROWS, ROWS), ROWS), :]
    x3_own = rms(h2_own, ln3_v[...].reshape(1, D)).astype(F32)
    logits = dot_nt(x3_own, rw[...].reshape(NDEV, D), precision=lax.Precision.HIGHEST)
    ex = jnp.exp(logits - jnp.max(logits, axis=-1, keepdims=True))
    probs = ex / jnp.sum(ex, axis=-1, keepdims=True)
    mine = iota((ROWS, NDEV), 1).astype(F32) == idx_own[:, 0:NDEV]
    gate = jnp.sum(jnp.where(mine, probs, 0.0), axis=-1, keepdims=True)
    gate = jnp.where(slot < float(NDEV), gate, 0.0)

    for n in range(3):
        desc(r9.at[n, pl.ds(0, 7)], 16 + n).wait_recv()
    yv = jnp.concatenate([jnp.sum(r9[n], axis=0) for n in range(3)], axis=-1).astype(BF16).astype(F32)
    out_h[...] = (h2_own + yv * gate).astype(BF16)

    for buf, ph in ((m1, 0), (st2, 1), (r7, 6), (rw, 11), (ix, 12)):
        desc(buf.at[pl.ds(0, NDEV - 1)], ph).wait_send()
    for n in range(3):
        desc(st9.at[n, pl.ds(0, 7)], 16 + n).wait_send()
        desc(r8.at[n], 13 + n).wait_send()
    for buf, ph in ((c3, 2), (r4, 3), (st5, 4), (c6, 5), (hs, 7)):
        desc(buf.at[pl.ds(0, 3)], ph).wait_send()
    for w, ph in ((wgo, 8), (wgq, 9), (wgc, 10)):
        desc(w.at[pl.ds(0, 3), 0], ph).wait_send()
        desc(w.at[pl.ds(0, 3), 0], ph + 11).wait_send()


def store(h_in, k_in, v_in, h_out, k_out, v_out, sem):
    parts = [(src.at[:, :, lanes], dst.at[:, :, lanes]) for src, dst in ((k_in, k_out), (v_in, v_out))
             for lanes in (pl.ds(0, 128), pl.ds(128, LS - 128))]
    copies = [pltpu.make_async_copy(src, dst, sem.at[i])
              for i, (src, dst) in enumerate(((h_in, h_out), *parts))]
    for cp in copies:
        cp.start()
    for cp in copies:
        cp.wait()


def solution(mesh):
    rows = ('dp', 'ws')
    row_vec = P(rows)
    row_mat = P(rows, None)
    cache = P(rows, None, None, None)
    col = P(None, 'ws')
    in_specs = (row_mat, cache, cache, cache, cache, row_vec, row_mat, P(None, None), row_vec,
                P(None), P(None), P(None), col, col, col, col, col, col,
                col, P(None, None, 'ws'), P(None, 'ws', None))
    out_specs = (row_mat, cache, cache)

    any_spec = pl.BlockSpec(memory_space=pltpu.HBM)
    vmem = pl.BlockSpec(memory_space=pltpu.VMEM)

    def block(hidden, self_k, self_v, cross_k, cross_v, positions, enc_mask, rel_bias, expert_idx,
              ln_self, ln_cross, ln_ffn, wq_self, wk_self, wv_self, wo_self, wq_cross, wo_cross,
              w_router, w_in, w_out):
        def flat(cache_arr):
            return jnp.swapaxes(cache_arr, 2, 3).reshape(ROWS, D, cache_arr.shape[2])

        def unflat(arr):
            return jnp.swapaxes(arr.reshape(ROWS, HEADS, 64, LS), 2, 3)

        args = (hidden, flat(self_k), flat(self_v), flat(cross_k), flat(cross_v), positions, enc_mask, rel_bias,
                expert_idx, ln_self, ln_cross, ln_ffn,
                wq_self.T, wk_self.T, wv_self.T, wo_self.T, wq_cross.T, wo_cross.T, w_router.T,
                jnp.swapaxes(w_in, 1, 2), w_out)
        specs = [any_spec] * len(args)
        V = pltpu.VMEM
        scratch = [
            V((ROWS, D, LC), BF16), V((ROWS, D, LC), BF16), V((NDEV, 192, D), BF16), V((NDEV, 192, D), BF16),
            V((ROWS, LC), jnp.int32), V((HEADS, LS), F32), V((D,), F32), V((D,), F32), V((D,), F32), V((256, D), BF16),
            V((NDEV, ROWS, D), BF16), V((NDEV, ROWS, 128), BF16), V((NDEV, ROWS, 256), BF16), V((NDEV, ROWS, 256), BF16),
            V((4, 2, CB // 2, D), BF16), V((4, 2, CB // 2, D), BF16), V((4, 2, CB // 2, D), BF16), V((NDEV, 1, D), F32),
            V((4, ROWS, D), BF16), V((4, 4 * ROWS, 256), BF16), V((4, ROWS, 256), BF16), V((4, ROWS, 256), BF16),
            V((4, ROWS, D), BF16), V((NDEV, CB, 128), BF16), V((3, 2, 8, ROWS, 256), F32), V((3, 8, ROWS, 256), F32),
            V((3, 8, ROWS, 256), F32), V((3, 8, ROWS, 256), F32),
            V((ROWS, HPAD, LS), F32), V((ROWS, HPAD, LS), F32), V((ROWS, HPAD, LC), F32), V((ROWS, D), F32),
            V((NDEV * ROWS, D), F32), V((NDEV * ROWS, D), BF16), V((NDEV * ROWS, NDEV * 192), BF16),
            V((ROWS, D, LS), BF16), V((ROWS, D, LS), BF16), V((4, ROWS, D), BF16), V((ROWS, HPAD, D), BF16),
            pltpu.SMEM((ROWS,), jnp.int32), pltpu.SMEM((ROWS,), jnp.int32),
            pltpu.SemaphoreType.DMA((24,)), pltpu.SemaphoreType.DMA((22,)), pltpu.SemaphoreType.DMA((22,)),
            pltpu.SemaphoreType.DMA((2, 8)), pltpu.SemaphoreType.DMA((2, 8)),
        ]
        h_out, k_out, v_out = pl.pallas_call(
            kernel,
            out_shape=(V((ROWS, D), BF16), V((ROWS, D, LS), BF16), V((ROWS, D, LS), BF16)),
            in_specs=specs,
            out_specs=(vmem, vmem, vmem),
            scratch_shapes=scratch,
            compiler_params=pltpu.CompilerParams(collective_id=0, has_side_effects=True,
                                                 vmem_limit_bytes=67043328 - 2 * 3145728 - 16384),
        )(*args)
        outs = (jax.ShapeDtypeStruct((ROWS, D), BF16), jax.ShapeDtypeStruct((ROWS, D, LS), BF16),
                jax.ShapeDtypeStruct((ROWS, D, LS), BF16))
        h_out, k_out, v_out = pl.pallas_call(
            store, out_shape=outs, in_specs=[vmem] * 3, out_specs=(any_spec,) * 3,
            scratch_shapes=[pltpu.SemaphoreType.DMA((5,))],
            compiler_params=pltpu.CompilerParams(vmem_limit_bytes=4 * 1024 * 1024),
        )(h_out, k_out, v_out)
        return h_out, unflat(k_out), unflat(v_out)

    return jax.shard_map(block, mesh=mesh, in_specs=in_specs, out_specs=out_specs, check_vma=False)
```

```python
import jax
import jax.numpy as jnp
from jax import lax
from jax.experimental import pallas as pl
from jax.experimental.pallas import tpu as pltpu
from jax.sharding import PartitionSpec as P

EPS = 1e-6
NEG = -1e30
F32 = jnp.float32
BF16 = jnp.bfloat16
MESH = pl.DeviceIdType.MESH

ROWS = 8
D = 768
HEADS = 12
HPAD = 16
LS = 192
LC = 384
NDEV = 16
CB = 48
NT = (((1,), (1,)), ((), ()))

ALL_OFFS = [(kz, ky, kc) for kz in (2, 3, 1, 0) for ky in (1, 0) for kc in (1, 0) if (kz, ky, kc) != (0, 0, 0)]
CHIP_OFFS = [off for off in ALL_OFFS if off[2] == 0]
SIBLING = (0, 0, 1)
SUB_OFFS = [(0, 1, 1), (0, 1, 0), (0, 0, 1)]
Z_OFFS = [(2, 0, 0), (3, 0, 0), (1, 0, 0)]


def dot_nt(a, b, **kw):
    return lax.dot_general(a, b, NT, preferred_element_type=F32, **kw)


def iota(shape, axis):
    return lax.broadcasted_iota(jnp.int32, shape, axis)


def rms(x, g):
    inv = lax.rsqrt(jnp.mean(x * x, axis=-1, keepdims=True) + EPS)
    return (x * inv * g).astype(BF16)


def head_mask():
    row = iota((HPAD, D), 0) * 64
    col = iota((HPAD, D), 1)
    return (col >= row) & (col < row + 64)


def attention(q8, k_ref, v_ref, bias_of, s_ref, ctx_ref, q_ref, patch=None):
    hm = head_mask()
    for b in range(ROWS):
        qb = jnp.where(hm, jnp.broadcast_to(q8[b:b + 1, :], (HPAD, D)), 0.0).astype(BF16)
        q_ref[b] = qb
    if patch is not None:
        k8, v8, hit_of = patch
        new = dot_nt(q_ref[...].reshape(ROWS * HPAD, D), k8.astype(BF16))
        row = iota((ROWS * HPAD, ROWS), 0)
        col = iota((ROWS * HPAD, ROWS), 1) * HPAD
        new = jnp.sum(jnp.where((row >= col) & (row < col + HPAD), new, 0.0), axis=-1, keepdims=True)
    for b in range(ROWS):
        sb = jnp.dot(q_ref[b], k_ref[b], preferred_element_type=F32)
        if patch is not None:
            sb = jnp.where(hit_of(b), new[b * HPAD:(b + 1) * HPAD], sb)
        s_ref[b] = sb + bias_of(b)
    s = s_ref[...]
    p = jnp.exp(s - jnp.max(s, axis=-1, keepdims=True))
    s_ref[...] = p / jnp.sum(p, axis=-1, keepdims=True)
    for b in range(ROWS):
        pb = s_ref[b].astype(BF16)
        if patch is None:
            cb = dot_nt(pb, v_ref[b])
        else:
            pf = pb.astype(F32)
            hit = hit_of(b)
            at_pos = jnp.sum(jnp.where(hit, pf, 0.0), axis=-1, keepdims=True)
            cb = dot_nt(jnp.where(hit, 0.0, pf).astype(BF16), v_ref[b]) + at_pos * v8[b:b + 1, :]
        ctx_ref[b:b + 1, :] = jnp.sum(jnp.where(hm, cb, 0.0), axis=0, keepdims=True)


def kernel(hid, kT, vT, ckT, cvT, pos, mask, rel, idx, ln1, ln2, ln3, wq, wk, wv, wo, wqc, woc, wr, win, wout,
           out_h, k_v, v_v,
           ck_v, cv_v, win_v, wout_v, mask_v, rel_v, ln1_v, ln2_v, ln3_v, wqkv, m1, ix, st2, r2, wgo, wgq, wgc, rw,
           c3, r4, st5, r5, c6, r7, st8, r8, st9, r9, bias_s, s_self, s_cross, ctx_v, h2_v, x3_v, u_v,
           k_old, v_old, hs, q_v, pos_s, idx_s, ld, snd, rcv, direct, fwd):
    me = lax.axis_index('ws')
    dpi = lax.axis_index('dp')
    z = me // 4
    s = me % 4
    y = s // 2
    c = s % 2

    z_near = (z, z + 1 - 2 * (z % 2), 2 - z // 2, 3 * (1 - z // 2))
    chip = me // 2

    def chip_of(dist, ky):
        return z_near[dist] * 2 + (y + ky) % 2

    near_first = [(dist, ky) for dist in range(4) for ky in (0, 1)][1:]

    def peer_of(off):
        kz, ky, kc = off
        return ((z + kz) % 4) * 4 + ((y + ky) % 2) * 2 + (c + kc) % 2

    def send(src, dst, ph, off):
        pltpu.make_async_remote_copy(src_ref=src, dst_ref=dst, send_sem=snd.at[ph], recv_sem=rcv.at[ph],
                                     device_id={'ws': peer_of(off)}, device_id_type=MESH).start()

    def desc(buf, ph):
        return pltpu.make_async_remote_copy(src_ref=buf, dst_ref=buf, send_sem=snd.at[ph], recv_sem=rcv.at[ph],
                                            device_id={'ws': me}, device_id_type=MESH)

    def gather_start(buf, ph, row):
        for dist, ky in near_first[::-1]:
            pltpu.make_async_remote_copy(src_ref=buf.at[me], dst_ref=buf.at[me], send_sem=snd.at[ph],
                                         recv_sem=direct.at[row, chip],
                                         device_id={'ws': chip_of(dist, ky) * 2 + c}, device_id_type=MESH).start()
        gather_pass(buf, ph, row, me, chip)

    def gather_pass(buf, ph, row, src, src_chip):
        pltpu.make_async_remote_copy(src_ref=buf.at[src], dst_ref=buf.at[src], send_sem=snd.at[ph],
                                     recv_sem=fwd.at[row, src_chip],
                                     device_id={'ws': peer_of(SIBLING)}, device_id_type=MESH).start()

    def arrived(buf, ph, sem):
        pltpu.make_async_remote_copy(src_ref=buf.at[0], dst_ref=buf.at[0], send_sem=snd.at[ph], recv_sem=sem,
                                     device_id={'ws': me}, device_id_type=MESH).wait_recv()

    def gather_step(buf, ph, row, dist, ky):
        src_chip = chip_of(dist, ky)
        arrived(buf, ph, direct.at[row, src_chip])
        gather_pass(buf, ph, row, src_chip * 2 + c, src_chip)

    def subgroup(buf, ph):
        for off in SUB_OFFS:
            send(buf.at[s], buf.at[s], ph, off)

    def weight_start(w, ph):
        for off in Z_OFFS:
            send(w.at[z, dpi], w.at[z, dpi], ph, off)

    def weight_pass(w, ph):
        desc(w.at[pl.ds(0, 3), 0], ph).wait_recv()
        for kz in (1, 2, 3):
            src = (z + kz) % 4
            pltpu.make_async_remote_copy(src_ref=w.at[src, dpi], dst_ref=w.at[src, dpi], send_sem=snd.at[ph + 11],
                                         recv_sem=rcv.at[ph + 11], device_id={'dp': 1 - dpi, 'ws': me},
                                         device_id_type=MESH).start()

    def weight_finish(w, ph):
        desc(w.at[pl.ds(0, 3), 0], ph + 11).wait_recv()

    bar = pltpu.get_barrier_semaphore()
    pl.semaphore_signal(bar, inc=1, device_id={'dp': 1 - dpi, 'ws': me}, device_id_type=MESH)
    for off in ALL_OFFS:
        pl.semaphore_signal(bar, inc=1, device_id={'ws': peer_of(off)}, device_id_type=MESH)

    loads = {}

    def load(name, src, dst):
        cp = pltpu.make_async_copy(src, dst, ld.at[len(loads)])
        cp.start()
        loads[name] = cp

    load('hid', hid, hs.at[s])
    load('ln1', ln1, ln1_v)
    load('pos', pos, pos_s)
    load('idx', idx, idx_s)
    load('wq', wq, wqkv.at[pl.ds(0, CB)])
    load('wk', wk, wqkv.at[pl.ds(CB, CB)])
    load('wv', wv, wqkv.at[pl.ds(2 * CB, CB)])
    load('ln2', ln2, ln2_v)
    load('ln3', ln3, ln3_v)
    load('rel', rel, rel_v)
    load('mask', mask, mask_v)
    load('wr', wr, rw.at[me])
    load('wo0', wo.at[pl.ds(0, CB // 2)], wgo.at[z, 0])
    load('wo1', wo.at[pl.ds(CB // 2, CB // 2)], wgo.at[z, 1])
    load('wqc0', wqc.at[pl.ds(0, CB // 2)], wgq.at[z, 0])
    load('wqc1', wqc.at[pl.ds(CB // 2, CB // 2)], wgq.at[z, 1])
    load('woc0', woc.at[pl.ds(0, CB // 2)], wgc.at[z, 0])
    load('woc1', woc.at[pl.ds(CB // 2, CB // 2)], wgc.at[z, 1])

    wqkv[3 * CB:256, :] = jnp.zeros((256 - 3 * CB, D), BF16)
    loads['hid'].wait()
    loads['ln1'].wait()
    m1[me] = rms(hs[s].astype(F32), ln1_v[...].reshape(1, D))
    pl.semaphore_wait(bar, NDEV)

    gather_start(m1, 0, 0)
    loads['wo0'].wait()
    loads['wo1'].wait()
    weight_start(wgo, 8)
    subgroup(hs, 7)
    load('k', kT, k_old)
    load('v', vT, v_old)
    loads['pos'].wait()
    loads['idx'].wait()
    row8 = iota((ROWS, 128), 0)
    idx_own = jnp.zeros((ROWS, 128), jnp.int32)
    for i in range(ROWS):
        idx_own = jnp.where(row8 == i, idx_s[i], idx_own)
    idx_own = idx_own.astype(F32)
    ix[me] = idx_own.astype(BF16)

    loads['rel'].wait()
    loads['mask'].wait()
    rel_f = rel_v[...]
    rel_hi = rel_f.astype(BF16)
    rem = rel_f - rel_hi.astype(F32)
    rel_mid = rem.astype(BF16)
    rel_lo = (rem - rel_mid.astype(F32)).astype(BF16)
    src_i = iota((LS, LS), 0)
    dst_i = iota((LS, LS), 1)
    lane12 = iota((HEADS, LS), 1)
    bias_s[...] = jnp.zeros((ROWS, HPAD, LS), F32)
    for b in range(ROWS):
        pick = jnp.where(src_i + dst_i == pos_s[b], 1.0, 0.0).astype(BF16)
        bb = jnp.dot(rel_hi, pick, preferred_element_type=F32)
        bb = bb + jnp.dot(rel_mid, pick, preferred_element_type=F32)
        bb = bb + jnp.dot(rel_lo, pick, preferred_element_type=F32)
        bias_s[b, 0:HEADS, :] = jnp.where(lane12 <= pos_s[b], bb, NEG)
    for name in ('wq', 'wk', 'wv', 'ln2', 'ln3', 'wr', 'wqc0', 'wqc1', 'woc0', 'woc1'):
        loads[name].wait()

    for dist, ky in near_first:
        gather_step(m1, 0, 0, dist, ky)
    for dist in range(4):
        for ky in (0, 1):
            arrived(m1, 0, fwd.at[0, chip_of(dist, ky)])
    xn = m1[...].astype(F32).reshape(NDEV * ROWS, D).astype(BF16)
    st2[...] = dot_nt(xn, wqkv[...]).reshape(NDEV, ROWS, 256).astype(BF16)
    r2[me] = st2[me]
    for off in ALL_OFFS:
        send(st2.at[peer_of(off)], r2.at[me], 1, off)
    weight_start(wgq, 9)
    weight_start(wgc, 10)
    load('ck', ckT, ck_v)
    load('cv', cvT, cv_v)

    sel_r = iota((4 * CB, D), 0)
    sel_q = ((sel_r >= CB).astype(jnp.int32) + (sel_r >= 2 * CB).astype(jnp.int32)
             + (sel_r >= 3 * CB).astype(jnp.int32))
    sel = (iota((4 * CB, D), 1) == sel_r + sel_q * (4 * CB - CB) + s * CB)
    sel = jnp.where(sel, 1.0, 0.0).astype(BF16)
    desc(hs.at[pl.ds(0, 3)], 7).wait_recv()
    h_sub = hs[...].astype(F32).reshape(4 * ROWS, D).astype(BF16)
    h_blk = dot_nt(h_sub, sel)

    loads['k'].wait()
    loads['v'].wait()
    desc(r2.at[pl.ds(0, NDEV - 1)], 1).wait_recv()
    weight_pass(wgo, 8)
    rv = r2[...].astype(F32)

    def columns(lo):
        return jnp.concatenate([rv[d, :, lo:lo + CB] for d in range(NDEV)], axis=-1)

    q8 = columns(0)
    k8 = columns(CB)
    v8 = columns(2 * CB)
    lane_h = iota((HPAD, LS), 1)
    attention(q8, k_old, v_old, lambda b: bias_s[b], s_self, ctx_v, q_v,
              (k8, v8, lambda b: lane_h == pos_s[b]))

    def update(new, old, out):
        cols = new.T
        lane_s = iota((D, LS), 1)
        for b in range(ROWS):
            out[b] = jnp.where(lane_s == pos_s[b], jnp.broadcast_to(cols[:, b:b + 1], (D, LS)),
                               old[b].astype(F32)).astype(BF16)

    def natural(pieces):
        return jnp.concatenate([pieces[t][:, q * CB:(q + 1) * CB] for q in range(4) for t in range(4)], axis=-1)

    def unpack(blk):
        tail = jnp.concatenate([blk[32:48, 0:64], blk[32:48, 64:128]], axis=0)
        return jnp.concatenate([blk[0:32, :], tail], axis=-1)

    c3[s] = ctx_v[...].astype(BF16)
    subgroup(c3, 2)
    update(k8, k_old, k_v)
    weight_pass(wgq, 9)
    for off in ALL_OFFS:
        send(ix.at[me], ix.at[me], 12, off)
        send(rw.at[me], rw.at[me], 11, off)
    update(v8, v_old, v_v)
    load('win', win, win_v)
    load('wout', wout, wout_v)
    desc(c3.at[pl.ds(0, 3)], 2).wait_recv()
    weight_finish(wgo, 8)
    ctx = c3[...].astype(F32).reshape(4 * ROWS, D).astype(BF16)
    h1_blk = (h_blk + dot_nt(ctx, wgo[...].reshape(4 * CB, D))).astype(BF16)
    r4[s, :, 0:4 * CB] = h1_blk
    subgroup(r4, 3)
    desc(r4.at[pl.ds(0, 3)], 3).wait_recv()
    weight_finish(wgq, 9)
    r4f = r4[...].astype(F32)
    h1 = natural([r4f[t] for t in range(4)])
    x2 = rms(h1, ln2_v[...].reshape(1, D))
    st5[:, :, 0:4 * CB] = dot_nt(x2, wgq[...].reshape(4 * CB, D)).reshape(4, ROWS, 4 * CB).astype(BF16)
    r5[s] = st5[s]
    for off in SUB_OFFS:
        kz, ky, kc = off
        send(st5.at[((y + ky) % 2) * 2 + (c + kc) % 2], r5.at[s], 4, off)
    weight_pass(wgc, 10)
    loads['ck'].wait()
    loads['cv'].wait()
    desc(r5.at[pl.ds(0, 3)], 4).wait_recv()
    r5f = r5[...].astype(F32)
    q2 = natural([r5f[t] for t in range(4)])
    attention(q2, ck_v, cv_v, lambda b: jnp.where(mask_v[b:b + 1, :] == 1, 0.0, NEG), s_cross, ctx_v, q_v)

    c6[s] = ctx_v[...].astype(BF16)
    subgroup(c6, 5)
    desc(c6.at[pl.ds(0, 3)], 5).wait_recv()
    weight_finish(wgc, 10)
    ctx2 = c6[...].astype(F32).reshape(4 * ROWS, D).astype(BF16)
    h2_blk = (h1_blk.astype(F32) + dot_nt(ctx2, wgc[...].reshape(4 * CB, D))).astype(BF16)
    h2_f = h2_blk.astype(F32)
    r7[me, 0:32, :] = h2_f[:, 0:128].astype(BF16)
    r7[me, 32:48, :] = jnp.concatenate([h2_f[0:16, 128:192], h2_f[16:32, 128:192]], axis=-1).astype(BF16)

    gather_start(r7, 6, 1)
    desc(ix.at[pl.ds(0, NDEV - 1)], 12).wait_recv()
    idx_all = ix[...].astype(F32).reshape(NDEV * ROWS, 128)
    idx_t = idx_all.T
    earlier = (idx_t[0:ROWS, :] == idx_own) & (iota((ROWS, 128), 1) < me * ROWS + row8)
    slot = jnp.sum(jnp.where(earlier, 1.0, 0.0), axis=-1, keepdims=True)
    loads['win'].wait()
    loads['wout'].wait()

    def group(dist):
        for ky in (0, 1):
            arrived(r7, 6, fwd.at[1, chip_of(dist, ky)])
        t = z_near[dist]
        h2g = natural([unpack(r7[4 * t + u].astype(F32)) for u in range(4)])
        at = pl.ds(pl.multiple_of(32 * t, 32), 32)
        h2_v[at, :] = h2g
        x3_v[at, :] = rms(h2g, ln3_v[...].reshape(1, D))

    for dist, ky in near_first[:5]:
        gather_step(r7, 6, 1, dist, ky)
    group(0)
    gather_step(r7, 6, 1, *near_first[5])
    gather_step(r7, 6, 1, *near_first[6])
    group(1)
    group(2)
    group(3)
    x3 = x3_v[...]
    idx3 = jnp.concatenate([idx_all, idx_all, idx_all], axis=-1)
    half = (iota((NDEV * ROWS, 384), 1) >= 192).astype(F32)
    for p in range(8):
        hh = dot_nt(x3, win_v[2 * p:2 * p + 2].reshape(384, D))
        u_v[:, 384 * p:384 * p + 384] = jnp.where(idx3 == half + float(2 * p), jnp.maximum(hh, 0.0), 0.0).astype(BF16)
    def partial(n):
        yn = jnp.dot(u_v[...], wout_v[:, :, 256 * n:256 * n + 256].reshape(NDEV * 192, 256),
                     preferred_element_type=F32).reshape(8, 2, ROWS, 256)
        st8[n, 0] = yn[:, 0]
        st8[n, 1] = yn[:, 1]
        send(st8.at[n, 1 - c], r8.at[n], 13 + n, SIBLING)

    def reduce_send(n):
        desc(r8.at[n], 13 + n).wait_recv()
        st9[n] = st8[n, c] + r8[n]
        for off in CHIP_OFFS:
            send(st9.at[n, peer_of(off) // 2], r9.at[n, chip], 16 + n, off)
        r9[n, chip] = st9[n, chip]

    partial(0)
    partial(1)
    partial(2)
    reduce_send(0)
    reduce_send(1)
    reduce_send(2)

    desc(rw.at[pl.ds(0, NDEV - 1)], 11).wait_recv()
    h2_own = h2_v[pl.ds(pl.multiple_of(me * ROWS, ROWS), ROWS), :]
    x3_own = rms(h2_own, ln3_v[...].reshape(1, D)).astype(F32)
    logits = dot_nt(x3_own, rw[...].reshape(NDEV, D), precision=lax.Precision.HIGHEST)
    ex = jnp.exp(logits - jnp.max(logits, axis=-1, keepdims=True))
    probs = ex / jnp.sum(ex, axis=-1, keepdims=True)
    mine = iota((ROWS, NDEV), 1).astype(F32) == idx_own[:, 0:NDEV]
    gate = jnp.sum(jnp.where(mine, probs, 0.0), axis=-1, keepdims=True)
    gate = jnp.where(slot < float(NDEV), gate, 0.0)

    for n in range(3):
        desc(r9.at[n, pl.ds(0, 7)], 16 + n).wait_recv()
    yv = jnp.concatenate([jnp.sum(r9[n], axis=0) for n in range(3)], axis=-1).astype(BF16).astype(F32)
    out_h[...] = (h2_own + yv * gate).astype(BF16)

    for buf, ph in ((m1, 0), (st2, 1), (r7, 6), (rw, 11), (ix, 12)):
        desc(buf.at[pl.ds(0, NDEV - 1)], ph).wait_send()
    for n in range(3):
        desc(st9.at[n, pl.ds(0, 7)], 16 + n).wait_send()
        desc(r8.at[n], 13 + n).wait_send()
    for buf, ph in ((c3, 2), (r4, 3), (st5, 4), (c6, 5), (hs, 7)):
        desc(buf.at[pl.ds(0, 3)], ph).wait_send()
    for w, ph in ((wgo, 8), (wgq, 9), (wgc, 10)):
        desc(w.at[pl.ds(0, 3), 0], ph).wait_send()
        desc(w.at[pl.ds(0, 3), 0], ph + 11).wait_send()


def store(h_in, k_in, v_in, h_out, k_out, v_out, sem):
    copies = [pltpu.make_async_copy(src, dst, sem.at[i])
              for i, (src, dst) in enumerate(((k_in, k_out), (v_in, v_out), (h_in, h_out)))]
    for cp in copies:
        cp.start()
    for cp in copies:
        cp.wait()


def solution(mesh):
    rows = ('dp', 'ws')
    row_vec = P(rows)
    row_mat = P(rows, None)
    cache = P(rows, None, None, None)
    col = P(None, 'ws')
    in_specs = (row_mat, cache, cache, cache, cache, row_vec, row_mat, P(None, None), row_vec,
                P(None), P(None), P(None), col, col, col, col, col, col,
                col, P(None, None, 'ws'), P(None, 'ws', None))
    out_specs = (row_mat, cache, cache)

    any_spec = pl.BlockSpec(memory_space=pltpu.HBM)
    vmem = pl.BlockSpec(memory_space=pltpu.VMEM)

    def block(hidden, self_k, self_v, cross_k, cross_v, positions, enc_mask, rel_bias, expert_idx,
              ln_self, ln_cross, ln_ffn, wq_self, wk_self, wv_self, wo_self, wq_cross, wo_cross,
              w_router, w_in, w_out):
        def flat(cache_arr):
            return jnp.swapaxes(cache_arr, 2, 3).reshape(ROWS, D, cache_arr.shape[2])

        def unflat(arr):
            return jnp.swapaxes(arr.reshape(ROWS, HEADS, 64, LS), 2, 3)

        args = (hidden, flat(self_k), flat(self_v), flat(cross_k), flat(cross_v), positions, enc_mask, rel_bias,
                expert_idx, ln_self, ln_cross, ln_ffn,
                wq_self.T, wk_self.T, wv_self.T, wo_self.T, wq_cross.T, wo_cross.T, w_router.T,
                jnp.swapaxes(w_in, 1, 2), w_out)
        specs = [any_spec] * len(args)
        V = pltpu.VMEM
        scratch = [
            V((ROWS, D, LC), BF16), V((ROWS, D, LC), BF16), V((NDEV, 192, D), BF16), V((NDEV, 192, D), BF16),
            V((ROWS, LC), jnp.int32), V((HEADS, LS), F32), V((D,), F32), V((D,), F32), V((D,), F32), V((256, D), BF16),
            V((NDEV, ROWS, D), BF16), V((NDEV, ROWS, 128), BF16), V((NDEV, ROWS, 256), BF16), V((NDEV, ROWS, 256), BF16),
            V((4, 2, CB // 2, D), BF16), V((4, 2, CB // 2, D), BF16), V((4, 2, CB // 2, D), BF16), V((NDEV, 1, D), F32),
            V((4, ROWS, D), BF16), V((4, 4 * ROWS, 256), BF16), V((4, ROWS, 256), BF16), V((4, ROWS, 256), BF16),
            V((4, ROWS, D), BF16), V((NDEV, CB, 128), BF16), V((3, 2, 8, ROWS, 256), F32), V((3, 8, ROWS, 256), F32),
            V((3, 8, ROWS, 256), F32), V((3, 8, ROWS, 256), F32),
            V((ROWS, HPAD, LS), F32), V((ROWS, HPAD, LS), F32), V((ROWS, HPAD, LC), F32), V((ROWS, D), F32),
            V((NDEV * ROWS, D), F32), V((NDEV * ROWS, D), BF16), V((NDEV * ROWS, NDEV * 192), BF16),
            V((ROWS, D, LS), BF16), V((ROWS, D, LS), BF16), V((4, ROWS, D), BF16), V((ROWS, HPAD, D), BF16),
            pltpu.SMEM((ROWS,), jnp.int32), pltpu.SMEM((ROWS,), jnp.int32),
            pltpu.SemaphoreType.DMA((24,)), pltpu.SemaphoreType.DMA((22,)), pltpu.SemaphoreType.DMA((22,)),
            pltpu.SemaphoreType.DMA((2, 8)), pltpu.SemaphoreType.DMA((2, 8)),
        ]
        h_out, k_out, v_out = pl.pallas_call(
            kernel,
            out_shape=(V((ROWS, D), BF16), V((ROWS, D, LS), BF16), V((ROWS, D, LS), BF16)),
            in_specs=specs,
            out_specs=(vmem, vmem, vmem),
            scratch_shapes=scratch,
            compiler_params=pltpu.CompilerParams(collective_id=0, has_side_effects=True,
                                                 vmem_limit_bytes=67043328 - 2 * 3145728 - 16384),
        )(*args)
        outs = (jax.ShapeDtypeStruct((ROWS, D), BF16), jax.ShapeDtypeStruct((ROWS, D, LS), BF16),
                jax.ShapeDtypeStruct((ROWS, D, LS), BF16))
        h_out, k_out, v_out = pl.pallas_call(
            store, out_shape=outs, in_specs=[vmem] * 3, out_specs=(any_spec,) * 3,
            scratch_shapes=[pltpu.SemaphoreType.DMA((3,))],
            compiler_params=pltpu.CompilerParams(vmem_limit_bytes=4 * 1024 * 1024),
        )(h_out, k_out, v_out)
        return h_out, unflat(k_out), unflat(v_out)

    return jax.shard_map(block, mesh=mesh, in_specs=in_specs, out_specs=out_specs, check_vma=False)
```

```python
import jax
import jax.numpy as jnp
from jax import lax
from jax.experimental import pallas as pl
from jax.experimental.pallas import tpu as pltpu
from jax.sharding import PartitionSpec as P

EPS = 1e-6
NEG = -1e30
F32 = jnp.float32
BF16 = jnp.bfloat16
MESH = pl.DeviceIdType.MESH

ROWS = 8
D = 768
HEADS = 12
HPAD = 16
LS = 192
LC = 384
NDEV = 16
CB = 48
NT = (((1,), (1,)), ((), ()))

ALL_OFFS = [(kz, ky, kc) for kz in (2, 3, 1, 0) for ky in (1, 0) for kc in (1, 0) if (kz, ky, kc) != (0, 0, 0)]
CHIP_OFFS = [off for off in ALL_OFFS if off[2] == 0]
SIBLING = (0, 0, 1)
SUB_OFFS = [(0, 1, 1), (0, 1, 0), (0, 0, 1)]
Z_OFFS = [(2, 0, 0), (3, 0, 0), (1, 0, 0)]


def dot_nt(a, b, **kw):
    return lax.dot_general(a, b, NT, preferred_element_type=F32, **kw)


def iota(shape, axis):
    return lax.broadcasted_iota(jnp.int32, shape, axis)


def rms(x, g):
    inv = lax.rsqrt(jnp.mean(x * x, axis=-1, keepdims=True) + EPS)
    return (x * inv * g).astype(BF16)


def head_mask():
    row = iota((HPAD, D), 0) * 64
    col = iota((HPAD, D), 1)
    return (col >= row) & (col < row + 64)


def attention(q8, k_ref, v_ref, bias_of, s_ref, ctx_ref, q_ref, patch=None):
    hm = head_mask()
    for b in range(ROWS):
        qb = jnp.where(hm, jnp.broadcast_to(q8[b:b + 1, :], (HPAD, D)), 0.0).astype(BF16)
        q_ref[b] = qb
    if patch is not None:
        k8, v8, hit_of = patch
        new = dot_nt(q_ref[...].reshape(ROWS * HPAD, D), k8.astype(BF16))
        row = iota((ROWS * HPAD, ROWS), 0)
        col = iota((ROWS * HPAD, ROWS), 1) * HPAD
        new = jnp.sum(jnp.where((row >= col) & (row < col + HPAD), new, 0.0), axis=-1, keepdims=True)
    for b in range(ROWS):
        sb = jnp.dot(q_ref[b], k_ref[b], preferred_element_type=F32)
        if patch is not None:
            sb = jnp.where(hit_of(b), new[b * HPAD:(b + 1) * HPAD], sb)
        s_ref[b] = sb + bias_of(b)
    s = s_ref[...]
    p = jnp.exp(s - jnp.max(s, axis=-1, keepdims=True))
    s_ref[...] = p / jnp.sum(p, axis=-1, keepdims=True)
    for b in range(ROWS):
        pb = s_ref[b].astype(BF16)
        if patch is None:
            cb = dot_nt(pb, v_ref[b])
        else:
            pf = pb.astype(F32)
            hit = hit_of(b)
            at_pos = jnp.sum(jnp.where(hit, pf, 0.0), axis=-1, keepdims=True)
            cb = dot_nt(jnp.where(hit, 0.0, pf).astype(BF16), v_ref[b]) + at_pos * v8[b:b + 1, :]
        ctx_ref[b:b + 1, :] = jnp.sum(jnp.where(hm, cb, 0.0), axis=0, keepdims=True)


def kernel(hid, kT, vT, ckT, cvT, pos, mask, rel, idx, ln1, ln2, ln3, wq, wk, wv, wo, wqc, woc, wr, win, wout,
           out_h, k_v, v_v,
           ck_v, cv_v, win_v, wout_v, mask_v, rel_v, ln1_v, ln2_v, ln3_v, wqkv, m1, ix, st2, r2, wgo, wgq, wgc, rw,
           c3, r4, st5, r5, c6, r7, st8, r8, st9, r9, bias_s, s_self, s_cross, ctx_v, h2_v, x3_v, u_v,
           k_old, v_old, hs, q_v, pos_s, idx_s, ld, snd, rcv, direct, fwd):
    me = lax.axis_index('ws')
    dpi = lax.axis_index('dp')
    z = me // 4
    s = me % 4
    y = s // 2
    c = s % 2

    z_near = (z, z + 1 - 2 * (z % 2), 2 - z // 2, 3 * (1 - z // 2))
    chip = me // 2

    def chip_of(dist, ky):
        return z_near[dist] * 2 + (y + ky) % 2

    near_first = [(dist, ky) for dist in range(4) for ky in (0, 1)][1:]

    def peer_of(off):
        kz, ky, kc = off
        return ((z + kz) % 4) * 4 + ((y + ky) % 2) * 2 + (c + kc) % 2

    def send(src, dst, ph, off):
        pltpu.make_async_remote_copy(src_ref=src, dst_ref=dst, send_sem=snd.at[ph], recv_sem=rcv.at[ph],
                                     device_id={'ws': peer_of(off)}, device_id_type=MESH).start()

    def desc(buf, ph):
        return pltpu.make_async_remote_copy(src_ref=buf, dst_ref=buf, send_sem=snd.at[ph], recv_sem=rcv.at[ph],
                                            device_id={'ws': me}, device_id_type=MESH)

    def gather_start(buf, ph, row):
        for dist, ky in near_first[::-1]:
            pltpu.make_async_remote_copy(src_ref=buf.at[me], dst_ref=buf.at[me], send_sem=snd.at[ph],
                                         recv_sem=direct.at[row, chip],
                                         device_id={'ws': chip_of(dist, ky) * 2 + c}, device_id_type=MESH).start()
        gather_pass(buf, ph, row, me, chip)

    def gather_pass(buf, ph, row, src, src_chip):
        pltpu.make_async_remote_copy(src_ref=buf.at[src], dst_ref=buf.at[src], send_sem=snd.at[ph],
                                     recv_sem=fwd.at[row, src_chip],
                                     device_id={'ws': peer_of(SIBLING)}, device_id_type=MESH).start()

    def arrived(buf, ph, sem):
        pltpu.make_async_remote_copy(src_ref=buf.at[0], dst_ref=buf.at[0], send_sem=snd.at[ph], recv_sem=sem,
                                     device_id={'ws': me}, device_id_type=MESH).wait_recv()

    def gather_step(buf, ph, row, dist, ky):
        src_chip = chip_of(dist, ky)
        arrived(buf, ph, direct.at[row, src_chip])
        gather_pass(buf, ph, row, src_chip * 2 + c, src_chip)

    def subgroup(buf, ph):
        for off in SUB_OFFS:
            send(buf.at[s], buf.at[s], ph, off)

    def weight_start(w, ph):
        for off in Z_OFFS:
            send(w.at[z, dpi], w.at[z, dpi], ph, off)

    def weight_pass(w, ph):
        desc(w.at[pl.ds(0, 3), 0], ph).wait_recv()
        for kz in (1, 2, 3):
            src = (z + kz) % 4
            pltpu.make_async_remote_copy(src_ref=w.at[src, dpi], dst_ref=w.at[src, dpi], send_sem=snd.at[ph + 11],
                                         recv_sem=rcv.at[ph + 11], device_id={'dp': 1 - dpi, 'ws': me},
                                         device_id_type=MESH).start()

    def weight_finish(w, ph):
        desc(w.at[pl.ds(0, 3), 0], ph + 11).wait_recv()

    bar = pltpu.get_barrier_semaphore()
    pl.semaphore_signal(bar, inc=1, device_id={'dp': 1 - dpi, 'ws': me}, device_id_type=MESH)
    for off in ALL_OFFS:
        pl.semaphore_signal(bar, inc=1, device_id={'ws': peer_of(off)}, device_id_type=MESH)

    loads = {}

    def load(name, src, dst):
        cp = pltpu.make_async_copy(src, dst, ld.at[len(loads)])
        cp.start()
        loads[name] = cp

    load('hid', hid, hs.at[s])
    load('ln1', ln1, ln1_v)
    load('pos', pos, pos_s)
    load('idx', idx, idx_s)
    load('wq', wq, wqkv.at[pl.ds(0, CB)])
    load('wk', wk, wqkv.at[pl.ds(CB, CB)])
    load('wv', wv, wqkv.at[pl.ds(2 * CB, CB)])
    load('ln2', ln2, ln2_v)
    load('ln3', ln3, ln3_v)
    load('rel', rel, rel_v)
    load('mask', mask, mask_v)
    load('wr', wr, rw.at[me])
    load('wo0', wo.at[pl.ds(0, CB // 2)], wgo.at[z, 0])
    load('wo1', wo.at[pl.ds(CB // 2, CB // 2)], wgo.at[z, 1])
    load('wqc0', wqc.at[pl.ds(0, CB // 2)], wgq.at[z, 0])
    load('wqc1', wqc.at[pl.ds(CB // 2, CB // 2)], wgq.at[z, 1])
    load('woc0', woc.at[pl.ds(0, CB // 2)], wgc.at[z, 0])
    load('woc1', woc.at[pl.ds(CB // 2, CB // 2)], wgc.at[z, 1])

    wqkv[3 * CB:256, :] = jnp.zeros((256 - 3 * CB, D), BF16)
    loads['hid'].wait()
    loads['ln1'].wait()
    m1[me] = rms(hs[s].astype(F32), ln1_v[...].reshape(1, D))
    pl.semaphore_wait(bar, NDEV)

    gather_start(m1, 0, 0)
    loads['wo0'].wait()
    loads['wo1'].wait()
    weight_start(wgo, 8)
    subgroup(hs, 7)
    load('k', kT, k_old)
    load('v', vT, v_old)
    loads['pos'].wait()
    loads['idx'].wait()
    row8 = iota((ROWS, 128), 0)
    idx_own = jnp.zeros((ROWS, 128), jnp.int32)
    for i in range(ROWS):
        idx_own = jnp.where(row8 == i, idx_s[i], idx_own)
    idx_own = idx_own.astype(F32)
    ix[me] = idx_own.astype(BF16)

    loads['rel'].wait()
    loads['mask'].wait()
    rel_f = rel_v[...]
    rel_hi = rel_f.astype(BF16)
    rem = rel_f - rel_hi.astype(F32)
    rel_mid = rem.astype(BF16)
    rel_lo = (rem - rel_mid.astype(F32)).astype(BF16)
    src_i = iota((LS, LS), 0)
    dst_i = iota((LS, LS), 1)
    lane12 = iota((HEADS, LS), 1)
    bias_s[...] = jnp.zeros((ROWS, HPAD, LS), F32)
    for b in range(ROWS):
        pick = jnp.where(src_i + dst_i == pos_s[b], 1.0, 0.0).astype(BF16)
        bb = jnp.dot(rel_hi, pick, preferred_element_type=F32)
        bb = bb + jnp.dot(rel_mid, pick, preferred_element_type=F32)
        bb = bb + jnp.dot(rel_lo, pick, preferred_element_type=F32)
        bias_s[b, 0:HEADS, :] = jnp.where(lane12 <= pos_s[b], bb, NEG)
    for name in ('wq', 'wk', 'wv', 'ln2', 'ln3', 'wr', 'wqc0', 'wqc1', 'woc0', 'woc1'):
        loads[name].wait()

    for dist, ky in near_first:
        gather_step(m1, 0, 0, dist, ky)
    for dist in range(4):
        for ky in (0, 1):
            arrived(m1, 0, fwd.at[0, chip_of(dist, ky)])
    xn = m1[...].astype(F32).reshape(NDEV * ROWS, D).astype(BF16)
    st2[...] = dot_nt(xn, wqkv[...]).reshape(NDEV, ROWS, 256).astype(BF16)
    r2[me] = st2[me]
    for off in ALL_OFFS:
        send(st2.at[peer_of(off)], r2.at[me], 1, off)
    weight_start(wgq, 9)
    weight_start(wgc, 10)
    load('ck', ckT, ck_v)
    load('cv', cvT, cv_v)

    sel_r = iota((4 * CB, D), 0)
    sel_q = ((sel_r >= CB).astype(jnp.int32) + (sel_r >= 2 * CB).astype(jnp.int32)
             + (sel_r >= 3 * CB).astype(jnp.int32))
    sel = (iota((4 * CB, D), 1) == sel_r + sel_q * (4 * CB - CB) + s * CB)
    sel = jnp.where(sel, 1.0, 0.0).astype(BF16)
    desc(hs.at[pl.ds(0, 3)], 7).wait_recv()
    h_sub = hs[...].astype(F32).reshape(4 * ROWS, D).astype(BF16)
    h_blk = dot_nt(h_sub, sel)

    loads['k'].wait()
    loads['v'].wait()
    desc(r2.at[pl.ds(0, NDEV - 1)], 1).wait_recv()
    weight_pass(wgo, 8)
    rv = r2[...].astype(F32)

    def columns(lo):
        return jnp.concatenate([rv[d, :, lo:lo + CB] for d in range(NDEV)], axis=-1)

    q8 = columns(0)
    k8 = columns(CB)
    v8 = columns(2 * CB)
    lane_h = iota((HPAD, LS), 1)
    attention(q8, k_old, v_old, lambda b: bias_s[b], s_self, ctx_v, q_v,
              (k8, v8, lambda b: lane_h == pos_s[b]))

    def update(new, old, out):
        cols = new.T
        lane_s = iota((D, LS), 1)
        for b in range(ROWS):
            out[b] = jnp.where(lane_s == pos_s[b], jnp.broadcast_to(cols[:, b:b + 1], (D, LS)),
                               old[b].astype(F32)).astype(BF16)

    def natural(pieces):
        return jnp.concatenate([pieces[t][:, q * CB:(q + 1) * CB] for q in range(4) for t in range(4)], axis=-1)

    def unpack(blk):
        tail = jnp.concatenate([blk[32:48, 0:64], blk[32:48, 64:128]], axis=0)
        return jnp.concatenate([blk[0:32, :], tail], axis=-1)

    c3[s] = ctx_v[...].astype(BF16)
    subgroup(c3, 2)
    update(k8, k_old, k_v)
    weight_pass(wgq, 9)
    for off in ALL_OFFS:
        send(ix.at[me], ix.at[me], 12, off)
        send(rw.at[me], rw.at[me], 11, off)
    update(v8, v_old, v_v)
    load('win', win, win_v)
    load('wout', wout, wout_v)
    desc(c3.at[pl.ds(0, 3)], 2).wait_recv()
    weight_finish(wgo, 8)
    ctx = c3[...].astype(F32).reshape(4 * ROWS, D).astype(BF16)
    h1_blk = (h_blk + dot_nt(ctx, wgo[...].reshape(4 * CB, D))).astype(BF16)
    r4[s, :, 0:4 * CB] = h1_blk
    subgroup(r4, 3)
    desc(r4.at[pl.ds(0, 3)], 3).wait_recv()
    weight_finish(wgq, 9)
    r4f = r4[...].astype(F32)
    h1 = natural([r4f[t] for t in range(4)])
    x2 = rms(h1, ln2_v[...].reshape(1, D))
    st5[:, :, 0:4 * CB] = dot_nt(x2, wgq[...].reshape(4 * CB, D)).reshape(4, ROWS, 4 * CB).astype(BF16)
    r5[s] = st5[s]
    for off in SUB_OFFS:
        kz, ky, kc = off
        send(st5.at[((y + ky) % 2) * 2 + (c + kc) % 2], r5.at[s], 4, off)
    weight_pass(wgc, 10)
    loads['ck'].wait()
    loads['cv'].wait()
    desc(r5.at[pl.ds(0, 3)], 4).wait_recv()
    r5f = r5[...].astype(F32)
    q2 = natural([r5f[t] for t in range(4)])
    attention(q2, ck_v, cv_v, lambda b: jnp.where(mask_v[b:b + 1, :] == 1, 0.0, NEG), s_cross, ctx_v, q_v)

    c6[s] = ctx_v[...].astype(BF16)
    subgroup(c6, 5)
    desc(c6.at[pl.ds(0, 3)], 5).wait_recv()
    weight_finish(wgc, 10)
    ctx2 = c6[...].astype(F32).reshape(4 * ROWS, D).astype(BF16)
    h2_blk = (h1_blk.astype(F32) + dot_nt(ctx2, wgc[...].reshape(4 * CB, D))).astype(BF16)
    h2_f = h2_blk.astype(F32)
    r7[me, 0:32, :] = h2_f[:, 0:128].astype(BF16)
    r7[me, 32:48, :] = jnp.concatenate([h2_f[0:16, 128:192], h2_f[16:32, 128:192]], axis=-1).astype(BF16)

    gather_start(r7, 6, 1)
    desc(ix.at[pl.ds(0, NDEV - 1)], 12).wait_recv()
    idx_all = ix[...].astype(F32).reshape(NDEV * ROWS, 128)
    idx_t = idx_all.T
    earlier = (idx_t[0:ROWS, :] == idx_own) & (iota((ROWS, 128), 1) < me * ROWS + row8)
    slot = jnp.sum(jnp.where(earlier, 1.0, 0.0), axis=-1, keepdims=True)
    loads['win'].wait()
    loads['wout'].wait()
    half_lane = (iota((64, 384), 1) >= 192).astype(F32)

    def group(dist):
        for ky in (0, 1):
            arrived(r7, 6, fwd.at[1, chip_of(dist, ky)])
        t = z_near[dist]
        h2g = natural([unpack(r7[4 * t + u].astype(F32)) for u in range(4)])
        h2_v[32 * dist:32 * dist + 32, :] = h2g
        x3_v[32 * dist:32 * dist + 32, :] = rms(h2g, ln3_v[...].reshape(1, D))

    def hidden_units(hf):
        rows = pl.ds(64 * hf, 64)
        x3 = x3_v[rows, :]
        idx_h = jnp.concatenate([ix[pl.ds(4 * z_near[2 * hf + i], 4)].astype(F32).reshape(32, 128) for i in (0, 1)],
                                axis=0)
        idx3 = jnp.concatenate([idx_h, idx_h, idx_h], axis=-1)
        for p in range(8):
            hh = dot_nt(x3, win_v[2 * p:2 * p + 2].reshape(384, D))
            kept = idx3 == half_lane + float(2 * p)
            u_v[rows, 384 * p:384 * p + 384] = jnp.where(kept, jnp.maximum(hh, 0.0), 0.0).astype(BF16)

    def partial(hf, n):
        yn = jnp.dot(u_v[pl.ds(64 * hf, 64), :], wout_v[:, :, 256 * n:256 * n + 256].reshape(NDEV * 192, 256),
                     preferred_element_type=F32).reshape(4, 2, ROWS, 256)
        st8[hf, n, 0] = yn[:, 0]
        st8[hf, n, 1] = yn[:, 1]
        send(st8.at[hf, n, 1 - c], r8.at[hf, n], 22 + 3 * hf + n, SIBLING)

    def reduce_send(hf, n):
        desc(r8.at[hf, n], 22 + 3 * hf + n).wait_recv()
        st9[hf, n] = st8[hf, n, c] + r8[hf, n]
        for dist in (2 * hf + 1, 2 * hf):
            for ky in ((1,) if dist == 0 else (1, 0)):
                part = 2 * (dist - 2 * hf) + (y + ky) % 2
                ph = 28 + 3 * hf + n
                pltpu.make_async_remote_copy(src_ref=st9.at[hf, n, part], dst_ref=r9.at[n, chip],
                                             send_sem=snd.at[ph], recv_sem=rcv.at[ph],
                                             device_id={'ws': chip_of(dist, ky) * 2 + c}, device_id_type=MESH).start()
        if hf == 0:
            r9[n, chip] = st9[0, n, y]

    for dist, ky in near_first[:3]:
        gather_step(r7, 6, 1, dist, ky)
    group(0)
    group(1)
    hidden_units(0)
    for dist, ky in near_first[3:]:
        gather_step(r7, 6, 1, dist, ky)
    for n in range(3):
        partial(0, n)
    group(2)
    group(3)
    hidden_units(1)
    for n in range(3):
        partial(1, n)
    for n in range(3):
        reduce_send(0, n)
    for n in range(3):
        reduce_send(1, n)

    desc(rw.at[pl.ds(0, NDEV - 1)], 11).wait_recv()
    h2_own = h2_v[pl.ds(pl.multiple_of(s * ROWS, ROWS), ROWS), :]
    x3_own = rms(h2_own, ln3_v[...].reshape(1, D)).astype(F32)
    logits = dot_nt(x3_own, rw[...].reshape(NDEV, D), precision=lax.Precision.HIGHEST)
    ex = jnp.exp(logits - jnp.max(logits, axis=-1, keepdims=True))
    probs = ex / jnp.sum(ex, axis=-1, keepdims=True)
    mine = iota((ROWS, NDEV), 1).astype(F32) == idx_own[:, 0:NDEV]
    gate = jnp.sum(jnp.where(mine, probs, 0.0), axis=-1, keepdims=True)
    gate = jnp.where(slot < float(NDEV), gate, 0.0)

    for n in range(3):
        desc(r9.at[n, pl.ds(0, 3)], 28 + n).wait_recv()
        desc(r9.at[n, pl.ds(0, 4)], 31 + n).wait_recv()
    yv = jnp.concatenate([jnp.sum(r9[n], axis=0) for n in range(3)], axis=-1).astype(BF16).astype(F32)
    out_h[...] = (h2_own + yv * gate).astype(BF16)

    for buf, ph in ((m1, 0), (st2, 1), (r7, 6), (rw, 11), (ix, 12)):
        desc(buf.at[pl.ds(0, NDEV - 1)], ph).wait_send()
    for n in range(3):
        desc(r9.at[n, pl.ds(0, 3)], 28 + n).wait_send()
        desc(r9.at[n, pl.ds(0, 4)], 31 + n).wait_send()
        desc(r8.at[0, n], 22 + n).wait_send()
        desc(r8.at[1, n], 25 + n).wait_send()
    for buf, ph in ((c3, 2), (r4, 3), (st5, 4), (c6, 5), (hs, 7)):
        desc(buf.at[pl.ds(0, 3)], ph).wait_send()
    for w, ph in ((wgo, 8), (wgq, 9), (wgc, 10)):
        desc(w.at[pl.ds(0, 3), 0], ph).wait_send()
        desc(w.at[pl.ds(0, 3), 0], ph + 11).wait_send()


def store(h_in, k_in, v_in, h_out, k_out, v_out, sem):
    copies = [pltpu.make_async_copy(src, dst, sem.at[i])
              for i, (src, dst) in enumerate(((k_in, k_out), (v_in, v_out), (h_in, h_out)))]
    for cp in copies:
        cp.start()
    for cp in copies:
        cp.wait()


def solution(mesh):
    rows = ('dp', 'ws')
    row_vec = P(rows)
    row_mat = P(rows, None)
    cache = P(rows, None, None, None)
    col = P(None, 'ws')
    in_specs = (row_mat, cache, cache, cache, cache, row_vec, row_mat, P(None, None), row_vec,
                P(None), P(None), P(None), col, col, col, col, col, col,
                col, P(None, None, 'ws'), P(None, 'ws', None))
    out_specs = (row_mat, cache, cache)

    any_spec = pl.BlockSpec(memory_space=pltpu.HBM)
    vmem = pl.BlockSpec(memory_space=pltpu.VMEM)

    def block(hidden, self_k, self_v, cross_k, cross_v, positions, enc_mask, rel_bias, expert_idx,
              ln_self, ln_cross, ln_ffn, wq_self, wk_self, wv_self, wo_self, wq_cross, wo_cross,
              w_router, w_in, w_out):
        def flat(cache_arr):
            return jnp.swapaxes(cache_arr, 2, 3).reshape(ROWS, D, cache_arr.shape[2])

        def unflat(arr):
            return jnp.swapaxes(arr.reshape(ROWS, HEADS, 64, LS), 2, 3)

        args = (hidden, flat(self_k), flat(self_v), flat(cross_k), flat(cross_v), positions, enc_mask, rel_bias,
                expert_idx, ln_self, ln_cross, ln_ffn,
                wq_self.T, wk_self.T, wv_self.T, wo_self.T, wq_cross.T, wo_cross.T, w_router.T,
                jnp.swapaxes(w_in, 1, 2), w_out)
        specs = [any_spec] * len(args)
        V = pltpu.VMEM
        scratch = [
            V((ROWS, D, LC), BF16), V((ROWS, D, LC), BF16), V((NDEV, 192, D), BF16), V((NDEV, 192, D), BF16),
            V((ROWS, LC), jnp.int32), V((HEADS, LS), F32), V((D,), F32), V((D,), F32), V((D,), F32), V((256, D), BF16),
            V((NDEV, ROWS, D), BF16), V((NDEV, ROWS, 128), BF16), V((NDEV, ROWS, 256), BF16), V((NDEV, ROWS, 256), BF16),
            V((4, 2, CB // 2, D), BF16), V((4, 2, CB // 2, D), BF16), V((4, 2, CB // 2, D), BF16), V((NDEV, 1, D), F32),
            V((4, ROWS, D), BF16), V((4, 4 * ROWS, 256), BF16), V((4, ROWS, 256), BF16), V((4, ROWS, 256), BF16),
            V((4, ROWS, D), BF16), V((NDEV, CB, 128), BF16), V((2, 3, 2, 4, ROWS, 256), F32), V((2, 3, 4, ROWS, 256), F32),
            V((2, 3, 4, ROWS, 256), F32), V((3, 8, ROWS, 256), F32),
            V((ROWS, HPAD, LS), F32), V((ROWS, HPAD, LS), F32), V((ROWS, HPAD, LC), F32), V((ROWS, D), F32),
            V((NDEV * ROWS, D), F32), V((NDEV * ROWS, D), BF16), V((NDEV * ROWS, NDEV * 192), BF16),
            V((ROWS, D, LS), BF16), V((ROWS, D, LS), BF16), V((4, ROWS, D), BF16), V((ROWS, HPAD, D), BF16),
            pltpu.SMEM((ROWS,), jnp.int32), pltpu.SMEM((ROWS,), jnp.int32),
            pltpu.SemaphoreType.DMA((24,)), pltpu.SemaphoreType.DMA((34,)), pltpu.SemaphoreType.DMA((34,)),
            pltpu.SemaphoreType.DMA((2, 8)), pltpu.SemaphoreType.DMA((2, 8)),
        ]
        h_out, k_out, v_out = pl.pallas_call(
            kernel,
            out_shape=(V((ROWS, D), BF16), V((ROWS, D, LS), BF16), V((ROWS, D, LS), BF16)),
            in_specs=specs,
            out_specs=(vmem, vmem, vmem),
            scratch_shapes=scratch,
            compiler_params=pltpu.CompilerParams(collective_id=0, has_side_effects=True,
                                                 vmem_limit_bytes=67043328 - 2 * 3145728 - 16384),
        )(*args)
        outs = (jax.ShapeDtypeStruct((ROWS, D), BF16), jax.ShapeDtypeStruct((ROWS, D, LS), BF16),
                jax.ShapeDtypeStruct((ROWS, D, LS), BF16))
        h_out, k_out, v_out = pl.pallas_call(
            store, out_shape=outs, in_specs=[vmem] * 3, out_specs=(any_spec,) * 3,
            scratch_shapes=[pltpu.SemaphoreType.DMA((3,))],
            compiler_params=pltpu.CompilerParams(vmem_limit_bytes=4 * 1024 * 1024),
        )(h_out, k_out, v_out)
        return h_out, unflat(k_out), unflat(v_out)

    return jax.shard_map(block, mesh=mesh, in_specs=in_specs, out_specs=out_specs, check_vma=False)
```

```python
import jax
import jax.numpy as jnp
from jax import lax
from jax.experimental import pallas as pl
from jax.experimental.pallas import tpu as pltpu
from jax.sharding import PartitionSpec as P

EPS = 1e-6
NEG = -1e30
F32 = jnp.float32
BF16 = jnp.bfloat16
MESH = pl.DeviceIdType.MESH

ROWS = 8
D = 768
HEADS = 12
HPAD = 16
LS = 192
LC = 384
NDEV = 16
CB = 48
NT = (((1,), (1,)), ((), ()))

ALL_OFFS = [(kz, ky, kc) for kz in (2, 3, 1, 0) for ky in (1, 0) for kc in (1, 0) if (kz, ky, kc) != (0, 0, 0)]
CHIP_OFFS = [off for off in ALL_OFFS if off[2] == 0]
SIBLING = (0, 0, 1)
SUB_OFFS = [(0, 1, 1), (0, 1, 0), (0, 0, 1)]
Z_OFFS = [(2, 0, 0), (3, 0, 0), (1, 0, 0)]


def dot_nt(a, b, **kw):
    return lax.dot_general(a, b, NT, preferred_element_type=F32, **kw)


def iota(shape, axis):
    return lax.broadcasted_iota(jnp.int32, shape, axis)


def rms(x, g):
    inv = lax.rsqrt(jnp.mean(x * x, axis=-1, keepdims=True) + EPS)
    return (x * inv * g).astype(BF16)


def head_mask():
    row = iota((HPAD, D), 0) * 64
    col = iota((HPAD, D), 1)
    return (col >= row) & (col < row + 64)


def attention(q8, k_ref, v_ref, bias_of, s_ref, ctx_ref, q_ref, patch=None):
    hm = head_mask()
    for b in range(ROWS):
        qb = jnp.where(hm, jnp.broadcast_to(q8[b:b + 1, :], (HPAD, D)), 0.0).astype(BF16)
        q_ref[b] = qb
    if patch is not None:
        k8, v8, hit_of = patch
        new = dot_nt(q_ref[...].reshape(ROWS * HPAD, D), k8.astype(BF16))
        row = iota((ROWS * HPAD, ROWS), 0)
        col = iota((ROWS * HPAD, ROWS), 1) * HPAD
        new = jnp.sum(jnp.where((row >= col) & (row < col + HPAD), new, 0.0), axis=-1, keepdims=True)
    for b in range(ROWS):
        sb = jnp.dot(q_ref[b], k_ref[b], preferred_element_type=F32)
        if patch is not None:
            sb = jnp.where(hit_of(b), new[b * HPAD:(b + 1) * HPAD], sb)
        s_ref[b] = sb + bias_of(b)
    s = s_ref[...]
    p = jnp.exp(s - jnp.max(s, axis=-1, keepdims=True))
    s_ref[...] = p / jnp.sum(p, axis=-1, keepdims=True)
    for b in range(ROWS):
        pb = s_ref[b].astype(BF16)
        if patch is None:
            cb = dot_nt(pb, v_ref[b])
        else:
            pf = pb.astype(F32)
            hit = hit_of(b)
            at_pos = jnp.sum(jnp.where(hit, pf, 0.0), axis=-1, keepdims=True)
            cb = dot_nt(jnp.where(hit, 0.0, pf).astype(BF16), v_ref[b]) + at_pos * v8[b:b + 1, :]
        ctx_ref[b:b + 1, :] = jnp.sum(jnp.where(hm, cb, 0.0), axis=0, keepdims=True)


def kernel(hid, kT, vT, ckT, cvT, pos, mask, rel, idx, ln1, ln2, ln3, wq, wk, wv, wo, wqc, woc, wr, win, wout,
           out_h, k_v, v_v,
           ck_v, cv_v, win_v, wout_v, mask_v, rel_v, ln1_v, ln2_v, ln3_v, wqkv, m1, ix, st2, r2, wgo, wgq, wgc, rw,
           c3, r4, st5, r5, c6, r7, st8, r8, st9, r9, bias_s, s_self, s_cross, ctx_v, h2_v, x3_v, u_v,
           k_old, v_old, hs, q_v, pos_s, idx_s, ld, snd, rcv, direct, fwd):
    me = lax.axis_index('ws')
    dpi = lax.axis_index('dp')
    z = me // 4
    s = me % 4
    y = s // 2
    c = s % 2

    z_near = (z, z + 1 - 2 * (z % 2), 2 - z // 2, 3 * (1 - z // 2))
    chip = me // 2

    def chip_of(dist, ky):
        return z_near[dist] * 2 + (y + ky) % 2

    near_first = [(dist, ky) for dist in range(4) for ky in (0, 1)][1:]

    def far_first():
        return [chip_of(dist, ky) * 2 + (c + kc) % 2 for dist in (3, 2, 1, 0) for ky in (1, 0) for kc in (1, 0)][:-1]

    def peer_of(off):
        kz, ky, kc = off
        return ((z + kz) % 4) * 4 + ((y + ky) % 2) * 2 + (c + kc) % 2

    def send(src, dst, ph, off):
        send_to(src, dst, ph, peer_of(off))

    def send_to(src, dst, ph, dev):
        pltpu.make_async_remote_copy(src_ref=src, dst_ref=dst, send_sem=snd.at[ph], recv_sem=rcv.at[ph],
                                     device_id={'ws': dev}, device_id_type=MESH).start()

    def desc(buf, ph):
        return pltpu.make_async_remote_copy(src_ref=buf, dst_ref=buf, send_sem=snd.at[ph], recv_sem=rcv.at[ph],
                                            device_id={'ws': me}, device_id_type=MESH)

    def gather_start(buf, ph, row):
        for dist, ky in near_first[::-1]:
            pltpu.make_async_remote_copy(src_ref=buf.at[me], dst_ref=buf.at[me], send_sem=snd.at[ph],
                                         recv_sem=direct.at[row, chip],
                                         device_id={'ws': chip_of(dist, ky) * 2 + c}, device_id_type=MESH).start()
        gather_pass(buf, ph, row, me, chip)

    def gather_pass(buf, ph, row, src, src_chip):
        pltpu.make_async_remote_copy(src_ref=buf.at[src], dst_ref=buf.at[src], send_sem=snd.at[ph],
                                     recv_sem=fwd.at[row, src_chip],
                                     device_id={'ws': peer_of(SIBLING)}, device_id_type=MESH).start()

    def arrived(buf, ph, sem):
        pltpu.make_async_remote_copy(src_ref=buf.at[0], dst_ref=buf.at[0], send_sem=snd.at[ph], recv_sem=sem,
                                     device_id={'ws': me}, device_id_type=MESH).wait_recv()

    def gather_step(buf, ph, row, dist, ky):
        src_chip = chip_of(dist, ky)
        arrived(buf, ph, direct.at[row, src_chip])
        gather_pass(buf, ph, row, src_chip * 2 + c, src_chip)

    def subgroup(buf, ph):
        for off in SUB_OFFS:
            send(buf.at[s], buf.at[s], ph, off)

    def weight_start(w, ph):
        for off in Z_OFFS:
            send(w.at[z, dpi], w.at[z, dpi], ph, off)

    def weight_pass(w, ph):
        desc(w.at[pl.ds(0, 3), 0], ph).wait_recv()
        for kz in (1, 2, 3):
            src = (z + kz) % 4
            pltpu.make_async_remote_copy(src_ref=w.at[src, dpi], dst_ref=w.at[src, dpi], send_sem=snd.at[ph + 11],
                                         recv_sem=rcv.at[ph + 11], device_id={'dp': 1 - dpi, 'ws': me},
                                         device_id_type=MESH).start()

    def weight_finish(w, ph):
        desc(w.at[pl.ds(0, 3), 0], ph + 11).wait_recv()

    bar = pltpu.get_barrier_semaphore()
    pl.semaphore_signal(bar, inc=1, device_id={'dp': 1 - dpi, 'ws': me}, device_id_type=MESH)
    for off in ALL_OFFS:
        pl.semaphore_signal(bar, inc=1, device_id={'ws': peer_of(off)}, device_id_type=MESH)

    loads = {}

    def load(name, src, dst):
        cp = pltpu.make_async_copy(src, dst, ld.at[len(loads)])
        cp.start()
        loads[name] = cp

    load('hid', hid, hs.at[s])
    load('ln1', ln1, ln1_v)
    load('pos', pos, pos_s)
    load('idx', idx, idx_s)
    load('wq', wq, wqkv.at[pl.ds(0, CB)])
    load('wk', wk, wqkv.at[pl.ds(CB, CB)])
    load('wv', wv, wqkv.at[pl.ds(2 * CB, CB)])
    load('ln2', ln2, ln2_v)
    load('ln3', ln3, ln3_v)
    load('rel', rel, rel_v)
    load('mask', mask, mask_v)
    load('wr', wr, rw.at[me])
    load('wo0', wo.at[pl.ds(0, CB // 2)], wgo.at[z, 0])
    load('wo1', wo.at[pl.ds(CB // 2, CB // 2)], wgo.at[z, 1])
    load('wqc0', wqc.at[pl.ds(0, CB // 2)], wgq.at[z, 0])
    load('wqc1', wqc.at[pl.ds(CB // 2, CB // 2)], wgq.at[z, 1])
    load('woc0', woc.at[pl.ds(0, CB // 2)], wgc.at[z, 0])
    load('woc1', woc.at[pl.ds(CB // 2, CB // 2)], wgc.at[z, 1])

    wqkv[3 * CB:256, :] = jnp.zeros((256 - 3 * CB, D), BF16)
    loads['hid'].wait()
    loads['ln1'].wait()
    m1[me] = rms(hs[s].astype(F32), ln1_v[...].reshape(1, D))
    pl.semaphore_wait(bar, NDEV)

    gather_start(m1, 0, 0)
    loads['wo0'].wait()
    loads['wo1'].wait()
    weight_start(wgo, 8)
    subgroup(hs, 7)
    load('k', kT, k_old)
    load('v', vT, v_old)
    loads['pos'].wait()
    loads['idx'].wait()
    row8 = iota((ROWS, 128), 0)
    idx_own = jnp.zeros((ROWS, 128), jnp.int32)
    for i in range(ROWS):
        idx_own = jnp.where(row8 == i, idx_s[i], idx_own)
    idx_own = idx_own.astype(F32)
    ix[me] = idx_own.astype(BF16)

    loads['rel'].wait()
    loads['mask'].wait()
    rel_f = rel_v[...]
    rel_hi = rel_f.astype(BF16)
    rem = rel_f - rel_hi.astype(F32)
    rel_mid = rem.astype(BF16)
    rel_lo = (rem - rel_mid.astype(F32)).astype(BF16)
    src_i = iota((LS, LS), 0)
    dst_i = iota((LS, LS), 1)
    lane12 = iota((HEADS, LS), 1)
    bias_s[...] = jnp.zeros((ROWS, HPAD, LS), F32)
    for b in range(ROWS):
        pick = jnp.where(src_i + dst_i == pos_s[b], 1.0, 0.0).astype(BF16)
        bb = jnp.dot(rel_hi, pick, preferred_element_type=F32)
        bb = bb + jnp.dot(rel_mid, pick, preferred_element_type=F32)
        bb = bb + jnp.dot(rel_lo, pick, preferred_element_type=F32)
        bias_s[b, 0:HEADS, :] = jnp.where(lane12 <= pos_s[b], bb, NEG)
    for name in ('wq', 'wk', 'wv', 'ln2', 'ln3', 'wr', 'wqc0', 'wqc1', 'woc0', 'woc1'):
        loads[name].wait()

    for dist, ky in near_first:
        gather_step(m1, 0, 0, dist, ky)
    for dist in range(4):
        for ky in (0, 1):
            arrived(m1, 0, fwd.at[0, chip_of(dist, ky)])
    xn = m1[...].astype(F32).reshape(NDEV * ROWS, D).astype(BF16)
    st2[...] = dot_nt(xn, wqkv[...]).reshape(NDEV, ROWS, 256).astype(BF16)
    r2[me] = st2[me]
    for dev in far_first():
        send_to(st2.at[dev], r2.at[me], 1, dev)
    weight_start(wgq, 9)
    load('ck', ckT, ck_v)
    load('cv', cvT, cv_v)

    sel_r = iota((4 * CB, D), 0)
    sel_q = ((sel_r >= CB).astype(jnp.int32) + (sel_r >= 2 * CB).astype(jnp.int32)
             + (sel_r >= 3 * CB).astype(jnp.int32))
    sel = (iota((4 * CB, D), 1) == sel_r + sel_q * (4 * CB - CB) + s * CB)
    sel = jnp.where(sel, 1.0, 0.0).astype(BF16)
    desc(hs.at[pl.ds(0, 3)], 7).wait_recv()
    h_sub = hs[...].astype(F32).reshape(4 * ROWS, D).astype(BF16)
    h_blk = dot_nt(h_sub, sel)

    loads['k'].wait()
    loads['v'].wait()
    desc(r2.at[pl.ds(0, NDEV - 1)], 1).wait_recv()
    weight_pass(wgo, 8)
    weight_start(wgc, 10)
    rv = r2[...].astype(F32)

    def columns(lo):
        return jnp.concatenate([rv[d, :, lo:lo + CB] for d in range(NDEV)], axis=-1)

    q8 = columns(0)
    k8 = columns(CB)
    v8 = columns(2 * CB)
    lane_h = iota((HPAD, LS), 1)
    attention(q8, k_old, v_old, lambda b: bias_s[b], s_self, ctx_v, q_v,
              (k8, v8, lambda b: lane_h == pos_s[b]))

    def update(new, old, out):
        cols = new.T
        lane_s = iota((D, LS), 1)
        for b in range(ROWS):
            out[b] = jnp.where(lane_s == pos_s[b], jnp.broadcast_to(cols[:, b:b + 1], (D, LS)),
                               old[b].astype(F32)).astype(BF16)

    def natural(pieces):
        return jnp.concatenate([pieces[t][:, q * CB:(q + 1) * CB] for q in range(4) for t in range(4)], axis=-1)

    def pack(buf, i, blk):
        buf[i, 0:32, :] = blk[:, 0:128].astype(BF16)
        buf[i, 32:48, :] = jnp.concatenate([blk[0:16, 128:192], blk[16:32, 128:192]], axis=-1).astype(BF16)

    def unpack(blk):
        tail = jnp.concatenate([blk[32:48, 0:64], blk[32:48, 64:128]], axis=0)
        return jnp.concatenate([blk[0:32, :], tail], axis=-1)

    c3[s] = ctx_v[...].astype(BF16)
    subgroup(c3, 2)
    update(k8, k_old, k_v)
    weight_pass(wgq, 9)
    for off in ALL_OFFS:
        send(ix.at[me], ix.at[me], 12, off)
        send(rw.at[me], rw.at[me], 11, off)
    update(v8, v_old, v_v)
    load('win', win, win_v)
    load('wout', wout, wout_v)
    desc(c3.at[pl.ds(0, 3)], 2).wait_recv()
    weight_finish(wgo, 8)
    ctx = c3[...].astype(F32).reshape(4 * ROWS, D).astype(BF16)
    h1_blk = (h_blk + dot_nt(ctx, wgo[...].reshape(4 * CB, D))).astype(BF16)
    pack(r4, s, h1_blk.astype(F32))
    subgroup(r4, 3)
    desc(r4.at[pl.ds(0, 3)], 3).wait_recv()
    weight_finish(wgq, 9)
    r4f = r4[...].astype(F32)
    h1 = natural([unpack(r4f[t]) for t in range(4)])
    x2 = rms(h1, ln2_v[...].reshape(1, D))
    st5[:, :, 0:4 * CB] = dot_nt(x2, wgq[...].reshape(4 * CB, D)).reshape(4, ROWS, 4 * CB).astype(BF16)
    r5[s] = st5[s]
    for off in SUB_OFFS:
        kz, ky, kc = off
        send(st5.at[((y + ky) % 2) * 2 + (c + kc) % 2], r5.at[s], 4, off)
    weight_pass(wgc, 10)
    loads['ck'].wait()
    loads['cv'].wait()
    desc(r5.at[pl.ds(0, 3)], 4).wait_recv()
    r5f = r5[...].astype(F32)
    q2 = natural([r5f[t] for t in range(4)])
    attention(q2, ck_v, cv_v, lambda b: jnp.where(mask_v[b:b + 1, :] == 1, 0.0, NEG), s_cross, ctx_v, q_v)

    c6[s] = ctx_v[...].astype(BF16)
    subgroup(c6, 5)
    desc(c6.at[pl.ds(0, 3)], 5).wait_recv()
    weight_finish(wgc, 10)
    ctx2 = c6[...].astype(F32).reshape(4 * ROWS, D).astype(BF16)
    h2_blk = (h1_blk.astype(F32) + dot_nt(ctx2, wgc[...].reshape(4 * CB, D))).astype(BF16)
    pack(r7, me, h2_blk.astype(F32))

    gather_start(r7, 6, 1)
    desc(ix.at[pl.ds(0, NDEV - 1)], 12).wait_recv()
    idx_all = ix[...].astype(F32).reshape(NDEV * ROWS, 128)
    idx_t = idx_all.T
    earlier = (idx_t[0:ROWS, :] == idx_own) & (iota((ROWS, 128), 1) < me * ROWS + row8)
    slot = jnp.sum(jnp.where(earlier, 1.0, 0.0), axis=-1, keepdims=True)
    loads['win'].wait()
    loads['wout'].wait()

    def group(dist):
        for ky in (0, 1):
            arrived(r7, 6, fwd.at[1, chip_of(dist, ky)])
        t = z_near[dist]
        h2g = natural([unpack(r7[4 * t + u].astype(F32)) for u in range(4)])
        at = pl.ds(pl.multiple_of(32 * t, 32), 32)
        h2_v[at, :] = h2g
        x3_v[at, :] = rms(h2g, ln3_v[...].reshape(1, D))

    for dist, ky in near_first[:5]:
        gather_step(r7, 6, 1, dist, ky)
    group(0)
    gather_step(r7, 6, 1, *near_first[5])
    gather_step(r7, 6, 1, *near_first[6])
    group(1)
    group(2)
    group(3)
    x3 = x3_v[...]
    idx3 = jnp.concatenate([idx_all, idx_all, idx_all], axis=-1)
    half = (iota((NDEV * ROWS, 384), 1) >= 192).astype(F32)
    for p in range(8):
        hh = dot_nt(x3, win_v[2 * p:2 * p + 2].reshape(384, D))
        u_v[:, 384 * p:384 * p + 384] = jnp.where(idx3 == half + float(2 * p), jnp.maximum(hh, 0.0), 0.0).astype(BF16)
    def partial(n):
        yn = jnp.dot(u_v[...], wout_v[:, :, 256 * n:256 * n + 256].reshape(NDEV * 192, 256),
                     preferred_element_type=F32).reshape(8, 2, ROWS, 256)
        st8[n, 0] = yn[:, 0]
        st8[n, 1] = yn[:, 1]
        send(st8.at[n, 1 - c], r8.at[n], 13 + n, SIBLING)

    def reduce_send(n):
        desc(r8.at[n], 13 + n).wait_recv()
        st9[n] = st8[n, c] + r8[n]
        for dist, ky in near_first[::-1]:
            dest = chip_of(dist, ky)
            send_to(st9.at[n, dest], r9.at[n, chip], 16 + n, dest * 2 + c)
        r9[n, chip] = st9[n, chip]

    partial(0)
    partial(1)
    partial(2)
    reduce_send(0)
    reduce_send(1)
    reduce_send(2)

    desc(rw.at[pl.ds(0, NDEV - 1)], 11).wait_recv()
    h2_own = h2_v[pl.ds(pl.multiple_of(me * ROWS, ROWS), ROWS), :]
    x3_own = rms(h2_own, ln3_v[...].reshape(1, D)).astype(F32)
    logits = dot_nt(x3_own, rw[...].reshape(NDEV, D), precision=lax.Precision.HIGHEST)
    ex = jnp.exp(logits - jnp.max(logits, axis=-1, keepdims=True))
    probs = ex / jnp.sum(ex, axis=-1, keepdims=True)
    mine = iota((ROWS, NDEV), 1).astype(F32) == idx_own[:, 0:NDEV]
    gate = jnp.sum(jnp.where(mine, probs, 0.0), axis=-1, keepdims=True)
    gate = jnp.where(slot < float(NDEV), gate, 0.0)

    for n in range(3):
        desc(r9.at[n, pl.ds(0, 7)], 16 + n).wait_recv()
    yv = jnp.concatenate([jnp.sum(r9[n], axis=0) for n in range(3)], axis=-1).astype(BF16).astype(F32)
    out_h[...] = (h2_own + yv * gate).astype(BF16)

    for buf, ph in ((m1, 0), (st2, 1), (r7, 6), (rw, 11), (ix, 12)):
        desc(buf.at[pl.ds(0, NDEV - 1)], ph).wait_send()
    for n in range(3):
        desc(st9.at[n, pl.ds(0, 7)], 16 + n).wait_send()
        desc(r8.at[n], 13 + n).wait_send()
    for buf, ph in ((c3, 2), (r4, 3), (st5, 4), (c6, 5), (hs, 7)):
        desc(buf.at[pl.ds(0, 3)], ph).wait_send()
    for w, ph in ((wgo, 8), (wgq, 9), (wgc, 10)):
        desc(w.at[pl.ds(0, 3), 0], ph).wait_send()
        desc(w.at[pl.ds(0, 3), 0], ph + 11).wait_send()


def store(h_in, k_in, v_in, h_out, k_out, v_out, sem):
    copies = [pltpu.make_async_copy(src, dst, sem.at[i])
              for i, (src, dst) in enumerate(((k_in, k_out), (v_in, v_out), (h_in, h_out)))]
    for cp in copies:
        cp.start()
    for cp in copies:
        cp.wait()


def solution(mesh):
    rows = ('dp', 'ws')
    row_vec = P(rows)
    row_mat = P(rows, None)
    cache = P(rows, None, None, None)
    col = P(None, 'ws')
    in_specs = (row_mat, cache, cache, cache, cache, row_vec, row_mat, P(None, None), row_vec,
                P(None), P(None), P(None), col, col, col, col, col, col,
                col, P(None, None, 'ws'), P(None, 'ws', None))
    out_specs = (row_mat, cache, cache)

    any_spec = pl.BlockSpec(memory_space=pltpu.HBM)
    vmem = pl.BlockSpec(memory_space=pltpu.VMEM)

    def block(hidden, self_k, self_v, cross_k, cross_v, positions, enc_mask, rel_bias, expert_idx,
              ln_self, ln_cross, ln_ffn, wq_self, wk_self, wv_self, wo_self, wq_cross, wo_cross,
              w_router, w_in, w_out):
        def flat(cache_arr):
            return jnp.swapaxes(cache_arr, 2, 3).reshape(ROWS, D, cache_arr.shape[2])

        def unflat(arr):
            return jnp.swapaxes(arr.reshape(ROWS, HEADS, 64, LS), 2, 3)

        args = (hidden, flat(self_k), flat(self_v), flat(cross_k), flat(cross_v), positions, enc_mask, rel_bias,
                expert_idx, ln_self, ln_cross, ln_ffn,
                wq_self.T, wk_self.T, wv_self.T, wo_self.T, wq_cross.T, wo_cross.T, w_router.T,
                jnp.swapaxes(w_in, 1, 2), w_out)
        specs = [any_spec] * len(args)
        V = pltpu.VMEM
        scratch = [
            V((ROWS, D, LC), BF16), V((ROWS, D, LC), BF16), V((NDEV, 192, D), BF16), V((NDEV, 192, D), BF16),
            V((ROWS, LC), jnp.int32), V((HEADS, LS), F32), V((D,), F32), V((D,), F32), V((D,), F32), V((256, D), BF16),
            V((NDEV, ROWS, D), BF16), V((NDEV, ROWS, 128), BF16), V((NDEV, ROWS, 256), BF16), V((NDEV, ROWS, 256), BF16),
            V((4, 2, CB // 2, D), BF16), V((4, 2, CB // 2, D), BF16), V((4, 2, CB // 2, D), BF16), V((NDEV, 1, D), F32),
            V((4, ROWS, D), BF16), V((4, CB, 128), BF16), V((4, ROWS, 256), BF16), V((4, ROWS, 256), BF16),
            V((4, ROWS, D), BF16), V((NDEV, CB, 128), BF16), V((3, 2, 8, ROWS, 256), F32), V((3, 8, ROWS, 256), F32),
            V((3, 8, ROWS, 256), F32), V((3, 8, ROWS, 256), F32),
            V((ROWS, HPAD, LS), F32), V((ROWS, HPAD, LS), F32), V((ROWS, HPAD, LC), F32), V((ROWS, D), F32),
            V((NDEV * ROWS, D), F32), V((NDEV * ROWS, D), BF16), V((NDEV * ROWS, NDEV * 192), BF16),
            V((ROWS, D, LS), BF16), V((ROWS, D, LS), BF16), V((4, ROWS, D), BF16), V((ROWS, HPAD, D), BF16),
            pltpu.SMEM((ROWS,), jnp.int32), pltpu.SMEM((ROWS,), jnp.int32),
            pltpu.SemaphoreType.DMA((24,)), pltpu.SemaphoreType.DMA((22,)), pltpu.SemaphoreType.DMA((22,)),
            pltpu.SemaphoreType.DMA((2, 8)), pltpu.SemaphoreType.DMA((2, 8)),
        ]
        h_out, k_out, v_out = pl.pallas_call(
            kernel,
            out_shape=(V((ROWS, D), BF16), V((ROWS, D, LS), BF16), V((ROWS, D, LS), BF16)),
            in_specs=specs,
            out_specs=(vmem, vmem, vmem),
            scratch_shapes=scratch,
            compiler_params=pltpu.CompilerParams(collective_id=0, has_side_effects=True,
                                                 vmem_limit_bytes=67043328 - 2 * 3145728 - 16384),
        )(*args)
        outs = (jax.ShapeDtypeStruct((ROWS, D), BF16), jax.ShapeDtypeStruct((ROWS, D, LS), BF16),
                jax.ShapeDtypeStruct((ROWS, D, LS), BF16))
        h_out, k_out, v_out = pl.pallas_call(
            store, out_shape=outs, in_specs=[vmem] * 3, out_specs=(any_spec,) * 3,
            scratch_shapes=[pltpu.SemaphoreType.DMA((3,))],
            compiler_params=pltpu.CompilerParams(vmem_limit_bytes=4 * 1024 * 1024),
        )(h_out, k_out, v_out)
        return h_out, unflat(k_out), unflat(v_out)

    return jax.shard_map(block, mesh=mesh, in_specs=in_specs, out_specs=out_specs, check_vma=False)
```

```python
import jax
import jax.numpy as jnp
from jax import lax
from jax.experimental import pallas as pl
from jax.experimental.pallas import tpu as pltpu
from jax.sharding import PartitionSpec as P

EPS = 1e-6
NEG = -1e30
F32 = jnp.float32
BF16 = jnp.bfloat16
MESH = pl.DeviceIdType.MESH

ROWS = 8
D = 768
HEADS = 12
HPAD = 16
LS = 192
LC = 384
NDEV = 16
CB = 48
NT = (((1,), (1,)), ((), ()))

ALL_OFFS = [(kz, ky, kc) for kz in (2, 3, 1, 0) for ky in (1, 0) for kc in (1, 0) if (kz, ky, kc) != (0, 0, 0)]
CHIP_OFFS = [off for off in ALL_OFFS if off[2] == 0]
SIBLING = (0, 0, 1)
SUB_OFFS = [(0, 1, 1), (0, 1, 0), (0, 0, 1)]
Z_OFFS = [(2, 0, 0), (3, 0, 0), (1, 0, 0)]


def dot_nt(a, b, **kw):
    return lax.dot_general(a, b, NT, preferred_element_type=F32, **kw)


def iota(shape, axis):
    return lax.broadcasted_iota(jnp.int32, shape, axis)


def rms(x, g):
    inv = lax.rsqrt(jnp.mean(x * x, axis=-1, keepdims=True) + EPS)
    return (x * inv * g).astype(BF16)


def head_mask():
    row = iota((HPAD, D), 0) * 64
    col = iota((HPAD, D), 1)
    return (col >= row) & (col < row + 64)


def attention(q8, k_ref, v_ref, bias_of, s_ref, ctx_ref, q_ref, patch=None):
    hm = head_mask()
    for b in range(ROWS):
        qb = jnp.where(hm, jnp.broadcast_to(q8[b:b + 1, :], (HPAD, D)), 0.0).astype(BF16)
        q_ref[b] = qb
    if patch is not None:
        k8, v8, hit_of = patch
        new = dot_nt(q_ref[...].reshape(ROWS * HPAD, D), k8.astype(BF16))
        row = iota((ROWS * HPAD, ROWS), 0)
        col = iota((ROWS * HPAD, ROWS), 1) * HPAD
        new = jnp.sum(jnp.where((row >= col) & (row < col + HPAD), new, 0.0), axis=-1, keepdims=True)
    for b in range(ROWS):
        sb = jnp.dot(q_ref[b], k_ref[b], preferred_element_type=F32)
        if patch is not None:
            sb = jnp.where(hit_of(b), new[b * HPAD:(b + 1) * HPAD], sb)
        s_ref[b] = sb + bias_of(b)
    s = s_ref[...]
    p = jnp.exp(s - jnp.max(s, axis=-1, keepdims=True))
    s_ref[...] = p / jnp.sum(p, axis=-1, keepdims=True)
    for b in range(ROWS):
        pb = s_ref[b].astype(BF16)
        if patch is None:
            cb = dot_nt(pb, v_ref[b])
        else:
            pf = pb.astype(F32)
            hit = hit_of(b)
            at_pos = jnp.sum(jnp.where(hit, pf, 0.0), axis=-1, keepdims=True)
            cb = dot_nt(jnp.where(hit, 0.0, pf).astype(BF16), v_ref[b]) + at_pos * v8[b:b + 1, :]
        ctx_ref[b:b + 1, :] = jnp.sum(jnp.where(hm, cb, 0.0), axis=0, keepdims=True)


def kernel(hid, kT, vT, ckT, cvT, pos, mask, rel, idx, ln1, ln2, ln3, wq, wk, wv, wo, wqc, woc, wr, win, wout,
           out_h, k_v, v_v,
           ck_v, cv_v, win_v, wout_v, mask_v, rel_v, ln1_v, ln2_v, ln3_v, wqkv, m1, ix, st2, r2, wgo, wgq, wgc, rw,
           c3, r4, st5, r5, c6, r7, st8, r8, st9, r9, bias_s, s_self, s_cross, ctx_v, h2_v, x3_v, u_v,
           k_old, v_old, hs, q_v, pos_s, idx_s, ld, snd, rcv, direct, fwd):
    me = lax.axis_index('ws')
    dpi = lax.axis_index('dp')
    z = me // 4
    s = me % 4
    y = s // 2
    c = s % 2

    z_near = (z, z + 1 - 2 * (z % 2), 2 - z // 2, 3 * (1 - z // 2))
    chip = me // 2

    def chip_of(dist, ky):
        return z_near[dist] * 2 + (y + ky) % 2

    near_first = [(dist, ky) for dist in range(4) for ky in (0, 1)][1:]

    def far_first():
        return [chip_of(dist, ky) * 2 + (c + kc) % 2 for dist in (3, 2, 1, 0) for ky in (1, 0) for kc in (1, 0)][:-1]

    def peer_of(off):
        kz, ky, kc = off
        return ((z + kz) % 4) * 4 + ((y + ky) % 2) * 2 + (c + kc) % 2

    def send(src, dst, ph, off):
        send_to(src, dst, ph, peer_of(off))

    def send_to(src, dst, ph, dev):
        pltpu.make_async_remote_copy(src_ref=src, dst_ref=dst, send_sem=snd.at[ph], recv_sem=rcv.at[ph],
                                     device_id={'ws': dev}, device_id_type=MESH).start()

    def desc(buf, ph):
        return pltpu.make_async_remote_copy(src_ref=buf, dst_ref=buf, send_sem=snd.at[ph], recv_sem=rcv.at[ph],
                                            device_id={'ws': me}, device_id_type=MESH)

    def gather_start(buf, ph, row):
        for dist, ky in near_first[::-1]:
            pltpu.make_async_remote_copy(src_ref=buf.at[me], dst_ref=buf.at[me], send_sem=snd.at[ph],
                                         recv_sem=direct.at[row, chip],
                                         device_id={'ws': chip_of(dist, ky) * 2 + c}, device_id_type=MESH).start()
        gather_pass(buf, ph, row, me, chip)

    def gather_pass(buf, ph, row, src, src_chip):
        pltpu.make_async_remote_copy(src_ref=buf.at[src], dst_ref=buf.at[src], send_sem=snd.at[ph],
                                     recv_sem=fwd.at[row, src_chip],
                                     device_id={'ws': peer_of(SIBLING)}, device_id_type=MESH).start()

    def arrived(buf, ph, sem):
        pltpu.make_async_remote_copy(src_ref=buf.at[0], dst_ref=buf.at[0], send_sem=snd.at[ph], recv_sem=sem,
                                     device_id={'ws': me}, device_id_type=MESH).wait_recv()

    def gather_step(buf, ph, row, dist, ky):
        src_chip = chip_of(dist, ky)
        arrived(buf, ph, direct.at[row, src_chip])
        gather_pass(buf, ph, row, src_chip * 2 + c, src_chip)

    def subgroup(buf, ph):
        for off in SUB_OFFS:
            send(buf.at[s], buf.at[s], ph, off)

    def weight_start(w, ph):
        for off in Z_OFFS:
            send(w.at[z, dpi], w.at[z, dpi], ph, off)

    def weight_pass(w, ph):
        desc(w.at[pl.ds(0, 3), 0], ph).wait_recv()
        for kz in (1, 2, 3):
            src = (z + kz) % 4
            pltpu.make_async_remote_copy(src_ref=w.at[src, dpi], dst_ref=w.at[src, dpi], send_sem=snd.at[ph + 11],
                                         recv_sem=rcv.at[ph + 11], device_id={'dp': 1 - dpi, 'ws': me},
                                         device_id_type=MESH).start()

    def weight_finish(w, ph):
        desc(w.at[pl.ds(0, 3), 0], ph + 11).wait_recv()

    bar = pltpu.get_barrier_semaphore()
    pl.semaphore_signal(bar, inc=1, device_id={'dp': 1 - dpi, 'ws': me}, device_id_type=MESH)
    for off in ALL_OFFS:
        pl.semaphore_signal(bar, inc=1, device_id={'ws': peer_of(off)}, device_id_type=MESH)

    loads = {}

    def load(name, src, dst):
        cp = pltpu.make_async_copy(src, dst, ld.at[len(loads)])
        cp.start()
        loads[name] = cp

    load('hid', hid, hs.at[s])
    load('ln1', ln1, ln1_v)
    load('pos', pos, pos_s)
    load('idx', idx, idx_s)
    load('wq', wq, wqkv.at[pl.ds(0, CB)])
    load('wk', wk, wqkv.at[pl.ds(CB, CB)])
    load('wv', wv, wqkv.at[pl.ds(2 * CB, CB)])
    load('ln2', ln2, ln2_v)
    load('ln3', ln3, ln3_v)
    load('rel', rel, rel_v)
    load('mask', mask, mask_v)
    load('wr', wr, rw.at[me])
    load('wo0', wo.at[pl.ds(0, CB // 2)], wgo.at[z, 0])
    load('wo1', wo.at[pl.ds(CB // 2, CB // 2)], wgo.at[z, 1])
    load('wqc0', wqc.at[pl.ds(0, CB // 2)], wgq.at[z, 0])
    load('wqc1', wqc.at[pl.ds(CB // 2, CB // 2)], wgq.at[z, 1])
    load('woc0', woc.at[pl.ds(0, CB // 2)], wgc.at[z, 0])
    load('woc1', woc.at[pl.ds(CB // 2, CB // 2)], wgc.at[z, 1])

    wqkv[3 * CB:256, :] = jnp.zeros((256 - 3 * CB, D), BF16)
    loads['hid'].wait()
    loads['ln1'].wait()
    m1[me] = rms(hs[s].astype(F32), ln1_v[...].reshape(1, D))
    pl.semaphore_wait(bar, NDEV)

    gather_start(m1, 0, 0)
    loads['wo0'].wait()
    loads['wo1'].wait()
    weight_start(wgo, 8)
    subgroup(hs, 7)
    load('k', kT, k_old)
    load('v', vT, v_old)
    loads['pos'].wait()
    loads['idx'].wait()
    row8 = iota((ROWS, 128), 0)
    idx_own = jnp.zeros((ROWS, 128), jnp.int32)
    for i in range(ROWS):
        idx_own = jnp.where(row8 == i, idx_s[i], idx_own)
    idx_own = idx_own.astype(F32)
    ix[me] = idx_own.astype(BF16)

    loads['rel'].wait()
    loads['mask'].wait()
    rel_f = rel_v[...]
    rel_hi = rel_f.astype(BF16)
    rem = rel_f - rel_hi.astype(F32)
    rel_mid = rem.astype(BF16)
    rel_lo = (rem - rel_mid.astype(F32)).astype(BF16)
    src_i = iota((LS, LS), 0)
    dst_i = iota((LS, LS), 1)
    lane12 = iota((HEADS, LS), 1)
    bias_s[...] = jnp.zeros((ROWS, HPAD, LS), F32)
    for b in range(ROWS):
        pick = jnp.where(src_i + dst_i == pos_s[b], 1.0, 0.0).astype(BF16)
        bb = jnp.dot(rel_hi, pick, preferred_element_type=F32)
        bb = bb + jnp.dot(rel_mid, pick, preferred_element_type=F32)
        bb = bb + jnp.dot(rel_lo, pick, preferred_element_type=F32)
        bias_s[b, 0:HEADS, :] = jnp.where(lane12 <= pos_s[b], bb, NEG)
    for name in ('wq', 'wk', 'wv', 'ln2', 'ln3', 'wr', 'wqc0', 'wqc1', 'woc0', 'woc1'):
        loads[name].wait()

    for dist, ky in near_first:
        gather_step(m1, 0, 0, dist, ky)
    for dist in range(4):
        for ky in (0, 1):
            arrived(m1, 0, fwd.at[0, chip_of(dist, ky)])
    xn = m1[...].astype(F32).reshape(NDEV * ROWS, D).astype(BF16)
    st2[...] = dot_nt(xn, wqkv[...]).reshape(NDEV, ROWS, 256).astype(BF16)
    r2[me] = st2[me]
    for dev in far_first():
        send_to(st2.at[dev], r2.at[me], 1, dev)
    weight_start(wgq, 9)
    load('ck', ckT, ck_v)
    load('cv', cvT, cv_v)

    sel_r = iota((4 * CB, D), 0)
    sel_q = ((sel_r >= CB).astype(jnp.int32) + (sel_r >= 2 * CB).astype(jnp.int32)
             + (sel_r >= 3 * CB).astype(jnp.int32))
    sel = (iota((4 * CB, D), 1) == sel_r + sel_q * (4 * CB - CB) + s * CB)
    sel = jnp.where(sel, 1.0, 0.0).astype(BF16)
    desc(hs.at[pl.ds(0, 3)], 7).wait_recv()
    h_sub = hs[...].astype(F32).reshape(4 * ROWS, D).astype(BF16)
    h_blk = dot_nt(h_sub, sel)

    weight_pass(wgo, 8)
    loads['k'].wait()
    loads['v'].wait()
    desc(r2.at[pl.ds(0, NDEV - 1)], 1).wait_recv()
    weight_start(wgc, 10)
    rv = r2[...].astype(F32)

    def columns(lo):
        return jnp.concatenate([rv[d, :, lo:lo + CB] for d in range(NDEV)], axis=-1)

    q8 = columns(0)
    k8 = columns(CB)
    v8 = columns(2 * CB)
    lane_h = iota((HPAD, LS), 1)
    attention(q8, k_old, v_old, lambda b: bias_s[b], s_self, ctx_v, q_v,
              (k8, v8, lambda b: lane_h == pos_s[b]))

    def update(new, old, out):
        cols = new.T
        lane_s = iota((D, LS), 1)
        for b in range(ROWS):
            out[b] = jnp.where(lane_s == pos_s[b], jnp.broadcast_to(cols[:, b:b + 1], (D, LS)),
                               old[b].astype(F32)).astype(BF16)

    def natural(pieces):
        return jnp.concatenate([pieces[t][:, q * CB:(q + 1) * CB] for q in range(4) for t in range(4)], axis=-1)

    def pack(buf, i, blk):
        buf[i, 0:32, :] = blk[:, 0:128].astype(BF16)
        buf[i, 32:48, :] = jnp.concatenate([blk[0:16, 128:192], blk[16:32, 128:192]], axis=-1).astype(BF16)

    def unpack(blk):
        tail = jnp.concatenate([blk[32:48, 0:64], blk[32:48, 64:128]], axis=0)
        return jnp.concatenate([blk[0:32, :], tail], axis=-1)

    c3[s] = ctx_v[...].astype(BF16)
    subgroup(c3, 2)
    weight_pass(wgq, 9)
    update(k8, k_old, k_v)
    for off in ALL_OFFS:
        send(ix.at[me], ix.at[me], 12, off)
        send(rw.at[me], rw.at[me], 11, off)
    update(v8, v_old, v_v)
    load('win', win, win_v)
    load('wout', wout, wout_v)
    desc(c3.at[pl.ds(0, 3)], 2).wait_recv()
    weight_finish(wgo, 8)
    ctx = c3[...].astype(F32).reshape(4 * ROWS, D).astype(BF16)
    h1_blk = (h_blk + dot_nt(ctx, wgo[...].reshape(4 * CB, D))).astype(BF16)
    pack(r4, s, h1_blk.astype(F32))
    subgroup(r4, 3)
    desc(r4.at[pl.ds(0, 3)], 3).wait_recv()
    weight_finish(wgq, 9)
    r4f = r4[...].astype(F32)
    h1 = natural([unpack(r4f[t]) for t in range(4)])
    x2 = rms(h1, ln2_v[...].reshape(1, D))
    st5[:, :, 0:4 * CB] = dot_nt(x2, wgq[...].reshape(4 * CB, D)).reshape(4, ROWS, 4 * CB).astype(BF16)
    r5[s] = st5[s]
    for off in SUB_OFFS:
        kz, ky, kc = off
        send(st5.at[((y + ky) % 2) * 2 + (c + kc) % 2], r5.at[s], 4, off)
    weight_pass(wgc, 10)
    loads['ck'].wait()
    loads['cv'].wait()
    desc(r5.at[pl.ds(0, 3)], 4).wait_recv()
    r5f = r5[...].astype(F32)
    q2 = natural([r5f[t] for t in range(4)])
    attention(q2, ck_v, cv_v, lambda b: jnp.where(mask_v[b:b + 1, :] == 1, 0.0, NEG), s_cross, ctx_v, q_v)

    c6[s] = ctx_v[...].astype(BF16)
    subgroup(c6, 5)
    desc(c6.at[pl.ds(0, 3)], 5).wait_recv()
    weight_finish(wgc, 10)
    ctx2 = c6[...].astype(F32).reshape(4 * ROWS, D).astype(BF16)
    h2_blk = (h1_blk.astype(F32) + dot_nt(ctx2, wgc[...].reshape(4 * CB, D))).astype(BF16)
    pack(r7, me, h2_blk.astype(F32))

    gather_start(r7, 6, 1)
    desc(ix.at[pl.ds(0, NDEV - 1)], 12).wait_recv()
    idx_all = ix[...].astype(F32).reshape(NDEV * ROWS, 128)
    idx_t = idx_all.T
    earlier = (idx_t[0:ROWS, :] == idx_own) & (iota((ROWS, 128), 1) < me * ROWS + row8)
    slot = jnp.sum(jnp.where(earlier, 1.0, 0.0), axis=-1, keepdims=True)
    loads['win'].wait()
    loads['wout'].wait()

    def group(dist):
        for ky in (0, 1):
            arrived(r7, 6, fwd.at[1, chip_of(dist, ky)])
        t = z_near[dist]
        h2g = natural([unpack(r7[4 * t + u].astype(F32)) for u in range(4)])
        at = pl.ds(pl.multiple_of(32 * t, 32), 32)
        h2_v[at, :] = h2g
        x3_v[at, :] = rms(h2g, ln3_v[...].reshape(1, D))

    for dist, ky in near_first[:5]:
        gather_step(r7, 6, 1, dist, ky)
    group(0)
    gather_step(r7, 6, 1, *near_first[5])
    gather_step(r7, 6, 1, *near_first[6])
    group(1)
    group(2)
    group(3)
    x3 = x3_v[...]
    idx3 = jnp.concatenate([idx_all, idx_all, idx_all], axis=-1)
    half = (iota((NDEV * ROWS, 384), 1) >= 192).astype(F32)
    for p in range(8):
        hh = dot_nt(x3, win_v[2 * p:2 * p + 2].reshape(384, D))
        u_v[:, 384 * p:384 * p + 384] = jnp.where(idx3 == half + float(2 * p), jnp.maximum(hh, 0.0), 0.0).astype(BF16)
    def partial(n):
        yn = jnp.dot(u_v[...], wout_v[:, :, 256 * n:256 * n + 256].reshape(NDEV * 192, 256),
                     preferred_element_type=F32).reshape(8, 2, ROWS, 256)
        st8[n, 0] = yn[:, 0]
        st8[n, 1] = yn[:, 1]
        send(st8.at[n, 1 - c], r8.at[n], 13 + n, SIBLING)

    def reduce_send(n):
        desc(r8.at[n], 13 + n).wait_recv()
        st9[n] = st8[n, c] + r8[n]
        for dist, ky in near_first[::-1]:
            dest = chip_of(dist, ky)
            send_to(st9.at[n, dest], r9.at[n, chip], 16 + n, dest * 2 + c)
        r9[n, chip] = st9[n, chip]

    partial(0)
    partial(1)
    partial(2)
    reduce_send(0)
    reduce_send(1)
    reduce_send(2)

    desc(rw.at[pl.ds(0, NDEV - 1)], 11).wait_recv()
    h2_own = h2_v[pl.ds(pl.multiple_of(me * ROWS, ROWS), ROWS), :]
    x3_own = rms(h2_own, ln3_v[...].reshape(1, D)).astype(F32)
    logits = dot_nt(x3_own, rw[...].reshape(NDEV, D), precision=lax.Precision.HIGHEST)
    ex = jnp.exp(logits - jnp.max(logits, axis=-1, keepdims=True))
    probs = ex / jnp.sum(ex, axis=-1, keepdims=True)
    mine = iota((ROWS, NDEV), 1).astype(F32) == idx_own[:, 0:NDEV]
    gate = jnp.sum(jnp.where(mine, probs, 0.0), axis=-1, keepdims=True)
    gate = jnp.where(slot < float(NDEV), gate, 0.0)

    for n in range(3):
        desc(r9.at[n, pl.ds(0, 7)], 16 + n).wait_recv()
    yv = jnp.concatenate([jnp.sum(r9[n], axis=0) for n in range(3)], axis=-1).astype(BF16).astype(F32)
    out_h[...] = (h2_own + yv * gate).astype(BF16)

    for buf, ph in ((m1, 0), (st2, 1), (r7, 6), (rw, 11), (ix, 12)):
        desc(buf.at[pl.ds(0, NDEV - 1)], ph).wait_send()
    for n in range(3):
        desc(st9.at[n, pl.ds(0, 7)], 16 + n).wait_send()
        desc(r8.at[n], 13 + n).wait_send()
    for buf, ph in ((c3, 2), (r4, 3), (st5, 4), (c6, 5), (hs, 7)):
        desc(buf.at[pl.ds(0, 3)], ph).wait_send()
    for w, ph in ((wgo, 8), (wgq, 9), (wgc, 10)):
        desc(w.at[pl.ds(0, 3), 0], ph).wait_send()
        desc(w.at[pl.ds(0, 3), 0], ph + 11).wait_send()


def store(h_in, k_in, v_in, h_out, k_out, v_out, sem):
    copies = [pltpu.make_async_copy(src, dst, sem.at[i])
              for i, (src, dst) in enumerate(((k_in, k_out), (v_in, v_out), (h_in, h_out)))]
    for cp in copies:
        cp.start()
    for cp in copies:
        cp.wait()


def solution(mesh):
    rows = ('dp', 'ws')
    row_vec = P(rows)
    row_mat = P(rows, None)
    cache = P(rows, None, None, None)
    col = P(None, 'ws')
    in_specs = (row_mat, cache, cache, cache, cache, row_vec, row_mat, P(None, None), row_vec,
                P(None), P(None), P(None), col, col, col, col, col, col,
                col, P(None, None, 'ws'), P(None, 'ws', None))
    out_specs = (row_mat, cache, cache)

    any_spec = pl.BlockSpec(memory_space=pltpu.HBM)
    vmem = pl.BlockSpec(memory_space=pltpu.VMEM)

    def block(hidden, self_k, self_v, cross_k, cross_v, positions, enc_mask, rel_bias, expert_idx,
              ln_self, ln_cross, ln_ffn, wq_self, wk_self, wv_self, wo_self, wq_cross, wo_cross,
              w_router, w_in, w_out):
        def flat(cache_arr):
            return jnp.swapaxes(cache_arr, 2, 3).reshape(ROWS, D, cache_arr.shape[2])

        def unflat(arr):
            return jnp.swapaxes(arr.reshape(ROWS, HEADS, 64, LS), 2, 3)

        args = (hidden, flat(self_k), flat(self_v), flat(cross_k), flat(cross_v), positions, enc_mask, rel_bias,
                expert_idx, ln_self, ln_cross, ln_ffn,
                wq_self.T, wk_self.T, wv_self.T, wo_self.T, wq_cross.T, wo_cross.T, w_router.T,
                jnp.swapaxes(w_in, 1, 2), w_out)
        specs = [any_spec] * len(args)
        V = pltpu.VMEM
        scratch = [
            V((ROWS, D, LC), BF16), V((ROWS, D, LC), BF16), V((NDEV, 192, D), BF16), V((NDEV, 192, D), BF16),
            V((ROWS, LC), jnp.int32), V((HEADS, LS), F32), V((D,), F32), V((D,), F32), V((D,), F32), V((256, D), BF16),
            V((NDEV, ROWS, D), BF16), V((NDEV, ROWS, 128), BF16), V((NDEV, ROWS, 256), BF16), V((NDEV, ROWS, 256), BF16),
            V((4, 2, CB // 2, D), BF16), V((4, 2, CB // 2, D), BF16), V((4, 2, CB // 2, D), BF16), V((NDEV, 1, D), F32),
            V((4, ROWS, D), BF16), V((4, CB, 128), BF16), V((4, ROWS, 256), BF16), V((4, ROWS, 256), BF16),
            V((4, ROWS, D), BF16), V((NDEV, CB, 128), BF16), V((3, 2, 8, ROWS, 256), F32), V((3, 8, ROWS, 256), F32),
            V((3, 8, ROWS, 256), F32), V((3, 8, ROWS, 256), F32),
            V((ROWS, HPAD, LS), F32), V((ROWS, HPAD, LS), F32), V((ROWS, HPAD, LC), F32), V((ROWS, D), F32),
            V((NDEV * ROWS, D), F32), V((NDEV * ROWS, D), BF16), V((NDEV * ROWS, NDEV * 192), BF16),
            V((ROWS, D, LS), BF16), V((ROWS, D, LS), BF16), V((4, ROWS, D), BF16), V((ROWS, HPAD, D), BF16),
            pltpu.SMEM((ROWS,), jnp.int32), pltpu.SMEM((ROWS,), jnp.int32),
            pltpu.SemaphoreType.DMA((24,)), pltpu.SemaphoreType.DMA((22,)), pltpu.SemaphoreType.DMA((22,)),
            pltpu.SemaphoreType.DMA((2, 8)), pltpu.SemaphoreType.DMA((2, 8)),
        ]
        h_out, k_out, v_out = pl.pallas_call(
            kernel,
            out_shape=(V((ROWS, D), BF16), V((ROWS, D, LS), BF16), V((ROWS, D, LS), BF16)),
            in_specs=specs,
            out_specs=(vmem, vmem, vmem),
            scratch_shapes=scratch,
            compiler_params=pltpu.CompilerParams(collective_id=0, has_side_effects=True,
                                                 vmem_limit_bytes=67043328 - 2 * 3145728 - 16384),
        )(*args)
        outs = (jax.ShapeDtypeStruct((ROWS, D), BF16), jax.ShapeDtypeStruct((ROWS, D, LS), BF16),
                jax.ShapeDtypeStruct((ROWS, D, LS), BF16))
        h_out, k_out, v_out = pl.pallas_call(
            store, out_shape=outs, in_specs=[vmem] * 3, out_specs=(any_spec,) * 3,
            scratch_shapes=[pltpu.SemaphoreType.DMA((3,))],
            compiler_params=pltpu.CompilerParams(vmem_limit_bytes=4 * 1024 * 1024),
        )(h_out, k_out, v_out)
        return h_out, unflat(k_out), unflat(v_out)

    return jax.shard_map(block, mesh=mesh, in_specs=in_specs, out_specs=out_specs, check_vma=False)
```

```python
import jax
import jax.numpy as jnp
from jax import lax
from jax.experimental import pallas as pl
from jax.experimental.pallas import tpu as pltpu
from jax.sharding import PartitionSpec as P

EPS = 1e-6
NEG = -1e30
F32 = jnp.float32
BF16 = jnp.bfloat16
MESH = pl.DeviceIdType.MESH

ROWS = 8
D = 768
HEADS = 12
HPAD = 16
LS = 192
LC = 384
NDEV = 16
CB = 48
NT = (((1,), (1,)), ((), ()))

ALL_OFFS = [(kz, ky, kc) for kz in (2, 3, 1, 0) for ky in (1, 0) for kc in (1, 0) if (kz, ky, kc) != (0, 0, 0)]
CHIP_OFFS = [off for off in ALL_OFFS if off[2] == 0]
SIBLING = (0, 0, 1)
SUB_OFFS = [(0, 1, 1), (0, 1, 0), (0, 0, 1)]
Z_OFFS = [(2, 0, 0), (3, 0, 0), (1, 0, 0)]


def dot_nt(a, b, **kw):
    return lax.dot_general(a, b, NT, preferred_element_type=F32, **kw)


def iota(shape, axis):
    return lax.broadcasted_iota(jnp.int32, shape, axis)


def rms(x, g):
    inv = lax.rsqrt(jnp.mean(x * x, axis=-1, keepdims=True) + EPS)
    return (x * inv * g).astype(BF16)


def head_mask():
    row = iota((HPAD, D), 0) * 64
    col = iota((HPAD, D), 1)
    return (col >= row) & (col < row + 64)


def attention(q8, k_ref, v_ref, bias_of, s_ref, ctx_ref, q_ref, patch=None):
    hm = head_mask()
    for b in range(ROWS):
        qb = jnp.where(hm, jnp.broadcast_to(q8[b:b + 1, :], (HPAD, D)), 0.0).astype(BF16)
        q_ref[b] = qb
    if patch is not None:
        k8, v8, hit_of = patch
        new = dot_nt(q_ref[...].reshape(ROWS * HPAD, D), k8.astype(BF16))
        row = iota((ROWS * HPAD, ROWS), 0)
        col = iota((ROWS * HPAD, ROWS), 1) * HPAD
        new = jnp.sum(jnp.where((row >= col) & (row < col + HPAD), new, 0.0), axis=-1, keepdims=True)
    for b in range(ROWS):
        sb = jnp.dot(q_ref[b], k_ref[b], preferred_element_type=F32)
        if patch is not None:
            sb = jnp.where(hit_of(b), new[b * HPAD:(b + 1) * HPAD], sb)
        s_ref[b] = sb + bias_of(b)
    s = s_ref[...]
    p = jnp.exp(s - jnp.max(s, axis=-1, keepdims=True))
    s_ref[...] = p / jnp.sum(p, axis=-1, keepdims=True)
    for b in range(ROWS):
        pb = s_ref[b].astype(BF16)
        if patch is None:
            cb = dot_nt(pb, v_ref[b])
        else:
            pf = pb.astype(F32)
            hit = hit_of(b)
            at_pos = jnp.sum(jnp.where(hit, pf, 0.0), axis=-1, keepdims=True)
            cb = dot_nt(jnp.where(hit, 0.0, pf).astype(BF16), v_ref[b]) + at_pos * v8[b:b + 1, :]
        ctx_ref[b:b + 1, :] = jnp.sum(jnp.where(hm, cb, 0.0), axis=0, keepdims=True)


def kernel(hid, kT, vT, ckT, cvT, pos, mask, rel, idx, ln1, ln2, ln3, wq, wk, wv, wo, wqc, woc, wr, win, wout,
           out_h, k_v, v_v,
           ck_v, cv_v, win_v, wout_v, mask_v, rel_v, ln1_v, ln2_v, ln3_v, wqkv, m1, ix, st2, r2, wgo, wgq, wgc, rw,
           c3, r4, st5, r5, c6, r7, st8, r8, st9, r9, bias_s, s_self, s_cross, ctx_v, h2_v, x3_v, u_v,
           k_old, v_old, hs, q_v, pos_s, idx_s, ld, snd, rcv, direct, fwd):
    me = lax.axis_index('ws')
    dpi = lax.axis_index('dp')
    z = me // 4
    s = me % 4
    y = s // 2
    c = s % 2

    z_near = (z, z + 1 - 2 * (z % 2), 2 - z // 2, 3 * (1 - z // 2))
    chip = me // 2

    def chip_of(dist, ky):
        return z_near[dist] * 2 + (y + ky) % 2

    near_first = [(dist, ky) for dist in range(4) for ky in (0, 1)][1:]

    def far_first():
        return [chip_of(dist, ky) * 2 + (c + kc) % 2 for dist in (3, 2, 1, 0) for ky in (1, 0) for kc in (1, 0)][:-1]

    def peer_of(off):
        kz, ky, kc = off
        return ((z + kz) % 4) * 4 + ((y + ky) % 2) * 2 + (c + kc) % 2

    def send(src, dst, ph, off):
        send_to(src, dst, ph, peer_of(off))

    def send_to(src, dst, ph, dev):
        pltpu.make_async_remote_copy(src_ref=src, dst_ref=dst, send_sem=snd.at[ph], recv_sem=rcv.at[ph],
                                     device_id={'ws': dev}, device_id_type=MESH).start()

    def desc(buf, ph):
        return pltpu.make_async_remote_copy(src_ref=buf, dst_ref=buf, send_sem=snd.at[ph], recv_sem=rcv.at[ph],
                                            device_id={'ws': me}, device_id_type=MESH)

    def gather_start(buf, ph, row):
        for dist, ky in near_first[::-1]:
            pltpu.make_async_remote_copy(src_ref=buf.at[me], dst_ref=buf.at[me], send_sem=snd.at[ph],
                                         recv_sem=direct.at[row, chip],
                                         device_id={'ws': chip_of(dist, ky) * 2 + c}, device_id_type=MESH).start()
        gather_pass(buf, ph, row, me, chip)

    def gather_pass(buf, ph, row, src, src_chip):
        pltpu.make_async_remote_copy(src_ref=buf.at[src], dst_ref=buf.at[src], send_sem=snd.at[ph],
                                     recv_sem=fwd.at[row, src_chip],
                                     device_id={'ws': peer_of(SIBLING)}, device_id_type=MESH).start()

    def arrived(buf, ph, sem):
        pltpu.make_async_remote_copy(src_ref=buf.at[0], dst_ref=buf.at[0], send_sem=snd.at[ph], recv_sem=sem,
                                     device_id={'ws': me}, device_id_type=MESH).wait_recv()

    def gather_step(buf, ph, row, dist, ky):
        src_chip = chip_of(dist, ky)
        arrived(buf, ph, direct.at[row, src_chip])
        gather_pass(buf, ph, row, src_chip * 2 + c, src_chip)

    def subgroup(buf, ph):
        for off in SUB_OFFS:
            send(buf.at[s], buf.at[s], ph, off)

    def weight_start(w, ph):
        for off in Z_OFFS:
            send(w.at[z, dpi], w.at[z, dpi], ph, off)

    def weight_pass(w, ph):
        desc(w.at[pl.ds(0, 3), 0], ph).wait_recv()
        for kz in (1, 2, 3):
            src = (z + kz) % 4
            pltpu.make_async_remote_copy(src_ref=w.at[src, dpi], dst_ref=w.at[src, dpi], send_sem=snd.at[ph + 11],
                                         recv_sem=rcv.at[ph + 11], device_id={'dp': 1 - dpi, 'ws': me},
                                         device_id_type=MESH).start()

    def weight_finish(w, ph):
        desc(w.at[pl.ds(0, 3), 0], ph + 11).wait_recv()

    bar = pltpu.get_barrier_semaphore()
    pl.semaphore_signal(bar, inc=1, device_id={'dp': 1 - dpi, 'ws': me}, device_id_type=MESH)
    for off in ALL_OFFS:
        pl.semaphore_signal(bar, inc=1, device_id={'ws': peer_of(off)}, device_id_type=MESH)

    loads = {}

    def load(name, src, dst):
        cp = pltpu.make_async_copy(src, dst, ld.at[len(loads)])
        cp.start()
        loads[name] = cp

    load('hid', hid, hs.at[s])
    load('ln1', ln1, ln1_v)
    load('pos', pos, pos_s)
    load('idx', idx, idx_s)
    load('wq', wq, wqkv.at[pl.ds(0, CB)])
    load('wk', wk, wqkv.at[pl.ds(CB, CB)])
    load('wv', wv, wqkv.at[pl.ds(2 * CB, CB)])
    load('ln2', ln2, ln2_v)
    load('ln3', ln3, ln3_v)
    load('rel', rel, rel_v)
    load('mask', mask, mask_v)
    load('wr', wr, rw.at[me])
    load('wo0', wo.at[pl.ds(0, CB // 2)], wgo.at[z, 0])
    load('wo1', wo.at[pl.ds(CB // 2, CB // 2)], wgo.at[z, 1])
    load('wqc0', wqc.at[pl.ds(0, CB // 2)], wgq.at[z, 0])
    load('wqc1', wqc.at[pl.ds(CB // 2, CB // 2)], wgq.at[z, 1])
    load('woc0', woc.at[pl.ds(0, CB // 2)], wgc.at[z, 0])
    load('woc1', woc.at[pl.ds(CB // 2, CB // 2)], wgc.at[z, 1])

    wqkv[3 * CB:256, :] = jnp.zeros((256 - 3 * CB, D), BF16)
    loads['hid'].wait()
    loads['ln1'].wait()
    m1[me] = rms(hs[s].astype(F32), ln1_v[...].reshape(1, D))
    pl.semaphore_wait(bar, NDEV)

    gather_start(m1, 0, 0)
    loads['wo0'].wait()
    loads['wo1'].wait()
    subgroup(hs, 7)
    load('k', kT, k_old)
    load('v', vT, v_old)
    loads['pos'].wait()
    loads['idx'].wait()
    row8 = iota((ROWS, 128), 0)
    idx_own = jnp.zeros((ROWS, 128), jnp.int32)
    for i in range(ROWS):
        idx_own = jnp.where(row8 == i, idx_s[i], idx_own)
    idx_own = idx_own.astype(F32)
    ix[me] = idx_own.astype(BF16)

    loads['rel'].wait()
    loads['mask'].wait()
    rel_f = rel_v[...]
    rel_hi = rel_f.astype(BF16)
    rem = rel_f - rel_hi.astype(F32)
    rel_mid = rem.astype(BF16)
    rel_lo = (rem - rel_mid.astype(F32)).astype(BF16)
    src_i = iota((LS, LS), 0)
    dst_i = iota((LS, LS), 1)
    lane12 = iota((HEADS, LS), 1)
    bias_s[...] = jnp.zeros((ROWS, HPAD, LS), F32)
    for b in range(ROWS):
        pick = jnp.where(src_i + dst_i == pos_s[b], 1.0, 0.0).astype(BF16)
        bb = jnp.dot(rel_hi, pick, preferred_element_type=F32)
        bb = bb + jnp.dot(rel_mid, pick, preferred_element_type=F32)
        bb = bb + jnp.dot(rel_lo, pick, preferred_element_type=F32)
        bias_s[b, 0:HEADS, :] = jnp.where(lane12 <= pos_s[b], bb, NEG)
    for name in ('wq', 'wk', 'wv', 'ln2', 'ln3', 'wr', 'wqc0', 'wqc1', 'woc0', 'woc1'):
        loads[name].wait()

    for dist, ky in near_first:
        gather_step(m1, 0, 0, dist, ky)
        if (dist, ky) == (0, 1):
            weight_start(wgo, 8)
    for dist in range(4):
        for ky in (0, 1):
            arrived(m1, 0, fwd.at[0, chip_of(dist, ky)])
    xn = m1[...].astype(F32).reshape(NDEV * ROWS, D).astype(BF16)
    st2[...] = dot_nt(xn, wqkv[...]).reshape(NDEV, ROWS, 256).astype(BF16)
    r2[me] = st2[me]
    for dev in far_first():
        send_to(st2.at[dev], r2.at[me], 1, dev)
    weight_start(wgq, 9)
    load('ck', ckT, ck_v)
    load('cv', cvT, cv_v)

    sel_r = iota((4 * CB, D), 0)
    sel_q = ((sel_r >= CB).astype(jnp.int32) + (sel_r >= 2 * CB).astype(jnp.int32)
             + (sel_r >= 3 * CB).astype(jnp.int32))
    sel = (iota((4 * CB, D), 1) == sel_r + sel_q * (4 * CB - CB) + s * CB)
    sel = jnp.where(sel, 1.0, 0.0).astype(BF16)
    desc(hs.at[pl.ds(0, 3)], 7).wait_recv()
    h_sub = hs[...].astype(F32).reshape(4 * ROWS, D).astype(BF16)
    h_blk = dot_nt(h_sub, sel)

    weight_pass(wgo, 8)
    loads['k'].wait()
    loads['v'].wait()
    desc(r2.at[pl.ds(0, NDEV - 1)], 1).wait_recv()
    weight_start(wgc, 10)
    rv = r2[...].astype(F32)

    def columns(lo):
        return jnp.concatenate([rv[d, :, lo:lo + CB] for d in range(NDEV)], axis=-1)

    q8 = columns(0)
    k8 = columns(CB)
    v8 = columns(2 * CB)
    lane_h = iota((HPAD, LS), 1)
    attention(q8, k_old, v_old, lambda b: bias_s[b], s_self, ctx_v, q_v,
              (k8, v8, lambda b: lane_h == pos_s[b]))

    def update(new, old, out):
        cols = new.T
        lane_s = iota((D, LS), 1)
        for b in range(ROWS):
            out[b] = jnp.where(lane_s == pos_s[b], jnp.broadcast_to(cols[:, b:b + 1], (D, LS)),
                               old[b].astype(F32)).astype(BF16)

    def natural(pieces):
        return jnp.concatenate([pieces[t][:, q * CB:(q + 1) * CB] for q in range(4) for t in range(4)], axis=-1)

    def pack(buf, i, blk):
        buf[i, 0:32, :] = blk[:, 0:128].astype(BF16)
        buf[i, 32:48, :] = jnp.concatenate([blk[0:16, 128:192], blk[16:32, 128:192]], axis=-1).astype(BF16)

    def unpack(blk):
        tail = jnp.concatenate([blk[32:48, 0:64], blk[32:48, 64:128]], axis=0)
        return jnp.concatenate([blk[0:32, :], tail], axis=-1)

    c3[s] = ctx_v[...].astype(BF16)
    subgroup(c3, 2)
    weight_pass(wgq, 9)
    update(k8, k_old, k_v)
    for off in ALL_OFFS:
        send(ix.at[me], ix.at[me], 12, off)
        send(rw.at[me], rw.at[me], 11, off)
    update(v8, v_old, v_v)
    load('win', win, win_v)
    load('wout', wout, wout_v)
    desc(c3.at[pl.ds(0, 3)], 2).wait_recv()
    weight_finish(wgo, 8)
    ctx = c3[...].astype(F32).reshape(4 * ROWS, D).astype(BF16)
    h1_blk = (h_blk + dot_nt(ctx, wgo[...].reshape(4 * CB, D))).astype(BF16)
    pack(r4, s, h1_blk.astype(F32))
    subgroup(r4, 3)
    desc(r4.at[pl.ds(0, 3)], 3).wait_recv()
    weight_finish(wgq, 9)
    r4f = r4[...].astype(F32)
    h1 = natural([unpack(r4f[t]) for t in range(4)])
    x2 = rms(h1, ln2_v[...].reshape(1, D))
    st5[:, :, 0:4 * CB] = dot_nt(x2, wgq[...].reshape(4 * CB, D)).reshape(4, ROWS, 4 * CB).astype(BF16)
    r5[s] = st5[s]
    for off in SUB_OFFS:
        kz, ky, kc = off
        send(st5.at[((y + ky) % 2) * 2 + (c + kc) % 2], r5.at[s], 4, off)
    weight_pass(wgc, 10)
    loads['ck'].wait()
    loads['cv'].wait()
    desc(r5.at[pl.ds(0, 3)], 4).wait_recv()
    r5f = r5[...].astype(F32)
    q2 = natural([r5f[t] for t in range(4)])
    attention(q2, ck_v, cv_v, lambda b: jnp.where(mask_v[b:b + 1, :] == 1, 0.0, NEG), s_cross, ctx_v, q_v)

    c6[s] = ctx_v[...].astype(BF16)
    subgroup(c6, 5)
    desc(c6.at[pl.ds(0, 3)], 5).wait_recv()
    weight_finish(wgc, 10)
    ctx2 = c6[...].astype(F32).reshape(4 * ROWS, D).astype(BF16)
    h2_blk = (h1_blk.astype(F32) + dot_nt(ctx2, wgc[...].reshape(4 * CB, D))).astype(BF16)
    pack(r7, me, h2_blk.astype(F32))

    gather_start(r7, 6, 1)
    desc(ix.at[pl.ds(0, NDEV - 1)], 12).wait_recv()
    idx_all = ix[...].astype(F32).reshape(NDEV * ROWS, 128)
    idx_t = idx_all.T
    earlier = (idx_t[0:ROWS, :] == idx_own) & (iota((ROWS, 128), 1) < me * ROWS + row8)
    slot = jnp.sum(jnp.where(earlier, 1.0, 0.0), axis=-1, keepdims=True)
    loads['win'].wait()
    loads['wout'].wait()

    def group(dist):
        for ky in (0, 1):
            arrived(r7, 6, fwd.at[1, chip_of(dist, ky)])
        t = z_near[dist]
        h2g = natural([unpack(r7[4 * t + u].astype(F32)) for u in range(4)])
        at = pl.ds(pl.multiple_of(32 * t, 32), 32)
        h2_v[at, :] = h2g
        x3_v[at, :] = rms(h2g, ln3_v[...].reshape(1, D))

    for dist, ky in near_first[:5]:
        gather_step(r7, 6, 1, dist, ky)
    group(0)
    gather_step(r7, 6, 1, *near_first[5])
    gather_step(r7, 6, 1, *near_first[6])
    group(1)
    group(2)
    group(3)
    x3 = x3_v[...]
    idx3 = jnp.concatenate([idx_all, idx_all, idx_all], axis=-1)
    half = (iota((NDEV * ROWS, 384), 1) >= 192).astype(F32)
    for p in range(8):
        hh = dot_nt(x3, win_v[2 * p:2 * p + 2].reshape(384, D))
        u_v[:, 384 * p:384 * p + 384] = jnp.where(idx3 == half + float(2 * p), jnp.maximum(hh, 0.0), 0.0).astype(BF16)
    def partial(n):
        yn = jnp.dot(u_v[...], wout_v[:, :, 256 * n:256 * n + 256].reshape(NDEV * 192, 256),
                     preferred_element_type=F32).reshape(8, 2, ROWS, 256)
        st8[n, 0] = yn[:, 0]
        st8[n, 1] = yn[:, 1]
        send(st8.at[n, 1 - c], r8.at[n], 13 + n, SIBLING)

    def reduce_send(n):
        desc(r8.at[n], 13 + n).wait_recv()
        st9[n] = st8[n, c] + r8[n]
        for dist, ky in near_first[::-1]:
            dest = chip_of(dist, ky)
            send_to(st9.at[n, dest], r9.at[n, chip], 16 + n, dest * 2 + c)
        r9[n, chip] = st9[n, chip]

    partial(0)
    partial(1)
    partial(2)
    reduce_send(0)
    reduce_send(1)
    reduce_send(2)

    desc(rw.at[pl.ds(0, NDEV - 1)], 11).wait_recv()
    h2_own = h2_v[pl.ds(pl.multiple_of(me * ROWS, ROWS), ROWS), :]
    x3_own = rms(h2_own, ln3_v[...].reshape(1, D)).astype(F32)
    logits = dot_nt(x3_own, rw[...].reshape(NDEV, D), precision=lax.Precision.HIGHEST)
    ex = jnp.exp(logits - jnp.max(logits, axis=-1, keepdims=True))
    probs = ex / jnp.sum(ex, axis=-1, keepdims=True)
    mine = iota((ROWS, NDEV), 1).astype(F32) == idx_own[:, 0:NDEV]
    gate = jnp.sum(jnp.where(mine, probs, 0.0), axis=-1, keepdims=True)
    gate = jnp.where(slot < float(NDEV), gate, 0.0)

    for n in range(3):
        desc(r9.at[n, pl.ds(0, 7)], 16 + n).wait_recv()
    yv = jnp.concatenate([jnp.sum(r9[n], axis=0) for n in range(3)], axis=-1).astype(BF16).astype(F32)
    out_h[...] = (h2_own + yv * gate).astype(BF16)

    for buf, ph in ((m1, 0), (st2, 1), (r7, 6), (rw, 11), (ix, 12)):
        desc(buf.at[pl.ds(0, NDEV - 1)], ph).wait_send()
    for n in range(3):
        desc(st9.at[n, pl.ds(0, 7)], 16 + n).wait_send()
        desc(r8.at[n], 13 + n).wait_send()
    for buf, ph in ((c3, 2), (r4, 3), (st5, 4), (c6, 5), (hs, 7)):
        desc(buf.at[pl.ds(0, 3)], ph).wait_send()
    for w, ph in ((wgo, 8), (wgq, 9), (wgc, 10)):
        desc(w.at[pl.ds(0, 3), 0], ph).wait_send()
        desc(w.at[pl.ds(0, 3), 0], ph + 11).wait_send()


def store(h_in, k_in, v_in, h_out, k_out, v_out, sem):
    parts = [(src.at[b], dst.at[b]) for b in range(ROWS) for src, dst in ((k_in, k_out), (v_in, v_out))]
    parts.append((h_in, h_out))
    copies = [pltpu.make_async_copy(src, dst, sem.at[i])
              for i, (src, dst) in enumerate(parts)]
    for cp in copies:
        cp.start()
    for cp in copies:
        cp.wait()


def solution(mesh):
    rows = ('dp', 'ws')
    row_vec = P(rows)
    row_mat = P(rows, None)
    cache = P(rows, None, None, None)
    col = P(None, 'ws')
    in_specs = (row_mat, cache, cache, cache, cache, row_vec, row_mat, P(None, None), row_vec,
                P(None), P(None), P(None), col, col, col, col, col, col,
                col, P(None, None, 'ws'), P(None, 'ws', None))
    out_specs = (row_mat, cache, cache)

    any_spec = pl.BlockSpec(memory_space=pltpu.HBM)
    vmem = pl.BlockSpec(memory_space=pltpu.VMEM)

    def block(hidden, self_k, self_v, cross_k, cross_v, positions, enc_mask, rel_bias, expert_idx,
              ln_self, ln_cross, ln_ffn, wq_self, wk_self, wv_self, wo_self, wq_cross, wo_cross,
              w_router, w_in, w_out):
        def flat(cache_arr):
            return jnp.swapaxes(cache_arr, 2, 3).reshape(ROWS, D, cache_arr.shape[2])

        def unflat(arr):
            return jnp.swapaxes(arr.reshape(ROWS, HEADS, 64, LS), 2, 3)

        args = (hidden, flat(self_k), flat(self_v), flat(cross_k), flat(cross_v), positions, enc_mask, rel_bias,
                expert_idx, ln_self, ln_cross, ln_ffn,
                wq_self.T, wk_self.T, wv_self.T, wo_self.T, wq_cross.T, wo_cross.T, w_router.T,
                jnp.swapaxes(w_in, 1, 2), w_out)
        specs = [any_spec] * len(args)
        V = pltpu.VMEM
        scratch = [
            V((ROWS, D, LC), BF16), V((ROWS, D, LC), BF16), V((NDEV, 192, D), BF16), V((NDEV, 192, D), BF16),
            V((ROWS, LC), jnp.int32), V((HEADS, LS), F32), V((D,), F32), V((D,), F32), V((D,), F32), V((256, D), BF16),
            V((NDEV, ROWS, D), BF16), V((NDEV, ROWS, 128), BF16), V((NDEV, ROWS, 256), BF16), V((NDEV, ROWS, 256), BF16),
            V((4, 2, CB // 2, D), BF16), V((4, 2, CB // 2, D), BF16), V((4, 2, CB // 2, D), BF16), V((NDEV, 1, D), F32),
            V((4, ROWS, D), BF16), V((4, CB, 128), BF16), V((4, ROWS, 256), BF16), V((4, ROWS, 256), BF16),
            V((4, ROWS, D), BF16), V((NDEV, CB, 128), BF16), V((3, 2, 8, ROWS, 256), F32), V((3, 8, ROWS, 256), F32),
            V((3, 8, ROWS, 256), F32), V((3, 8, ROWS, 256), F32),
            V((ROWS, HPAD, LS), F32), V((ROWS, HPAD, LS), F32), V((ROWS, HPAD, LC), F32), V((ROWS, D), F32),
            V((NDEV * ROWS, D), F32), V((NDEV * ROWS, D), BF16), V((NDEV * ROWS, NDEV * 192), BF16),
            V((ROWS, D, LS), BF16), V((ROWS, D, LS), BF16), V((4, ROWS, D), BF16), V((ROWS, HPAD, D), BF16),
            pltpu.SMEM((ROWS,), jnp.int32), pltpu.SMEM((ROWS,), jnp.int32),
            pltpu.SemaphoreType.DMA((24,)), pltpu.SemaphoreType.DMA((22,)), pltpu.SemaphoreType.DMA((22,)),
            pltpu.SemaphoreType.DMA((2, 8)), pltpu.SemaphoreType.DMA((2, 8)),
        ]
        h_out, k_out, v_out = pl.pallas_call(
            kernel,
            out_shape=(V((ROWS, D), BF16), V((ROWS, D, LS), BF16), V((ROWS, D, LS), BF16)),
            in_specs=specs,
            out_specs=(vmem, vmem, vmem),
            scratch_shapes=scratch,
            compiler_params=pltpu.CompilerParams(collective_id=0, has_side_effects=True,
                                                 vmem_limit_bytes=67043328 - 2 * 3145728 - 16384),
        )(*args)
        outs = (jax.ShapeDtypeStruct((ROWS, D), BF16), jax.ShapeDtypeStruct((ROWS, D, LS), BF16),
                jax.ShapeDtypeStruct((ROWS, D, LS), BF16))
        h_out, k_out, v_out = pl.pallas_call(
            store, out_shape=outs, in_specs=[vmem] * 3, out_specs=(any_spec,) * 3,
            scratch_shapes=[pltpu.SemaphoreType.DMA((2 * ROWS + 1,))],
            compiler_params=pltpu.CompilerParams(vmem_limit_bytes=4 * 1024 * 1024),
        )(h_out, k_out, v_out)
        return h_out, unflat(k_out), unflat(v_out)

    return jax.shard_map(block, mesh=mesh, in_specs=in_specs, out_specs=out_specs, check_vma=False)
```

```python
import jax
import jax.numpy as jnp
from jax import lax
from jax.experimental import pallas as pl
from jax.experimental.pallas import tpu as pltpu
from jax.sharding import PartitionSpec as P

EPS = 1e-6
NEG = -1e30
F32 = jnp.float32
BF16 = jnp.bfloat16
MESH = pl.DeviceIdType.MESH

ROWS = 8
D = 768
HEADS = 12
HPAD = 16
LS = 192
LC = 384
NDEV = 16
CB = 48
NT = (((1,), (1,)), ((), ()))

ALL_OFFS = [(kz, ky, kc) for kz in (2, 3, 1, 0) for ky in (1, 0) for kc in (1, 0) if (kz, ky, kc) != (0, 0, 0)]
CHIP_OFFS = [off for off in ALL_OFFS if off[2] == 0]
SIBLING = (0, 0, 1)
SUB_OFFS = [(0, 1, 1), (0, 1, 0), (0, 0, 1)]
Z_OFFS = [(2, 0, 0), (3, 0, 0), (1, 0, 0)]


def dot_nt(a, b, **kw):
    return lax.dot_general(a, b, NT, preferred_element_type=F32, **kw)


def iota(shape, axis):
    return lax.broadcasted_iota(jnp.int32, shape, axis)


def rms(x, g):
    inv = lax.rsqrt(jnp.mean(x * x, axis=-1, keepdims=True) + EPS)
    return (x * inv * g).astype(BF16)


def head_mask():
    row = iota((HPAD, D), 0) * 64
    col = iota((HPAD, D), 1)
    return (col >= row) & (col < row + 64)


def attention(q8, k_ref, v_ref, bias_of, s_ref, ctx_ref, q_ref, patch=None):
    hm = head_mask()
    for b in range(ROWS):
        qb = jnp.where(hm, jnp.broadcast_to(q8[b:b + 1, :], (HPAD, D)), 0.0).astype(BF16)
        q_ref[b] = qb
    if patch is not None:
        k8, v8, hit_of = patch
        new = dot_nt(q_ref[...].reshape(ROWS * HPAD, D), k8.astype(BF16))
        row = iota((ROWS * HPAD, ROWS), 0)
        col = iota((ROWS * HPAD, ROWS), 1) * HPAD
        new = jnp.sum(jnp.where((row >= col) & (row < col + HPAD), new, 0.0), axis=-1, keepdims=True)
    for b in range(ROWS):
        sb = jnp.dot(q_ref[b], k_ref[b], preferred_element_type=F32)
        if patch is not None:
            sb = jnp.where(hit_of(b), new[b * HPAD:(b + 1) * HPAD], sb)
        s_ref[b] = sb + bias_of(b)
    s = s_ref[...]
    p = jnp.exp(s - jnp.max(s, axis=-1, keepdims=True))
    s_ref[...] = p / jnp.sum(p, axis=-1, keepdims=True)
    for b in range(ROWS):
        pb = s_ref[b].astype(BF16)
        if patch is None:
            cb = dot_nt(pb, v_ref[b])
        else:
            pf = pb.astype(F32)
            hit = hit_of(b)
            at_pos = jnp.sum(jnp.where(hit, pf, 0.0), axis=-1, keepdims=True)
            cb = dot_nt(jnp.where(hit, 0.0, pf).astype(BF16), v_ref[b]) + at_pos * v8[b:b + 1, :]
        ctx_ref[b:b + 1, :] = jnp.sum(jnp.where(hm, cb, 0.0), axis=0, keepdims=True)


def kernel(hid, kT, vT, ckT, cvT, pos, mask, rel, idx, ln1, ln2, ln3, wq, wk, wv, wo, wqc, woc, wr, win, wout,
           out_h, k_v, v_v,
           ck_v, cv_v, win_v, wout_v, mask_v, rel_v, ln1_v, ln2_v, ln3_v, wqkv, m1, ix, st2, r2, wgo, wgq, wgc, rw,
           c3, r4, st5, r5, c6, r7, st8, r8, st9, r9, bias_s, s_self, s_cross, ctx_v, h2_v, x3_v, u_v,
           k_old, v_old, hs, q_v, pos_s, idx_s, ld, snd, rcv, direct, fwd):
    me = lax.axis_index('ws')
    dpi = lax.axis_index('dp')
    z = me // 4
    s = me % 4
    y = s // 2
    c = s % 2

    z_near = (z, z + 1 - 2 * (z % 2), 2 - z // 2, 3 * (1 - z // 2))
    chip = me // 2

    def chip_of(dist, ky):
        return z_near[dist] * 2 + (y + ky) % 2

    near_first = [(dist, ky) for dist in range(4) for ky in (0, 1)][1:]

    def far_first():
        return [chip_of(dist, ky) * 2 + (c + kc) % 2 for dist in (3, 2, 1, 0) for ky in (1, 0) for kc in (1, 0)][:-1]

    def peer_of(off):
        kz, ky, kc = off
        return ((z + kz) % 4) * 4 + ((y + ky) % 2) * 2 + (c + kc) % 2

    def send(src, dst, ph, off):
        send_to(src, dst, ph, peer_of(off))

    def send_to(src, dst, ph, dev):
        pltpu.make_async_remote_copy(src_ref=src, dst_ref=dst, send_sem=snd.at[ph], recv_sem=rcv.at[ph],
                                     device_id={'ws': dev}, device_id_type=MESH).start()

    def desc(buf, ph):
        return pltpu.make_async_remote_copy(src_ref=buf, dst_ref=buf, send_sem=snd.at[ph], recv_sem=rcv.at[ph],
                                            device_id={'ws': me}, device_id_type=MESH)

    def gather_start(buf, ph, row):
        for dist, ky in near_first[::-1]:
            pltpu.make_async_remote_copy(src_ref=buf.at[me], dst_ref=buf.at[me], send_sem=snd.at[ph],
                                         recv_sem=direct.at[row, chip],
                                         device_id={'ws': chip_of(dist, ky) * 2 + c}, device_id_type=MESH).start()
        gather_pass(buf, ph, row, me, chip)

    def gather_pass(buf, ph, row, src, src_chip):
        pltpu.make_async_remote_copy(src_ref=buf.at[src], dst_ref=buf.at[src], send_sem=snd.at[ph],
                                     recv_sem=fwd.at[row, src_chip],
                                     device_id={'ws': peer_of(SIBLING)}, device_id_type=MESH).start()

    def arrived(buf, ph, sem):
        pltpu.make_async_remote_copy(src_ref=buf.at[0], dst_ref=buf.at[0], send_sem=snd.at[ph], recv_sem=sem,
                                     device_id={'ws': me}, device_id_type=MESH).wait_recv()

    def gather_step(buf, ph, row, dist, ky):
        src_chip = chip_of(dist, ky)
        arrived(buf, ph, direct.at[row, src_chip])
        gather_pass(buf, ph, row, src_chip * 2 + c, src_chip)

    def subgroup(buf, ph):
        for off in SUB_OFFS:
            send(buf.at[s], buf.at[s], ph, off)

    def weight_start(w, ph, dists=(3, 2, 1)):
        for dist in dists:
            send_to(w.at[z, dpi], w.at[z, dpi], ph, chip_of(dist, 0) * 2 + c)

    def weight_pass(w, ph):
        desc(w.at[pl.ds(0, 3), 0], ph).wait_recv()
        for kz in (1, 2, 3):
            src = (z + kz) % 4
            pltpu.make_async_remote_copy(src_ref=w.at[src, dpi], dst_ref=w.at[src, dpi], send_sem=snd.at[ph + 11],
                                         recv_sem=rcv.at[ph + 11], device_id={'dp': 1 - dpi, 'ws': me},
                                         device_id_type=MESH).start()

    def weight_finish(w, ph):
        desc(w.at[pl.ds(0, 3), 0], ph + 11).wait_recv()

    bar = pltpu.get_barrier_semaphore()
    pl.semaphore_signal(bar, inc=1, device_id={'dp': 1 - dpi, 'ws': me}, device_id_type=MESH)
    for off in ALL_OFFS:
        pl.semaphore_signal(bar, inc=1, device_id={'ws': peer_of(off)}, device_id_type=MESH)

    loads = {}

    def load(name, src, dst):
        cp = pltpu.make_async_copy(src, dst, ld.at[len(loads)])
        cp.start()
        loads[name] = cp

    load('hid', hid, hs.at[s])
    load('ln1', ln1, ln1_v)
    load('pos', pos, pos_s)
    load('idx', idx, idx_s)
    load('wq', wq, wqkv.at[pl.ds(0, CB)])
    load('wk', wk, wqkv.at[pl.ds(CB, CB)])
    load('wv', wv, wqkv.at[pl.ds(2 * CB, CB)])
    load('ln2', ln2, ln2_v)
    load('ln3', ln3, ln3_v)
    load('rel', rel, rel_v)
    load('mask', mask, mask_v)
    load('wr', wr, rw.at[me])
    load('wo0', wo.at[pl.ds(0, CB // 2)], wgo.at[z, 0])
    load('wo1', wo.at[pl.ds(CB // 2, CB // 2)], wgo.at[z, 1])
    load('wqc0', wqc.at[pl.ds(0, CB // 2)], wgq.at[z, 0])
    load('wqc1', wqc.at[pl.ds(CB // 2, CB // 2)], wgq.at[z, 1])
    load('woc0', woc.at[pl.ds(0, CB // 2)], wgc.at[z, 0])
    load('woc1', woc.at[pl.ds(CB // 2, CB // 2)], wgc.at[z, 1])

    wqkv[3 * CB:256, :] = jnp.zeros((256 - 3 * CB, D), BF16)
    loads['hid'].wait()
    loads['ln1'].wait()
    m1[me] = rms(hs[s].astype(F32), ln1_v[...].reshape(1, D))
    pl.semaphore_wait(bar, NDEV)

    gather_start(m1, 0, 0)
    loads['wo0'].wait()
    loads['wo1'].wait()
    weight_start(wgo, 8, (3, 2))
    subgroup(hs, 7)
    load('k', kT, k_old)
    load('v', vT, v_old)
    loads['pos'].wait()
    loads['idx'].wait()
    row8 = iota((ROWS, 128), 0)
    idx_own = jnp.zeros((ROWS, 128), jnp.int32)
    for i in range(ROWS):
        idx_own = jnp.where(row8 == i, idx_s[i], idx_own)
    idx_own = idx_own.astype(F32)
    ix[me] = idx_own.astype(BF16)

    loads['rel'].wait()
    loads['mask'].wait()
    rel_f = rel_v[...]
    rel_hi = rel_f.astype(BF16)
    rem = rel_f - rel_hi.astype(F32)
    rel_mid = rem.astype(BF16)
    rel_lo = (rem - rel_mid.astype(F32)).astype(BF16)
    src_i = iota((LS, LS), 0)
    dst_i = iota((LS, LS), 1)
    lane12 = iota((HEADS, LS), 1)
    bias_s[...] = jnp.zeros((ROWS, HPAD, LS), F32)
    for b in range(ROWS):
        pick = jnp.where(src_i + dst_i == pos_s[b], 1.0, 0.0).astype(BF16)
        bb = jnp.dot(rel_hi, pick, preferred_element_type=F32)
        bb = bb + jnp.dot(rel_mid, pick, preferred_element_type=F32)
        bb = bb + jnp.dot(rel_lo, pick, preferred_element_type=F32)
        bias_s[b, 0:HEADS, :] = jnp.where(lane12 <= pos_s[b], bb, NEG)
    for name in ('wq', 'wk', 'wv', 'ln2', 'ln3', 'wr', 'wqc0', 'wqc1', 'woc0', 'woc1'):
        loads[name].wait()

    for dist, ky in near_first:
        gather_step(m1, 0, 0, dist, ky)
    for dist in range(4):
        for ky in (0, 1):
            arrived(m1, 0, fwd.at[0, chip_of(dist, ky)])
    xn = m1[...].astype(F32).reshape(NDEV * ROWS, D).astype(BF16)
    st2[...] = dot_nt(xn, wqkv[...]).reshape(NDEV, ROWS, 256).astype(BF16)
    r2[me] = st2[me]
    for dev in far_first():
        send_to(st2.at[dev], r2.at[me], 1, dev)
    weight_start(wgo, 8, (1,))
    weight_start(wgq, 9)
    load('ck', ckT, ck_v)
    load('cv', cvT, cv_v)

    sel_r = iota((4 * CB, D), 0)
    sel_q = ((sel_r >= CB).astype(jnp.int32) + (sel_r >= 2 * CB).astype(jnp.int32)
             + (sel_r >= 3 * CB).astype(jnp.int32))
    sel = (iota((4 * CB, D), 1) == sel_r + sel_q * (4 * CB - CB) + s * CB)
    sel = jnp.where(sel, 1.0, 0.0).astype(BF16)
    desc(hs.at[pl.ds(0, 3)], 7).wait_recv()
    h_sub = hs[...].astype(F32).reshape(4 * ROWS, D).astype(BF16)
    h_blk = dot_nt(h_sub, sel)

    weight_pass(wgo, 8)
    loads['k'].wait()
    loads['v'].wait()
    desc(r2.at[pl.ds(0, NDEV - 1)], 1).wait_recv()
    weight_start(wgc, 10)
    rv = r2[...].astype(F32)

    def columns(lo):
        return jnp.concatenate([rv[d, :, lo:lo + CB] for d in range(NDEV)], axis=-1)

    q8 = columns(0)
    k8 = columns(CB)
    v8 = columns(2 * CB)
    lane_h = iota((HPAD, LS), 1)
    attention(q8, k_old, v_old, lambda b: bias_s[b], s_self, ctx_v, q_v,
              (k8, v8, lambda b: lane_h == pos_s[b]))

    def update(new, old, out):
        cols = new.T
        lane_s = iota((D, LS), 1)
        for b in range(ROWS):
            out[b] = jnp.where(lane_s == pos_s[b], jnp.broadcast_to(cols[:, b:b + 1], (D, LS)),
                               old[b].astype(F32)).astype(BF16)

    def natural(pieces):
        return jnp.concatenate([pieces[t][:, q * CB:(q + 1) * CB] for q in range(4) for t in range(4)], axis=-1)

    def pack(buf, i, blk):
        buf[i, 0:32, :] = blk[:, 0:128].astype(BF16)
        buf[i, 32:48, :] = jnp.concatenate([blk[0:16, 128:192], blk[16:32, 128:192]], axis=-1).astype(BF16)

    def unpack(blk):
        tail = jnp.concatenate([blk[32:48, 0:64], blk[32:48, 64:128]], axis=0)
        return jnp.concatenate([blk[0:32, :], tail], axis=-1)

    c3[s] = ctx_v[...].astype(BF16)
    subgroup(c3, 2)
    weight_pass(wgq, 9)
    update(k8, k_old, k_v)
    for off in ALL_OFFS:
        send(ix.at[me], ix.at[me], 12, off)
        send(rw.at[me], rw.at[me], 11, off)
    update(v8, v_old, v_v)
    load('win', win, win_v)
    load('wout', wout, wout_v)
    desc(c3.at[pl.ds(0, 3)], 2).wait_recv()
    weight_finish(wgo, 8)
    ctx = c3[...].astype(F32).reshape(4 * ROWS, D).astype(BF16)
    h1_blk = (h_blk + dot_nt(ctx, wgo[...].reshape(4 * CB, D))).astype(BF16)
    pack(r4, s, h1_blk.astype(F32))
    subgroup(r4, 3)
    desc(r4.at[pl.ds(0, 3)], 3).wait_recv()
    weight_finish(wgq, 9)
    r4f = r4[...].astype(F32)
    h1 = natural([unpack(r4f[t]) for t in range(4)])
    x2 = rms(h1, ln2_v[...].reshape(1, D))
    st5[:, :, 0:4 * CB] = dot_nt(x2, wgq[...].reshape(4 * CB, D)).reshape(4, ROWS, 4 * CB).astype(BF16)
    r5[s] = st5[s]
    for off in SUB_OFFS:
        kz, ky, kc = off
        send(st5.at[((y + ky) % 2) * 2 + (c + kc) % 2], r5.at[s], 4, off)
    weight_pass(wgc, 10)
    loads['ck'].wait()
    loads['cv'].wait()
    desc(r5.at[pl.ds(0, 3)], 4).wait_recv()
    r5f = r5[...].astype(F32)
    q2 = natural([r5f[t] for t in range(4)])
    attention(q2, ck_v, cv_v, lambda b: jnp.where(mask_v[b:b + 1, :] == 1, 0.0, NEG), s_cross, ctx_v, q_v)

    c6[s] = ctx_v[...].astype(BF16)
    subgroup(c6, 5)
    desc(c6.at[pl.ds(0, 3)], 5).wait_recv()
    weight_finish(wgc, 10)
    ctx2 = c6[...].astype(F32).reshape(4 * ROWS, D).astype(BF16)
    h2_blk = (h1_blk.astype(F32) + dot_nt(ctx2, wgc[...].reshape(4 * CB, D))).astype(BF16)
    pack(r7, me, h2_blk.astype(F32))

    gather_start(r7, 6, 1)
    desc(ix.at[pl.ds(0, NDEV - 1)], 12).wait_recv()
    idx_all = ix[...].astype(F32).reshape(NDEV * ROWS, 128)
    idx_t = idx_all.T
    earlier = (idx_t[0:ROWS, :] == idx_own) & (iota((ROWS, 128), 1) < me * ROWS + row8)
    slot = jnp.sum(jnp.where(earlier, 1.0, 0.0), axis=-1, keepdims=True)
    loads['win'].wait()
    loads['wout'].wait()

    def group(dist):
        for ky in (0, 1):
            arrived(r7, 6, fwd.at[1, chip_of(dist, ky)])
        t = z_near[dist]
        h2g = natural([unpack(r7[4 * t + u].astype(F32)) for u in range(4)])
        at = pl.ds(pl.multiple_of(32 * t, 32), 32)
        h2_v[at, :] = h2g
        x3_v[at, :] = rms(h2g, ln3_v[...].reshape(1, D))

    for dist, ky in near_first[:5]:
        gather_step(r7, 6, 1, dist, ky)
    group(0)
    gather_step(r7, 6, 1, *near_first[5])
    gather_step(r7, 6, 1, *near_first[6])
    group(1)
    group(2)
    group(3)
    x3 = x3_v[...]
    idx3 = jnp.concatenate([idx_all, idx_all, idx_all], axis=-1)
    half = (iota((NDEV * ROWS, 384), 1) >= 192).astype(F32)
    for p in range(8):
        hh = dot_nt(x3, win_v[2 * p:2 * p + 2].reshape(384, D))
        u_v[:, 384 * p:384 * p + 384] = jnp.where(idx3 == half + float(2 * p), jnp.maximum(hh, 0.0), 0.0).astype(BF16)
    def partial(n):
        yn = jnp.dot(u_v[...], wout_v[:, :, 256 * n:256 * n + 256].reshape(NDEV * 192, 256),
                     preferred_element_type=F32).reshape(8, 2, ROWS, 256)
        st8[n, 0] = yn[:, 0]
        st8[n, 1] = yn[:, 1]
        send(st8.at[n, 1 - c], r8.at[n], 13 + n, SIBLING)

    def reduce_send(n):
        desc(r8.at[n], 13 + n).wait_recv()
        st9[n] = st8[n, c] + r8[n]
        for dist, ky in near_first[::-1]:
            dest = chip_of(dist, ky)
            send_to(st9.at[n, dest], r9.at[n, chip], 16 + n, dest * 2 + c)
        r9[n, chip] = st9[n, chip]

    partial(0)
    partial(1)
    partial(2)
    reduce_send(0)
    reduce_send(1)
    reduce_send(2)

    desc(rw.at[pl.ds(0, NDEV - 1)], 11).wait_recv()
    h2_own = h2_v[pl.ds(pl.multiple_of(me * ROWS, ROWS), ROWS), :]
    x3_own = rms(h2_own, ln3_v[...].reshape(1, D)).astype(F32)
    logits = dot_nt(x3_own, rw[...].reshape(NDEV, D), precision=lax.Precision.HIGHEST)
    ex = jnp.exp(logits - jnp.max(logits, axis=-1, keepdims=True))
    probs = ex / jnp.sum(ex, axis=-1, keepdims=True)
    mine = iota((ROWS, NDEV), 1).astype(F32) == idx_own[:, 0:NDEV]
    gate = jnp.sum(jnp.where(mine, probs, 0.0), axis=-1, keepdims=True)
    gate = jnp.where(slot < float(NDEV), gate, 0.0)

    for n in range(3):
        desc(r9.at[n, pl.ds(0, 7)], 16 + n).wait_recv()
    yv = jnp.concatenate([jnp.sum(r9[n], axis=0) for n in range(3)], axis=-1).astype(BF16).astype(F32)
    out_h[...] = (h2_own + yv * gate).astype(BF16)

    for buf, ph in ((m1, 0), (st2, 1), (r7, 6), (rw, 11), (ix, 12)):
        desc(buf.at[pl.ds(0, NDEV - 1)], ph).wait_send()
    for n in range(3):
        desc(st9.at[n, pl.ds(0, 7)], 16 + n).wait_send()
        desc(r8.at[n], 13 + n).wait_send()
    for buf, ph in ((c3, 2), (r4, 3), (st5, 4), (c6, 5), (hs, 7)):
        desc(buf.at[pl.ds(0, 3)], ph).wait_send()
    for w, ph in ((wgo, 8), (wgq, 9), (wgc, 10)):
        desc(w.at[pl.ds(0, 3), 0], ph).wait_send()
        desc(w.at[pl.ds(0, 3), 0], ph + 11).wait_send()


def store(h_in, k_in, v_in, h_out, k_out, v_out, sem):
    copies = [pltpu.make_async_copy(src, dst, sem.at[i])
              for i, (src, dst) in enumerate(((k_in, k_out), (v_in, v_out), (h_in, h_out)))]
    for cp in copies:
        cp.start()
    for cp in copies:
        cp.wait()


def solution(mesh):
    rows = ('dp', 'ws')
    row_vec = P(rows)
    row_mat = P(rows, None)
    cache = P(rows, None, None, None)
    col = P(None, 'ws')
    in_specs = (row_mat, cache, cache, cache, cache, row_vec, row_mat, P(None, None), row_vec,
                P(None), P(None), P(None), col, col, col, col, col, col,
                col, P(None, None, 'ws'), P(None, 'ws', None))
    out_specs = (row_mat, cache, cache)

    any_spec = pl.BlockSpec(memory_space=pltpu.HBM)
    vmem = pl.BlockSpec(memory_space=pltpu.VMEM)

    def block(hidden, self_k, self_v, cross_k, cross_v, positions, enc_mask, rel_bias, expert_idx,
              ln_self, ln_cross, ln_ffn, wq_self, wk_self, wv_self, wo_self, wq_cross, wo_cross,
              w_router, w_in, w_out):
        def flat(cache_arr):
            return jnp.swapaxes(cache_arr, 2, 3).reshape(ROWS, D, cache_arr.shape[2])

        def unflat(arr):
            return jnp.swapaxes(arr.reshape(ROWS, HEADS, 64, LS), 2, 3)

        args = (hidden, flat(self_k), flat(self_v), flat(cross_k), flat(cross_v), positions, enc_mask, rel_bias,
                expert_idx, ln_self, ln_cross, ln_ffn,
                wq_self.T, wk_self.T, wv_self.T, wo_self.T, wq_cross.T, wo_cross.T, w_router.T,
                jnp.swapaxes(w_in, 1, 2), w_out)
        specs = [any_spec] * len(args)
        V = pltpu.VMEM
        scratch = [
            V((ROWS, D, LC), BF16), V((ROWS, D, LC), BF16), V((NDEV, 192, D), BF16), V((NDEV, 192, D), BF16),
            V((ROWS, LC), jnp.int32), V((HEADS, LS), F32), V((D,), F32), V((D,), F32), V((D,), F32), V((256, D), BF16),
            V((NDEV, ROWS, D), BF16), V((NDEV, ROWS, 128), BF16), V((NDEV, ROWS, 256), BF16), V((NDEV, ROWS, 256), BF16),
            V((4, 2, CB // 2, D), BF16), V((4, 2, CB // 2, D), BF16), V((4, 2, CB // 2, D), BF16), V((NDEV, 1, D), F32),
            V((4, ROWS, D), BF16), V((4, CB, 128), BF16), V((4, ROWS, 256), BF16), V((4, ROWS, 256), BF16),
            V((4, ROWS, D), BF16), V((NDEV, CB, 128), BF16), V((3, 2, 8, ROWS, 256), F32), V((3, 8, ROWS, 256), F32),
            V((3, 8, ROWS, 256), F32), V((3, 8, ROWS, 256), F32),
            V((ROWS, HPAD, LS), F32), V((ROWS, HPAD, LS), F32), V((ROWS, HPAD, LC), F32), V((ROWS, D), F32),
            V((NDEV * ROWS, D), F32), V((NDEV * ROWS, D), BF16), V((NDEV * ROWS, NDEV * 192), BF16),
            V((ROWS, D, LS), BF16), V((ROWS, D, LS), BF16), V((4, ROWS, D), BF16), V((ROWS, HPAD, D), BF16),
            pltpu.SMEM((ROWS,), jnp.int32), pltpu.SMEM((ROWS,), jnp.int32),
            pltpu.SemaphoreType.DMA((24,)), pltpu.SemaphoreType.DMA((22,)), pltpu.SemaphoreType.DMA((22,)),
            pltpu.SemaphoreType.DMA((2, 8)), pltpu.SemaphoreType.DMA((2, 8)),
        ]
        h_out, k_out, v_out = pl.pallas_call(
            kernel,
            out_shape=(V((ROWS, D), BF16), V((ROWS, D, LS), BF16), V((ROWS, D, LS), BF16)),
            in_specs=specs,
            out_specs=(vmem, vmem, vmem),
            scratch_shapes=scratch,
            compiler_params=pltpu.CompilerParams(collective_id=0, has_side_effects=True,
                                                 vmem_limit_bytes=67043328 - 2 * 3145728 - 16384),
        )(*args)
        outs = (jax.ShapeDtypeStruct((ROWS, D), BF16), jax.ShapeDtypeStruct((ROWS, D, LS), BF16),
                jax.ShapeDtypeStruct((ROWS, D, LS), BF16))
        h_out, k_out, v_out = pl.pallas_call(
            store, out_shape=outs, in_specs=[vmem] * 3, out_specs=(any_spec,) * 3,
            scratch_shapes=[pltpu.SemaphoreType.DMA((3,))],
            compiler_params=pltpu.CompilerParams(vmem_limit_bytes=4 * 1024 * 1024),
        )(h_out, k_out, v_out)
        return h_out, unflat(k_out), unflat(v_out)

    return jax.shard_map(block, mesh=mesh, in_specs=in_specs, out_specs=out_specs, check_vma=False)
```

```python
import jax
import jax.numpy as jnp
from jax import lax
from jax.experimental import pallas as pl
from jax.experimental.pallas import tpu as pltpu
from jax.sharding import PartitionSpec as P

EPS = 1e-6
NEG = -1e30
F32 = jnp.float32
BF16 = jnp.bfloat16
MESH = pl.DeviceIdType.MESH

ROWS = 8
D = 768
HEADS = 12
HPAD = 16
LS = 192
LC = 384
NDEV = 16
CB = 48
NT = (((1,), (1,)), ((), ()))

ALL_OFFS = [(kz, ky, kc) for kz in (2, 3, 1, 0) for ky in (1, 0) for kc in (1, 0) if (kz, ky, kc) != (0, 0, 0)]
CHIP_OFFS = [off for off in ALL_OFFS if off[2] == 0]
SIBLING = (0, 0, 1)
SUB_OFFS = [(0, 1, 1), (0, 1, 0), (0, 0, 1)]
Z_OFFS = [(2, 0, 0), (3, 0, 0), (1, 0, 0)]


def dot_nt(a, b, **kw):
    return lax.dot_general(a, b, NT, preferred_element_type=F32, **kw)


def iota(shape, axis):
    return lax.broadcasted_iota(jnp.int32, shape, axis)


def rms(x, g):
    inv = lax.rsqrt(jnp.mean(x * x, axis=-1, keepdims=True) + EPS)
    return (x * inv * g).astype(BF16)


def head_mask():
    row = iota((HPAD, D), 0) * 64
    col = iota((HPAD, D), 1)
    return (col >= row) & (col < row + 64)


def attention(q8, k_ref, v_ref, bias_of, s_ref, ctx_ref, q_ref, patch=None):
    hm = head_mask()
    for b in range(ROWS):
        qb = jnp.where(hm, jnp.broadcast_to(q8[b:b + 1, :], (HPAD, D)), 0.0).astype(BF16)
        q_ref[b] = qb
    if patch is not None:
        k8, v8, hit_of = patch
        new = dot_nt(q_ref[...].reshape(ROWS * HPAD, D), k8.astype(BF16))
        row = iota((ROWS * HPAD, ROWS), 0)
        col = iota((ROWS * HPAD, ROWS), 1) * HPAD
        new = jnp.sum(jnp.where((row >= col) & (row < col + HPAD), new, 0.0), axis=-1, keepdims=True)
    for b in range(ROWS):
        sb = jnp.dot(q_ref[b], k_ref[b], preferred_element_type=F32)
        if patch is not None:
            sb = jnp.where(hit_of(b), new[b * HPAD:(b + 1) * HPAD], sb)
        s_ref[b] = sb + bias_of(b)
    s = s_ref[...]
    p = jnp.exp(s - jnp.max(s, axis=-1, keepdims=True))
    s_ref[...] = p / jnp.sum(p, axis=-1, keepdims=True)
    for b in range(ROWS):
        pb = s_ref[b].astype(BF16)
        if patch is None:
            cb = dot_nt(pb, v_ref[b])
        else:
            pf = pb.astype(F32)
            hit = hit_of(b)
            at_pos = jnp.sum(jnp.where(hit, pf, 0.0), axis=-1, keepdims=True)
            cb = dot_nt(jnp.where(hit, 0.0, pf).astype(BF16), v_ref[b]) + at_pos * v8[b:b + 1, :]
        ctx_ref[b:b + 1, :] = jnp.sum(jnp.where(hm, cb, 0.0), axis=0, keepdims=True)


def kernel(hid, kT, vT, ckT, cvT, pos, mask, rel, idx, ln1, ln2, ln3, wq, wk, wv, wo, wqc, woc, wr, win, wout,
           out_h, k_v, v_v,
           ck_v, cv_v, win_v, wout_v, mask_v, rel_v, ln1_v, ln2_v, ln3_v, wqkv, m1, ix, st2, r2, wgo, wgq, wgc, rw,
           c3, r4, st5, r5, c6, r7, st8, r8, st9, r9, bias_s, s_self, s_cross, ctx_v, h2_v, x3_v, u_v,
           k_old, v_old, hs, q_v, pos_s, idx_s, ld, snd, rcv, direct, fwd):
    me = lax.axis_index('ws')
    dpi = lax.axis_index('dp')
    z = me // 4
    s = me % 4
    y = s // 2
    c = s % 2

    z_near = (z, z + 1 - 2 * (z % 2), 2 - z // 2, 3 * (1 - z // 2))
    chip = me // 2

    def chip_of(dist, ky):
        return z_near[dist] * 2 + (y + ky) % 2

    near_first = [(dist, ky) for dist in range(4) for ky in (0, 1)][1:]

    def far_first():
        return [chip_of(dist, ky) * 2 + (c + kc) % 2 for dist in (3, 2, 1, 0) for ky in (1, 0) for kc in (1, 0)][:-1]

    def peer_of(off):
        kz, ky, kc = off
        return ((z + kz) % 4) * 4 + ((y + ky) % 2) * 2 + (c + kc) % 2

    def send(src, dst, ph, off):
        send_to(src, dst, ph, peer_of(off))

    def send_to(src, dst, ph, dev):
        pltpu.make_async_remote_copy(src_ref=src, dst_ref=dst, send_sem=snd.at[ph], recv_sem=rcv.at[ph],
                                     device_id={'ws': dev}, device_id_type=MESH).start()

    def desc(buf, ph):
        return pltpu.make_async_remote_copy(src_ref=buf, dst_ref=buf, send_sem=snd.at[ph], recv_sem=rcv.at[ph],
                                            device_id={'ws': me}, device_id_type=MESH)

    def gather_start(buf, ph, row):
        for dist, ky in near_first[::-1]:
            pltpu.make_async_remote_copy(src_ref=buf.at[me], dst_ref=buf.at[me], send_sem=snd.at[ph],
                                         recv_sem=direct.at[row, chip],
                                         device_id={'ws': chip_of(dist, ky) * 2 + c}, device_id_type=MESH).start()
        gather_pass(buf, ph, row, me, chip)

    def gather_pass(buf, ph, row, src, src_chip):
        pltpu.make_async_remote_copy(src_ref=buf.at[src], dst_ref=buf.at[src], send_sem=snd.at[ph],
                                     recv_sem=fwd.at[row, src_chip],
                                     device_id={'ws': peer_of(SIBLING)}, device_id_type=MESH).start()

    def arrived(buf, ph, sem):
        pltpu.make_async_remote_copy(src_ref=buf.at[0], dst_ref=buf.at[0], send_sem=snd.at[ph], recv_sem=sem,
                                     device_id={'ws': me}, device_id_type=MESH).wait_recv()

    def gather_step(buf, ph, row, dist, ky):
        src_chip = chip_of(dist, ky)
        arrived(buf, ph, direct.at[row, src_chip])
        gather_pass(buf, ph, row, src_chip * 2 + c, src_chip)

    def subgroup(buf, ph):
        for off in SUB_OFFS:
            send(buf.at[s], buf.at[s], ph, off)

    def weight_start(w, ph):
        for dist in (3, 2, 1):
            send_to(w.at[z, dpi], w.at[z, dpi], ph, chip_of(dist, 0) * 2 + c)

    def weight_pass(w, ph):
        desc(w.at[pl.ds(0, 3), 0], ph).wait_recv()
        for kz in (1, 2, 3):
            src = (z + kz) % 4
            pltpu.make_async_remote_copy(src_ref=w.at[src, dpi], dst_ref=w.at[src, dpi], send_sem=snd.at[ph + 11],
                                         recv_sem=rcv.at[ph + 11], device_id={'dp': 1 - dpi, 'ws': me},
                                         device_id_type=MESH).start()

    def weight_finish(w, ph):
        desc(w.at[pl.ds(0, 3), 0], ph + 11).wait_recv()

    bar = pltpu.get_barrier_semaphore()
    pl.semaphore_signal(bar, inc=1, device_id={'dp': 1 - dpi, 'ws': me}, device_id_type=MESH)
    for off in ALL_OFFS:
        pl.semaphore_signal(bar, inc=1, device_id={'ws': peer_of(off)}, device_id_type=MESH)

    loads = {}

    def load(name, src, dst):
        cp = pltpu.make_async_copy(src, dst, ld.at[len(loads)])
        cp.start()
        loads[name] = cp

    load('hid', hid, hs.at[s])
    load('ln1', ln1, ln1_v)
    load('pos', pos, pos_s)
    load('idx', idx, idx_s)
    load('wq', wq, wqkv.at[pl.ds(0, CB)])
    load('wk', wk, wqkv.at[pl.ds(CB, CB)])
    load('wv', wv, wqkv.at[pl.ds(2 * CB, CB)])
    load('ln2', ln2, ln2_v)
    load('ln3', ln3, ln3_v)
    load('rel', rel, rel_v)
    load('mask', mask, mask_v)
    load('wr', wr, rw.at[me])
    load('wo0', wo.at[pl.ds(0, CB // 2)], wgo.at[z, 0])
    load('wo1', wo.at[pl.ds(CB // 2, CB // 2)], wgo.at[z, 1])
    load('wqc0', wqc.at[pl.ds(0, CB // 2)], wgq.at[z, 0])
    load('wqc1', wqc.at[pl.ds(CB // 2, CB // 2)], wgq.at[z, 1])
    load('woc0', woc.at[pl.ds(0, CB // 2)], wgc.at[z, 0])
    load('woc1', woc.at[pl.ds(CB // 2, CB // 2)], wgc.at[z, 1])

    wqkv[3 * CB:256, :] = jnp.zeros((256 - 3 * CB, D), BF16)
    loads['hid'].wait()
    loads['ln1'].wait()
    m1[me] = rms(hs[s].astype(F32), ln1_v[...].reshape(1, D))
    pl.semaphore_wait(bar, NDEV)

    gather_start(m1, 0, 0)
    loads['wo0'].wait()
    loads['wo1'].wait()
    weight_start(wgo, 8)
    subgroup(hs, 7)
    load('k', kT, k_old)
    load('v', vT, v_old)
    loads['pos'].wait()
    loads['idx'].wait()
    row8 = iota((ROWS, 128), 0)
    idx_own = jnp.zeros((ROWS, 128), jnp.int32)
    for i in range(ROWS):
        idx_own = jnp.where(row8 == i, idx_s[i], idx_own)
    idx_own = idx_own.astype(F32)
    ix[me] = idx_own.astype(BF16)

    loads['rel'].wait()
    loads['mask'].wait()
    rel_f = rel_v[...]
    rel_hi = rel_f.astype(BF16)
    rem = rel_f - rel_hi.astype(F32)
    rel_mid = rem.astype(BF16)
    rel_lo = (rem - rel_mid.astype(F32)).astype(BF16)
    src_i = iota((LS, LS), 0)
    dst_i = iota((LS, LS), 1)
    lane12 = iota((HEADS, LS), 1)
    bias_s[...] = jnp.zeros((ROWS, HPAD, LS), F32)
    for b in range(ROWS):
        pick = jnp.where(src_i + dst_i == pos_s[b], 1.0, 0.0).astype(BF16)
        bb = jnp.dot(rel_hi, pick, preferred_element_type=F32)
        bb = bb + jnp.dot(rel_mid, pick, preferred_element_type=F32)
        bb = bb + jnp.dot(rel_lo, pick, preferred_element_type=F32)
        bias_s[b, 0:HEADS, :] = jnp.where(lane12 <= pos_s[b], bb, NEG)
    for name in ('wq', 'wk', 'wv', 'ln2', 'ln3', 'wr', 'wqc0', 'wqc1', 'woc0', 'woc1'):
        loads[name].wait()

    for dist, ky in near_first:
        gather_step(m1, 0, 0, dist, ky)
    for dist in range(4):
        for ky in (0, 1):
            arrived(m1, 0, fwd.at[0, chip_of(dist, ky)])
    xn = m1[...].astype(F32).reshape(NDEV * ROWS, D).astype(BF16)
    st2[...] = dot_nt(xn, wqkv[...]).reshape(NDEV, ROWS, 256).astype(BF16)
    r2[me] = st2[me]
    for dev in far_first():
        send_to(st2.at[dev], r2.at[me], 1, dev)
    weight_start(wgq, 9)
    load('ck', ckT, ck_v)
    load('cv', cvT, cv_v)

    sel_r = iota((4 * CB, D), 0)
    sel_q = ((sel_r >= CB).astype(jnp.int32) + (sel_r >= 2 * CB).astype(jnp.int32)
             + (sel_r >= 3 * CB).astype(jnp.int32))
    sel = (iota((4 * CB, D), 1) == sel_r + sel_q * (4 * CB - CB) + s * CB)
    sel = jnp.where(sel, 1.0, 0.0).astype(BF16)
    desc(hs.at[pl.ds(0, 3)], 7).wait_recv()
    h_sub = hs[...].astype(F32).reshape(4 * ROWS, D).astype(BF16)
    h_blk = dot_nt(h_sub, sel)

    weight_pass(wgo, 8)
    loads['k'].wait()
    loads['v'].wait()
    desc(r2.at[pl.ds(0, NDEV - 1)], 1).wait_recv()
    weight_start(wgc, 10)
    rv = r2[...].astype(F32)

    def columns(lo):
        return jnp.concatenate([rv[d, :, lo:lo + CB] for d in range(NDEV)], axis=-1)

    q8 = columns(0)
    k8 = columns(CB)
    v8 = columns(2 * CB)
    lane_h = iota((HPAD, LS), 1)
    attention(q8, k_old, v_old, lambda b: bias_s[b], s_self, ctx_v, q_v,
              (k8, v8, lambda b: lane_h == pos_s[b]))

    def update(new, old, out):
        cols = new.T
        lane_s = iota((D, LS), 1)
        for b in range(ROWS):
            out[b] = jnp.where(lane_s == pos_s[b], jnp.broadcast_to(cols[:, b:b + 1], (D, LS)),
                               old[b].astype(F32)).astype(BF16)

    def natural(pieces):
        return jnp.concatenate([pieces[t][:, q * CB:(q + 1) * CB] for q in range(4) for t in range(4)], axis=-1)

    def pack(buf, i, blk):
        buf[i, 0:32, :] = blk[:, 0:128].astype(BF16)
        buf[i, 32:48, :] = jnp.concatenate([blk[0:16, 128:192], blk[16:32, 128:192]], axis=-1).astype(BF16)

    def unpack(blk):
        tail = jnp.concatenate([blk[32:48, 0:64], blk[32:48, 64:128]], axis=0)
        return jnp.concatenate([blk[0:32, :], tail], axis=-1)

    c3[s] = ctx_v[...].astype(BF16)
    subgroup(c3, 2)
    weight_pass(wgq, 9)
    update(k8, k_old, k_v)
    update(v8, v_old, v_v)
    for off in ALL_OFFS:
        send(ix.at[me], ix.at[me], 12, off)
        send(rw.at[me], rw.at[me], 11, off)
    load('win', win, win_v)
    load('wout', wout, wout_v)
    desc(c3.at[pl.ds(0, 3)], 2).wait_recv()
    weight_finish(wgo, 8)
    ctx = c3[...].astype(F32).reshape(4 * ROWS, D).astype(BF16)
    h1_blk = (h_blk + dot_nt(ctx, wgo[...].reshape(4 * CB, D))).astype(BF16)
    pack(r4, s, h1_blk.astype(F32))
    subgroup(r4, 3)
    desc(r4.at[pl.ds(0, 3)], 3).wait_recv()
    weight_finish(wgq, 9)
    r4f = r4[...].astype(F32)
    h1 = natural([unpack(r4f[t]) for t in range(4)])
    x2 = rms(h1, ln2_v[...].reshape(1, D))
    st5[:, :, 0:4 * CB] = dot_nt(x2, wgq[...].reshape(4 * CB, D)).reshape(4, ROWS, 4 * CB).astype(BF16)
    r5[s] = st5[s]
    for off in SUB_OFFS:
        kz, ky, kc = off
        send(st5.at[((y + ky) % 2) * 2 + (c + kc) % 2], r5.at[s], 4, off)
    weight_pass(wgc, 10)
    loads['ck'].wait()
    loads['cv'].wait()
    desc(r5.at[pl.ds(0, 3)], 4).wait_recv()
    r5f = r5[...].astype(F32)
    q2 = natural([r5f[t] for t in range(4)])
    attention(q2, ck_v, cv_v, lambda b: jnp.where(mask_v[b:b + 1, :] == 1, 0.0, NEG), s_cross, ctx_v, q_v)

    c6[s] = ctx_v[...].astype(BF16)
    subgroup(c6, 5)
    desc(c6.at[pl.ds(0, 3)], 5).wait_recv()
    weight_finish(wgc, 10)
    ctx2 = c6[...].astype(F32).reshape(4 * ROWS, D).astype(BF16)
    h2_blk = (h1_blk.astype(F32) + dot_nt(ctx2, wgc[...].reshape(4 * CB, D))).astype(BF16)
    pack(r7, me, h2_blk.astype(F32))

    gather_start(r7, 6, 1)
    desc(ix.at[pl.ds(0, NDEV - 1)], 12).wait_recv()
    idx_all = ix[...].astype(F32).reshape(NDEV * ROWS, 128)
    idx_t = idx_all.T
    earlier = (idx_t[0:ROWS, :] == idx_own) & (iota((ROWS, 128), 1) < me * ROWS + row8)
    slot = jnp.sum(jnp.where(earlier, 1.0, 0.0), axis=-1, keepdims=True)
    loads['win'].wait()
    loads['wout'].wait()

    def group(dist):
        for ky in (0, 1):
            arrived(r7, 6, fwd.at[1, chip_of(dist, ky)])
        t = z_near[dist]
        h2g = natural([unpack(r7[4 * t + u].astype(F32)) for u in range(4)])
        at = pl.ds(pl.multiple_of(32 * t, 32), 32)
        h2_v[at, :] = h2g
        x3_v[at, :] = rms(h2g, ln3_v[...].reshape(1, D))

    for dist, ky in near_first[:5]:
        gather_step(r7, 6, 1, dist, ky)
    group(0)
    gather_step(r7, 6, 1, *near_first[5])
    gather_step(r7, 6, 1, *near_first[6])
    group(1)
    group(2)
    group(3)
    x3 = x3_v[...]
    idx3 = jnp.concatenate([idx_all, idx_all, idx_all], axis=-1)
    half = (iota((NDEV * ROWS, 384), 1) >= 192).astype(F32)
    for p in range(8):
        hh = dot_nt(x3, win_v[2 * p:2 * p + 2].reshape(384, D))
        u_v[:, 384 * p:384 * p + 384] = jnp.where(idx3 == half + float(2 * p), jnp.maximum(hh, 0.0), 0.0).astype(BF16)
    def partial(n):
        yn = jnp.dot(u_v[...], wout_v[:, :, 256 * n:256 * n + 256].reshape(NDEV * 192, 256),
                     preferred_element_type=F32).reshape(8, 2, ROWS, 256)
        st8[n, 0] = yn[:, 0]
        st8[n, 1] = yn[:, 1]
        send(st8.at[n, 1 - c], r8.at[n], 13 + n, SIBLING)

    def reduce_send(n):
        desc(r8.at[n], 13 + n).wait_recv()
        st9[n] = st8[n, c] + r8[n]
        for dist, ky in near_first[::-1]:
            dest = chip_of(dist, ky)
            send_to(st9.at[n, dest], r9.at[n, chip], 16 + n, dest * 2 + c)
        r9[n, chip] = st9[n, chip]

    partial(0)
    partial(1)
    partial(2)
    reduce_send(0)
    reduce_send(1)
    reduce_send(2)

    desc(rw.at[pl.ds(0, NDEV - 1)], 11).wait_recv()
    h2_own = h2_v[pl.ds(pl.multiple_of(me * ROWS, ROWS), ROWS), :]
    x3_own = rms(h2_own, ln3_v[...].reshape(1, D)).astype(F32)
    logits = dot_nt(x3_own, rw[...].reshape(NDEV, D), precision=lax.Precision.HIGHEST)
    ex = jnp.exp(logits - jnp.max(logits, axis=-1, keepdims=True))
    probs = ex / jnp.sum(ex, axis=-1, keepdims=True)
    mine = iota((ROWS, NDEV), 1).astype(F32) == idx_own[:, 0:NDEV]
    gate = jnp.sum(jnp.where(mine, probs, 0.0), axis=-1, keepdims=True)
    gate = jnp.where(slot < float(NDEV), gate, 0.0)

    for n in range(3):
        desc(r9.at[n, pl.ds(0, 7)], 16 + n).wait_recv()
    yv = jnp.concatenate([jnp.sum(r9[n], axis=0) for n in range(3)], axis=-1).astype(BF16).astype(F32)
    out_h[...] = (h2_own + yv * gate).astype(BF16)

    for buf, ph in ((m1, 0), (st2, 1), (r7, 6), (rw, 11), (ix, 12)):
        desc(buf.at[pl.ds(0, NDEV - 1)], ph).wait_send()
    for n in range(3):
        desc(st9.at[n, pl.ds(0, 7)], 16 + n).wait_send()
        desc(r8.at[n], 13 + n).wait_send()
    for buf, ph in ((c3, 2), (r4, 3), (st5, 4), (c6, 5), (hs, 7)):
        desc(buf.at[pl.ds(0, 3)], ph).wait_send()
    for w, ph in ((wgo, 8), (wgq, 9), (wgc, 10)):
        desc(w.at[pl.ds(0, 3), 0], ph).wait_send()
        desc(w.at[pl.ds(0, 3), 0], ph + 11).wait_send()


def store(h_in, k_in, v_in, h_out, k_out, v_out, sem):
    copies = [pltpu.make_async_copy(src, dst, sem.at[i])
              for i, (src, dst) in enumerate(((k_in, k_out), (v_in, v_out), (h_in, h_out)))]
    for cp in copies:
        cp.start()
    for cp in copies:
        cp.wait()


def solution(mesh):
    rows = ('dp', 'ws')
    row_vec = P(rows)
    row_mat = P(rows, None)
    cache = P(rows, None, None, None)
    col = P(None, 'ws')
    in_specs = (row_mat, cache, cache, cache, cache, row_vec, row_mat, P(None, None), row_vec,
                P(None), P(None), P(None), col, col, col, col, col, col,
                col, P(None, None, 'ws'), P(None, 'ws', None))
    out_specs = (row_mat, cache, cache)

    any_spec = pl.BlockSpec(memory_space=pltpu.HBM)
    vmem = pl.BlockSpec(memory_space=pltpu.VMEM)

    def block(hidden, self_k, self_v, cross_k, cross_v, positions, enc_mask, rel_bias, expert_idx,
              ln_self, ln_cross, ln_ffn, wq_self, wk_self, wv_self, wo_self, wq_cross, wo_cross,
              w_router, w_in, w_out):
        def flat(cache_arr):
            return jnp.swapaxes(cache_arr, 2, 3).reshape(ROWS, D, cache_arr.shape[2])

        def unflat(arr):
            return jnp.swapaxes(arr.reshape(ROWS, HEADS, 64, LS), 2, 3)

        args = (hidden, flat(self_k), flat(self_v), flat(cross_k), flat(cross_v), positions, enc_mask, rel_bias,
                expert_idx, ln_self, ln_cross, ln_ffn,
                wq_self.T, wk_self.T, wv_self.T, wo_self.T, wq_cross.T, wo_cross.T, w_router.T,
                jnp.swapaxes(w_in, 1, 2), w_out)
        specs = [any_spec] * len(args)
        V = pltpu.VMEM
        scratch = [
            V((ROWS, D, LC), BF16), V((ROWS, D, LC), BF16), V((NDEV, 192, D), BF16), V((NDEV, 192, D), BF16),
            V((ROWS, LC), jnp.int32), V((HEADS, LS), F32), V((D,), F32), V((D,), F32), V((D,), F32), V((256, D), BF16),
            V((NDEV, ROWS, D), BF16), V((NDEV, ROWS, 128), BF16), V((NDEV, ROWS, 256), BF16), V((NDEV, ROWS, 256), BF16),
            V((4, 2, CB // 2, D), BF16), V((4, 2, CB // 2, D), BF16), V((4, 2, CB // 2, D), BF16), V((NDEV, 1, D), F32),
            V((4, ROWS, D), BF16), V((4, CB, 128), BF16), V((4, ROWS, 256), BF16), V((4, ROWS, 256), BF16),
            V((4, ROWS, D), BF16), V((NDEV, CB, 128), BF16), V((3, 2, 8, ROWS, 256), F32), V((3, 8, ROWS, 256), F32),
            V((3, 8, ROWS, 256), F32), V((3, 8, ROWS, 256), F32),
            V((ROWS, HPAD, LS), F32), V((ROWS, HPAD, LS), F32), V((ROWS, HPAD, LC), F32), V((ROWS, D), F32),
            V((NDEV * ROWS, D), F32), V((NDEV * ROWS, D), BF16), V((NDEV * ROWS, NDEV * 192), BF16),
            V((ROWS, D, LS), BF16), V((ROWS, D, LS), BF16), V((4, ROWS, D), BF16), V((ROWS, HPAD, D), BF16),
            pltpu.SMEM((ROWS,), jnp.int32), pltpu.SMEM((ROWS,), jnp.int32),
            pltpu.SemaphoreType.DMA((24,)), pltpu.SemaphoreType.DMA((22,)), pltpu.SemaphoreType.DMA((22,)),
            pltpu.SemaphoreType.DMA((2, 8)), pltpu.SemaphoreType.DMA((2, 8)),
        ]
        h_out, k_out, v_out = pl.pallas_call(
            kernel,
            out_shape=(V((ROWS, D), BF16), V((ROWS, D, LS), BF16), V((ROWS, D, LS), BF16)),
            in_specs=specs,
            out_specs=(vmem, vmem, vmem),
            scratch_shapes=scratch,
            compiler_params=pltpu.CompilerParams(collective_id=0, has_side_effects=True,
                                                 vmem_limit_bytes=67043328 - 2 * 3145728 - 16384),
        )(*args)
        outs = (jax.ShapeDtypeStruct((ROWS, D), BF16), jax.ShapeDtypeStruct((ROWS, D, LS), BF16),
                jax.ShapeDtypeStruct((ROWS, D, LS), BF16))
        h_out, k_out, v_out = pl.pallas_call(
            store, out_shape=outs, in_specs=[vmem] * 3, out_specs=(any_spec,) * 3,
            scratch_shapes=[pltpu.SemaphoreType.DMA((3,))],
            compiler_params=pltpu.CompilerParams(vmem_limit_bytes=4 * 1024 * 1024),
        )(h_out, k_out, v_out)
        return h_out, unflat(k_out), unflat(v_out)

    return jax.shard_map(block, mesh=mesh, in_specs=in_specs, out_specs=out_specs, check_vma=False)
```
